32 devices in a mesh: ens: 2 (over y), box: 4 (over z), slab: 4 (over x, core).
Axes of the slice: x: 2, y: 2, z: 4, core: 2. Of those that a mesh axis runs over, the one named last changes fastest.
Arguments:
- pressure_now: float32 [4, 64, 64, 256], P('ens', 'box', 'slab'), parts along dimension 0, may hold values from -6 to 6
- pressure_prev: float32 [4, 64, 64, 256], P('ens', 'box', 'slab'), parts along dimension 0, may hold values from -6 to 6
- courant_sq: float32 [64, 64, 256], P('box', 'slab'), may hold values from 0.04 to 0.28
- member_profiles: float32 [8, 64], replicated, may hold values from -0.15 to 0.15
- member_ids: int32 [4], P('ens'), parts along dimension 0, may hold values from 0 to 7, as said below
- stored_slabs: float32 [8, 16, 6144], P('slab'), may hold values from -6 to 6
- slab_home: int32 [2], P('ens'), parts along dimension 0, may hold values from 0 to 7
- interp_weights: float32 [2, 16], replicated, may hold values from -1.5 to 1.5
- surface_cells: int32 [6, 1024], replicated, may hold values from 0 to 1048575, as said below
Outputs:
- pressure_next: float32 [4, 64, 64, 256], P('ens', 'box', 'slab'), parts along dimension 0
- pressure_last: float32 [4, 64, 64, 256], P('ens', 'box', 'slab'), parts along dimension 0
The draws below stay inside these ranges and needn't reach their ends.
There are 2 independent parts, one for each index of `ens`. The reference program is written for one: setup_inputs(seed, part) draws one part's arguments, and reference() takes and returns one part's arrays. A program takes and returns all parts, laid end to end along the dimension named above; an argument that names none is the same for every part. Nothing has to cross between parts.
Inputs may be any that keep to these rules, and one draw needn't show every extreme that they name: `surface_cells`: row f lists 1024 cells, flat index (x 64 + z) * 256 + y, on one face of the box surface 0 cells inside the grid: x low, x high, z low, z high, y low, y high in this order; the other two coordinates lie on the surface; on every face other than the two depth faces, every depth of the surface occurs; cells may repeat. `slab_home`: block k is stored on the slab device k // 2, in its slot k % 2. `member_ids`: the members' profiles are all different.
All inputs are finite; a program needn't handle non-finite values.
Results may differ from the reference program's by a relative error of at most 0.000098.
Values sent between devices are 32-bit elements; how exact they have to be, the bound alone decides.
No kernel may reach another device: no remote copies, remote signals or barrier semaphores. Data moves between devices by JAX's collectives and lax.ppermute only.
A program may use at most 64 MiB of HBM per device.

```python
import math
import jax
import jax.numpy as jnp
from jax import lax

MEMBERS = 2
STEPS = 2
SLAB_LEN = 16
BANK = 8
HUYGENS_GAP = 0
NY = 256
PTS_FACE = 1024
NX = 64
NZ = 64
BLOCKS = 8
POINTS = 6144


def draw_member_ids(key, part):
    order = jax.random.permutation(jax.random.fold_in(key, 29), jnp.arange(BANK, dtype=jnp.int32))
    return order[:MEMBERS].astype(jnp.int32)


def draw_surface_cells(key, part):
    subkeys = jax.random.split(jax.random.fold_in(key, 17), 4)
    face_index = jnp.arange(6, dtype=jnp.int32)[:, None]
    point_index = jnp.arange(PTS_FACE, dtype=jnp.int32)[None, :]
    along_x = jax.random.randint(subkeys[0], (6, PTS_FACE), HUYGENS_GAP, NX - HUYGENS_GAP)
    along_z = jax.random.randint(subkeys[1], (6, PTS_FACE), HUYGENS_GAP, NZ - HUYGENS_GAP)
    along_y = jax.random.randint(subkeys[2], (6, PTS_FACE), HUYGENS_GAP, NY - HUYGENS_GAP)
    depth_span = NZ - 2 * HUYGENS_GAP
    offset = jax.random.randint(subkeys[3], (6, 1), 0, depth_span)
    covering = HUYGENS_GAP + (point_index + offset) % depth_span
    along_z = jnp.where(point_index < depth_span, covering, along_z)
    along_x = jnp.where(face_index == 0, HUYGENS_GAP, jnp.where(face_index == 1, NX - 1 - HUYGENS_GAP, along_x))
    along_z = jnp.where(face_index == 2, HUYGENS_GAP, jnp.where(face_index == 3, NZ - 1 - HUYGENS_GAP, along_z))
    along_y = jnp.where(face_index == 4, HUYGENS_GAP, jnp.where(face_index == 5, NY - 1 - HUYGENS_GAP, along_y))
    return ((along_x * NZ + along_z) * NY + along_y).astype(jnp.int32)


def levels(own_key, extent, cuts, smallest, high):
    gain, own = 1.0, jax.random.fold_in(own_key, 6)
    for position, parts in cuts:
        heights = jnp.exp(jax.random.uniform(jax.random.fold_in(own, position), (parts,), jnp.float32, smallest / len(cuts), high / len(cuts)))
        gain = gain * jnp.repeat(heights, extent[position] // parts).reshape([-1 if axis == position else 1 for axis in range(len(extent))])
    return gain


def gaussian(rng, shape, width, reach, cuts=(), kind=jnp.bfloat16):
    values = jax.random.normal(rng, shape, jnp.float32) * width
    if len(cuts) > 0:
        values = levels(rng, shape, cuts, -0.22, 0.18) * values
    return jnp.clip(values, min=-reach, max=reach).astype(kind)


def setup_inputs(seed: int = 0, part: int = 0) -> dict:
    arg_keys = jax.random.split(jax.random.key(seed), 10)
    part_splits = jax.random.split(jax.random.fold_in(arg_keys[9], part), 10)
    pressure_now = gaussian(part_splits[0], (MEMBERS, NX, NZ, NY), 1.0, 6.0, ((1, 4), (2, 4)), jnp.float32)
    pressure_prev = gaussian(part_splits[1], (MEMBERS, NX, NZ, NY), 1.0, 6.0, ((1, 4), (2, 4)), jnp.float32)
    courant_sq = jnp.clip(jnp.exp(math.log(0.28) - 1.9459102 * jax.random.uniform(arg_keys[2], (NX, NZ, NY), jnp.float32) ** levels(arg_keys[2], (NX, NZ, NY), ((0, 4), (1, 4)), -0.2, 0.2)), 0.04, 0.28)
    member_profiles = jnp.clip(jax.random.uniform(arg_keys[3], (BANK, NZ), jnp.float32, -0.15, 0.15), -0.15, 0.15)
    member_ids = draw_member_ids(jax.random.fold_in(jax.random.fold_in(arg_keys[9], part), 71), part)
    stored_slabs = gaussian(arg_keys[5], (BLOCKS, SLAB_LEN, POINTS), 1.0, 6.0, ((0, 4),), jnp.float32)
    slab_home = jax.random.randint(part_splits[6], (1,), 0, BLOCKS).astype(jnp.int32)
    interp_weights = gaussian(arg_keys[7], (STEPS, SLAB_LEN), 0.3, 1.5, (), jnp.float32)
    surface_cells = draw_surface_cells(jax.random.fold_in(arg_keys[9], 71), part)
    return {"pressure_now": pressure_now, "pressure_prev": pressure_prev, "courant_sq": courant_sq, "member_profiles": member_profiles, "member_ids": member_ids, "stored_slabs": stored_slabs, "slab_home": slab_home, "interp_weights": interp_weights, "surface_cells": surface_cells}


def laplace(ext):
    inner = ext[:, 1:-1, 1:-1, :]
    beside = ext[:, 2:, 1:-1, :] + ext[:, :-2, 1:-1, :]
    beside = beside + ext[:, 1:-1, 2:, :] + ext[:, 1:-1, :-2, :]
    padded = jnp.pad(inner, ((0, 0), (0, 0), (0, 0), (1, 1)))
    beside = beside + padded[:, :, :, 2:] + padded[:, :, :, :-2]
    return beside - 6.0 * inner


def reference(pressure_now, pressure_prev, courant_sq, member_profiles, member_ids, stored_slabs, slab_home, interp_weights, surface_cells):
    profile = member_profiles[member_ids]
    coef = courant_sq[None] * (1.0 + profile[:, None, :, None])
    block = lax.dynamic_index_in_dim(stored_slabs, slab_home[0], 0, keepdims=False)
    values = jnp.dot(interp_weights, block, precision=lax.Precision.HIGHEST)
    cells = surface_cells.reshape(-1)
    prev, now = pressure_prev, pressure_now
    for step in range(STEPS):
        ext = jnp.pad(now, ((0, 0), (1, 1), (1, 1), (0, 0)))
        nxt = 2.0 * now - prev + coef * laplace(ext)
        source = jnp.zeros((NX * NZ * NY,), jnp.float32).at[cells].add(values[step])
        nxt = nxt + source.reshape(NX, NZ, NY)[None]
        prev, now = now, nxt
    return now, prev
```

```python
import functools

import jax
import jax.numpy as jnp
from jax import lax
from jax.experimental import pallas as pl
from jax.experimental.pallas import tpu as pltpu
from jax.sharding import PartitionSpec as P


F32 = jnp.float32
BF16 = jnp.bfloat16
VMEM = pl.BlockSpec(memory_space=pltpu.VMEM)
SMEM = pl.BlockSpec(memory_space=pltpu.SMEM)
HBM = pl.BlockSpec(memory_space=pl.ANY)


def rows_of(shape, axis):
    return lax.broadcasted_iota(jnp.int32, shape, axis)


def beside_y(v):
    length = v.shape[1]
    lane = rows_of(v.shape, 1)
    left = jnp.where(lane == 0, 0.0, pltpu.roll(v, 1, 1))
    right = jnp.where(lane == length - 1, 0.0, pltpu.roll(v, length - 1, 1))
    return left + right


def beside_rows(v, low, high):
    length = v.shape[0]
    row = rows_of(v.shape, 0)
    down = jnp.where(row == 0, low, pltpu.roll(v, 1, 0))
    up = jnp.where(row == length - 1, high, pltpu.roll(v, length - 1, 0))
    return down + up


def profile_planes(ids, prof, members, start_z, width_z, depth_y):
    row = rows_of((width_z, depth_y), 0)
    planes = []
    for m in range(members):
        plane = jnp.zeros((width_z, depth_y), F32)
        for z in range(width_z):
            plane = jnp.where(row == z, 1.0 + prof[ids[m], start_z + z], plane)
        planes.append(plane)
    return planes


def pack_kernel(
    slots, ids, home, weights, prof, now, prev, cour, slabs,
    local, za, zb, vals, xa, xb, block, sem,
):
    members, width_x, width_z, depth_y = now.shape
    steps, samples = weights.shape
    box, slab = lax.axis_index("box"), lax.axis_index("slab")
    fetch = pltpu.make_async_copy(slabs.at[lax.rem(home[0], slots)], block, sem)
    fetch.start()
    planes = profile_planes(ids, prof, members, slab * width_z, width_z, depth_y)
    zero = jnp.zeros((1, depth_y), F32)
    for m in range(members):
        for x in range(width_x):
            here = now[m, x]
            near = beside_y(here) + beside_rows(here, zero, zero)
            if x > 0:
                near = near + now[m, x - 1]
            if x < width_x - 1:
                near = near + now[m, x + 1]
            coef = cour[x] * planes[m]
            local[m, x] = 2.0 * here - prev[m, x] + coef * (near - 6.0 * here)
    face = lax.rem(box, 2)
    for out, x in ((xa, (1 - face) * (width_x - 1)), (xb, face * (width_x - 1))):
        for m in range(members):
            out[m * width_z : (m + 1) * width_z] = now[m, x]
            out[(members + m) * width_z : (members + m + 1) * width_z] = local[m, x]
        out[2 * members * width_z : (2 * members + 1) * width_z] = cour[x]
    side = lax.rem(slab, 2)
    for out, high in ((za, side == 0), (zb, side == 1)):

        def put(at, low_rows, high_rows):
            out[at * width_x : (at + 1) * width_x] = jnp.where(high, high_rows, low_rows)

        for m in range(members):
            put(m, now[m, :, 0], now[m, :, width_z - 1])
            put(members + m, local[m, :, 0], local[m, :, width_z - 1])
        put(2 * members, cour[:, 0], cour[:, width_z - 1])
    fetch.wait()
    owner = slab == home[0] // slots
    tail = (2 * members + 1) * width_x
    points = block.shape[1]
    chunks = points // depth_y
    sample = rows_of((samples, depth_y), 0)
    for t in range(steps):
        column = jnp.zeros((samples, depth_y), F32)
        for k in range(samples):
            column = jnp.where(sample == k, weights[t, k], column)
        column = jnp.where(owner, column, 0.0)
        for c in range(chunks):
            row = jnp.sum(column * block[:, c * depth_y : (c + 1) * depth_y], axis=0, keepdims=True)
            at = t * chunks + c
            vals[at : at + 1] = row
            za[tail + at : tail + at + 1] = row
            zb[tail + at : tail + at + 1] = row


def corner_kernel(members, width_x, za, zb, ca, cb):
    box, slab = lax.axis_index("box"), lax.axis_index("slab")
    face, side = lax.rem(box, 2), lax.rem(slab, 2)
    for out, last in ((ca, face == 0), (cb, face == 1)):
        for m in range(members):
            lo, hi = m * width_x, (m + 1) * width_x - 1
            a = jnp.where(last, za[hi : hi + 1], za[lo : lo + 1])
            b = jnp.where(last, zb[hi : hi + 1], zb[lo : lo + 1])
            out[2 * m : 2 * m + 1] = jnp.where(side == 0, b, a)
            out[2 * m + 1 : 2 * m + 2] = jnp.where(side == 0, a, b)


def extended_row(coordinate, start, width):
    d = coordinate - start
    edge = jnp.where(d == -1, width, jnp.where(d == width, width + 1, -1))
    return jnp.where((d >= 0) & (d < width), d, edge)


def three_parts(v):
    first = v.astype(BF16)
    rest = v - first.astype(F32)
    second = rest.astype(BF16)
    third = (rest - second.astype(F32)).astype(BF16)
    return first, second, third


def contract(lhs, rhs):
    return lax.dot_general(lhs, rhs, (((1,), (1,)), ((), ())), preferred_element_type=F32)


def face_source(values, row_index, lane_index, high, wide):
    points = row_index.shape[1]
    row = rows_of((high, points), 0)
    lane = rows_of((wide, points), 0)
    hit = row == row_index
    parts = []
    for v in values:
        for part in three_parts(v):
            parts.append(jnp.where(hit, part.astype(F32), 0.0).astype(BF16))
    lhs = jnp.concatenate(parts, axis=0)
    rhs = jnp.where(lane == lane_index, 1.0, 0.0).astype(BF16)
    out = contract(lhs, rhs)
    sums = []
    for t in range(len(values)):
        at = 3 * t * high
        one = out[at : at + high]
        two = out[at + high : at + 2 * high]
        three = out[at + 2 * high : at + 3 * high]
        sums.append((three + two) + one)
    return sums


def main_kernel(
    boxes, slabs, total_z, received, ids, prof, cells, now, local, cour, vals, za, zb, xa, xb, ca, cb,
    *rest,
):
    others, rest = rest[:received], rest[received:]
    nxt, one, xlo, xhi, zlo, zhi, value, src, xsrc, zsrc, hzlo, hzhi = rest
    members, width_x, width_z, depth_y = now.shape
    steps = src.shape[0]
    box, slab = lax.axis_index("box"), lax.axis_index("slab")
    start_x, start_z = box * width_x, slab * width_z
    face, side = lax.rem(box, 2), lax.rem(slab, 2)
    low_x, high_x = box > 0, box < boxes - 1
    low_z, high_z = slab > 0, slab < slabs - 1
    span_x = (2 * members + 1) * width_z
    span_z = (2 * members + 1) * width_x
    xlo[...] = jnp.where(low_x, jnp.where(face == 0, xb[...], xa[...]), 0.0)
    xhi[...] = jnp.where(high_x, jnp.where(face == 0, xa[...], xb[...]), 0.0)
    zlo[...] = jnp.where(low_z, jnp.where(side == 0, zb[:span_z], za[:span_z]), 0.0)
    zhi[...] = jnp.where(high_z, jnp.where(side == 0, za[:span_z], zb[:span_z]), 0.0)
    total = vals[...] + za[span_z:]
    if slabs == 4:
        total = total + zb[span_z:]
    for other in others:
        total = total + other[...]
    value[...] = total

    faces, per_face = cells.shape
    chunks = value.shape[0] // steps
    per = chunks // faces
    plane_size = total_z * depth_y
    low_high = (width_x + 2 + 15) // 16 * 16, (width_z + 2 + 15) // 16 * 16

    def of_face(f):
        cell = cells[pl.ds(f, 1), :]
        cx = cell // plane_size
        remain = cell - cx * plane_size
        cz = remain // depth_y
        cy = remain - cz * depth_y
        vs = []
        for t in range(steps):
            pieces = [value[pl.ds(t * chunks + f * per + i, 1), :] for i in range(per)]
            vs.append(jnp.concatenate(pieces, axis=1))
        return extended_row(cx, start_x, width_x), extended_row(cz, start_z, width_z), cy, vs

    on_x = (box == 0) | (box == boxes - 1)
    on_z = (slab == 0) | (slab == slabs - 1)
    rx, rz, ry, vs = of_face(jnp.where(box == 0, 0, 1))
    for t, s in enumerate(face_source(vs, jnp.where(on_x, rz, -1), ry, low_high[1], depth_y)):
        xsrc[t] = s
    rx, rz, ry, vs = of_face(jnp.where(slab == 0, 2, 3))
    for t, s in enumerate(face_source(vs, jnp.where(on_z, rx, -1), ry, low_high[0], depth_y)):
        zsrc[t] = s
    rx, rz, ry, vs = of_face(4)
    ylow = face_source(vs, rz, rx, low_high[1], 128)
    rx, rz, ry, vs = of_face(5)
    yhigh = face_source(vs, rz, rx, low_high[1], 128)

    lane = rows_of((width_z, depth_y), 1)
    row = rows_of((width_z, depth_y), 0)
    row_of_z = jnp.where(slab == 0, 0, jnp.where(slab == slabs - 1, width_z - 1, -1))
    row_of_x = jnp.where(box == 0, 0, jnp.where(box == boxes - 1, width_x - 1, -1))

    def column(t, x):
        lo = ylow[t][:width_z, x : x + 1]
        hi = yhigh[t][:width_z, x : x + 1]
        return jnp.where(lane == 0, lo, jnp.where(lane == depth_y - 1, hi, 0.0))

    def plane_source(t, x):
        out = column(t, x)
        out = out + jnp.where(row == row_of_z, zsrc[t, x : x + 1, :], 0.0)
        if x in (0, width_x - 1):
            out = out + jnp.where(row_of_x == x, xsrc[t, :width_z, :], 0.0)
        return out

    for t in range(steps):
        for x in range(width_x):
            src[t, x] = plane_source(t, x)
    halo_src_x = [plane_source(0, width_x), plane_source(0, width_x + 1)]
    lane_x = rows_of((width_x, depth_y), 1)
    row_x = rows_of((width_x, depth_y), 0)
    turned = [jnp.transpose(ylow[0]), jnp.transpose(yhigh[0])]
    halo_src_z = []
    for z in (width_z, width_z + 1):
        lo = turned[0][:width_x, z : z + 1]
        hi = turned[1][:width_x, z : z + 1]
        out = jnp.where(lane_x == 0, lo, jnp.where(lane_x == depth_y - 1, hi, 0.0))
        halo_src_z.append(out + jnp.where(row_x == row_of_x, xsrc[0, z : z + 1, :], 0.0))

    planes = profile_planes(ids, prof, members, start_z, width_z, depth_y)
    beyond = (jnp.maximum(start_z - 1, 0), jnp.minimum(start_z + width_z, total_z - 1))
    for m in range(members):
        lo_row, hi_row = m * width_x, m * width_z
        halo_x = []
        for s, (ref, x, got) in enumerate(((xlo, 0, (xb, xa)), (xhi, width_x - 1, (xa, xb)))):
            c = (cb, ca) if s == 0 else (ca, cb)
            d_low = jnp.where(face == 0, c[0][2 * m : 2 * m + 1], c[1][2 * m : 2 * m + 1])
            d_high = jnp.where(face == 0, c[0][2 * m + 1 : 2 * m + 2], c[1][2 * m + 1 : 2 * m + 2])
            d_low = jnp.where(low_z, d_low, 0.0)
            d_high = jnp.where(high_z, d_high, 0.0)
            coef = ref[2 * members * width_z :] * planes[m]
            own = now[m, x] + jnp.where(row == 0, d_low, 0.0) + jnp.where(row == width_z - 1, d_high, 0.0)
            base = ref[(members + m) * width_z : (members + m + 1) * width_z]
            halo_x.append(base + coef * own + halo_src_x[s])
        for s, (ref, out, z) in enumerate(((zlo, hzlo, 0), (zhi, hzhi, width_z - 1))):
            at = 2 * m + s
            open_z = low_z if s == 0 else high_z
            d_low = jnp.where(face == 0, cb[at : at + 1], ca[at : at + 1])
            d_high = jnp.where(face == 0, ca[at : at + 1], cb[at : at + 1])
            d_low = jnp.where(low_x, d_low, 0.0)
            d_high = jnp.where(high_x, d_high, 0.0)
            coef = ref[2 * members * width_x :] * (1.0 + prof[ids[m], beyond[s]])
            own = now[m, :, z]
            own = own + jnp.where(row_x == 0, d_low, 0.0) + jnp.where(row_x == width_x - 1, d_high, 0.0)
            base = ref[(members + m) * width_x : (members + m + 1) * width_x]
            out[...] = base + coef * own + halo_src_z[s]
        for x in range(width_x):
            at = m * width_x + x
            more = jnp.where(row == 0, zlo[at : at + 1], 0.0)
            more = more + jnp.where(row == width_z - 1, zhi[at : at + 1], 0.0)
            if x == 0:
                more = more + xlo[m * width_z : (m + 1) * width_z]
            if x == width_x - 1:
                more = more + xhi[m * width_z : (m + 1) * width_z]
            one[m, x] = local[m, x] + (cour[x] * planes[m]) * more + src[0, x]
        for x in range(width_x):
            here = one[m, x]
            near = beside_y(here) + beside_rows(here, hzlo[x : x + 1], hzhi[x : x + 1])
            near = near + (one[m, x - 1] if x > 0 else halo_x[0])
            near = near + (one[m, x + 1] if x < width_x - 1 else halo_x[1])
            coef = cour[x] * planes[m]
            nxt[m, x] = 2.0 * here - now[m, x] + coef * (near - 6.0 * here) + src[1, x]


def pairs_even(n):
    return [i ^ 1 for i in range(n)]


def pairs_odd(n):
    return [(i + 1) % n if i % 2 else (i - 1) % n for i in range(n)]


def on_device(
    boxes, slabs, pressure_now, pressure_prev, courant_sq, member_profiles, member_ids,
    stored_slabs, slab_home, interp_weights, surface_cells,
):
    members, width_x, width_z, depth_y = pressure_now.shape
    slots, samples, points = stored_slabs.shape
    steps = interp_weights.shape[0]
    total_z = width_z * slabs
    value_rows = steps * points // depth_y
    span_x = (2 * members + 1) * width_z
    span_z = (2 * members + 1) * width_x

    def shape(*dims):
        return jax.ShapeDtypeStruct(dims, F32)

    local, za, zb, vals, xa, xb = pl.pallas_call(
        functools.partial(pack_kernel, slots),
        out_shape=(
            shape(*pressure_now.shape),
            shape(span_z + value_rows, depth_y),
            shape(span_z + value_rows, depth_y),
            shape(value_rows, depth_y),
            shape(span_x, depth_y),
            shape(span_x, depth_y),
        ),
        in_specs=[SMEM, SMEM, SMEM, SMEM, VMEM, VMEM, VMEM, HBM],
        out_specs=(VMEM,) * 6,
        scratch_shapes=[pltpu.VMEM((samples, points), F32), pltpu.SemaphoreType.DMA],
        name="pack",
    )(
        member_ids, slab_home, interp_weights, member_profiles,
        pressure_now, pressure_prev, courant_sq, stored_slabs,
    )

    def over_slab(x, partner):
        return lax.ppermute(x, "slab", list(enumerate(partner)))

    def over_box(x, odd):
        pairs = []
        for b in range(boxes):
            other = b ^ 1
            if odd:
                other = b + 1 if b % 2 else b - 1
            for s in range(slabs):
                inside = 0 <= other < boxes
                to = other * slabs + s if inside else b * slabs + (s ^ 1)
                pairs.append((b * slabs + s, to))
        return lax.ppermute(x, ("box", "slab"), pairs)

    za = over_slab(za, pairs_even(slabs))
    zb = over_slab(zb, pairs_odd(slabs))
    xa, xb = over_box(xa, False), over_box(xb, True)
    others = [
        over_slab(vals, [i ^ k for i in range(slabs)])
        for k in range(2, slabs)
        if slabs != 4 or k != 3
    ]
    ca, cb = pl.pallas_call(
        functools.partial(corner_kernel, members, width_x),
        out_shape=(shape(2 * members, depth_y),) * 2,
        in_specs=[VMEM, VMEM],
        out_specs=(VMEM, VMEM),
        name="corner",
    )(za, zb)
    ca, cb = over_box(ca, False), over_box(cb, True)

    high_x, high_z = (width_x + 2 + 15) // 16 * 16, (width_z + 2 + 15) // 16 * 16
    nxt, one = pl.pallas_call(
        functools.partial(main_kernel, boxes, slabs, total_z, len(others)),
        out_shape=(shape(*pressure_now.shape),) * 2,
        in_specs=[SMEM, SMEM] + [VMEM] * (11 + len(others)),
        out_specs=(VMEM, VMEM),
        scratch_shapes=[
            pltpu.VMEM((span_x, depth_y), F32),
            pltpu.VMEM((span_x, depth_y), F32),
            pltpu.VMEM((span_z, depth_y), F32),
            pltpu.VMEM((span_z, depth_y), F32),
            pltpu.VMEM((value_rows, depth_y), F32),
            pltpu.VMEM((steps, width_x, width_z, depth_y), F32),
            pltpu.VMEM((steps, high_z, depth_y), F32),
            pltpu.VMEM((steps, high_x, depth_y), F32),
            pltpu.VMEM((width_x, depth_y), F32),
            pltpu.VMEM((width_x, depth_y), F32),
        ],
        name="main",
    )(
        member_ids, member_profiles, surface_cells, pressure_now, local, courant_sq,
        vals, za, zb, xa, xb, ca, cb, *others,
    )
    return nxt, one


def solution(mesh):
    in_specs = (
        P("ens", "box", "slab", None),
        P("ens", "box", "slab", None),
        P("box", "slab", None),
        P(),
        P("ens"),
        P("slab", None, None),
        P("ens"),
        P(),
        P(),
    )
    out_specs = (P("ens", "box", "slab", None), P("ens", "box", "slab", None))
    boxes, slabs = mesh.shape["box"], mesh.shape["slab"]
    return jax.shard_map(
        functools.partial(on_device, boxes, slabs),
        mesh=mesh,
        in_specs=in_specs,
        out_specs=out_specs,
        check_vma=False,
    )
```

```python
import functools

import jax
import jax.numpy as jnp
from jax import lax
from jax.experimental import pallas as pl
from jax.experimental.pallas import tpu as pltpu
from jax.sharding import PartitionSpec as P


F32 = jnp.float32
BF16 = jnp.bfloat16
VMEM = pl.BlockSpec(memory_space=pltpu.VMEM)
SMEM = pl.BlockSpec(memory_space=pltpu.SMEM)
HBM = pl.BlockSpec(memory_space=pl.ANY)
PARAMS = pltpu.CompilerParams(vmem_limit_bytes=16 * 1024 * 1024)


def rows_of(shape, axis):
    return lax.broadcasted_iota(jnp.int32, shape, axis)


def beside_y(v):
    length = v.shape[1]
    lane = rows_of(v.shape, 1)
    left = jnp.where(lane == 0, 0.0, pltpu.roll(v, 1, 1))
    right = jnp.where(lane == length - 1, 0.0, pltpu.roll(v, length - 1, 1))
    return left + right


def beside_rows(v, low, high):
    length = v.shape[0]
    row = rows_of(v.shape, 0)
    down = jnp.where(row == 0, low, pltpu.roll(v, 1, 0))
    up = jnp.where(row == length - 1, high, pltpu.roll(v, length - 1, 0))
    return down + up


def pack_kernel(
    slots, home, ids_in, weights_in, prof_in, now_in, prev_in, cour_in, cells_in, slabs,
    now, prev, cour, cells, planes, edges, za, zb, vals, xa, xb, ids, weights, prof, block, sems,
):
    members, width_x, width_z, depth_y = now.shape
    steps, samples = weights.shape
    box, slab = lax.axis_index("box"), lax.axis_index("slab")
    total_z = prof.shape[1]
    loads = [
        pltpu.make_async_copy(source, target, sems.at[i])
        for i, (source, target) in enumerate((
            (ids_in, ids),
            (prof_in, prof),
            (weights_in, weights),
            (now_in, now),
            (cour_in, cour),
            (prev_in, prev),
            (slabs.at[lax.rem(home[0], slots)], block),
            (cells_in, cells),
        ))
    ]
    for load in loads:
        load.start()
    start_z = slab * width_z
    for load in loads[:3]:
        load.wait()
    row = rows_of((width_z, depth_y), 0)
    for m in range(members):
        plane = jnp.zeros((width_z, depth_y), F32)
        for z in range(width_z):
            plane = jnp.where(row == z, 1.0 + prof[ids[m], start_z + z], plane)
        planes[m] = plane
        for s, z in ((0, start_z - 1), (1, start_z + width_z)):
            beyond = 1.0 + prof[ids[m], jnp.clip(z, 0, total_z - 1)]
            edges[2 * m + s : 2 * m + s + 1] = jnp.full((1, depth_y), beyond, F32)
    zero = jnp.zeros((1, depth_y), F32)
    for load in loads[3:6]:
        load.wait()
    face, side = lax.rem(box, 2), lax.rem(slab, 2)
    xs = []
    for x, inner in ((0, 1), (width_x - 1, width_x - 2)):
        rows = []
        for m in range(members):
            here = now[m, x]
            around = beside_y(here) + beside_rows(here, zero, zero) + now[m, inner]
            coef = cour[x] * planes[m]
            rows.append((here, 2.0 * here - prev[m, x] + coef * (around - 6.0 * here)))
        xs.append([r[0] for r in rows] + [r[1] for r in rows] + [cour[x]])
    for i, (low, high) in enumerate(zip(*xs)):
        at = slice(i * width_z, (i + 1) * width_z)
        xa[at] = jnp.where(face == 0, high, low)
        xb[at] = jnp.where(face == 1, high, low)
    zs = []
    for z, inner in ((0, 1), (width_z - 1, width_z - 2)):
        rows = []
        for m in range(members):
            here = now[m, :, z]
            around = beside_y(here) + beside_rows(here, zero, zero) + now[m, :, inner]
            coef = cour[:, z] * (1.0 + prof[ids[m], start_z + z])
            rows.append((here, 2.0 * here - prev[m, :, z] + coef * (around - 6.0 * here)))
        zs.append([r[0] for r in rows] + [r[1] for r in rows] + [cour[:, z]])
    for i, (low, high) in enumerate(zip(*zs)):
        at = slice(i * width_x, (i + 1) * width_x)
        za[at] = jnp.where(side == 0, high, low)
        zb[at] = jnp.where(side == 1, high, low)
    owner = slab == home[0] // slots
    points = block.shape[1]
    chunks = points // depth_y
    sample = rows_of((samples, depth_y), 0)
    columns = []
    for t in range(steps):
        column = jnp.zeros((samples, depth_y), F32)
        for k in range(samples):
            column = jnp.where(sample == k, weights[t, k], column)
        columns.append(jnp.where(owner, column, 0.0))
    loads[6].wait()
    for c in range(chunks):
        piece = block[:, c * depth_y : (c + 1) * depth_y]
        for t in range(steps):
            at = t * chunks + c
            vals[at : at + 1] = jnp.sum(columns[t] * piece, axis=0, keepdims=True)
    tail = (2 * members + 1) * width_x
    loads[7].wait()
    offered = vals[...]
    za[tail:] = offered
    zb[tail:] = offered


def corner_kernel(members, width_z, xa, xb, after, ca, cb):
    box, slab = lax.axis_index("box"), lax.axis_index("slab")
    face, side = lax.rem(box, 2), lax.rem(slab, 2)
    for out, last in ((ca, side == 0), (cb, side == 1)):
        for m in range(members):
            lo, hi = m * width_z, (m + 1) * width_z - 1
            a = jnp.where(last, xa[hi : hi + 1], xa[lo : lo + 1])
            b = jnp.where(last, xb[hi : hi + 1], xb[lo : lo + 1])
            out[2 * m : 2 * m + 1] = jnp.where(face == 0, b, a)
            out[2 * m + 1 : 2 * m + 2] = jnp.where(face == 0, a, b)


def split_cell(cell, total_z, depth_y):
    plane = total_z * depth_y
    x = cell // plane
    rest = cell - x * plane
    z = rest // depth_y
    return x, z, rest - z * depth_y


def one_hot(index, high):
    rows = rows_of((high, index.shape[1]), 0)
    return jnp.where(rows == index, 1.0, 0.0).astype(BF16)


def faces_of(boxes, slabs, box, slab):
    return jnp.where(box == 0, 0, 1), jnp.where(slab == 0, 2, 3)


def local_kernel(boxes, slabs, total_z, planes, cells, now, prev, cour, local, wide, narrow):
    members, width_x, width_z, depth_y = now.shape
    box, slab = lax.axis_index("box"), lax.axis_index("slab")
    zero = jnp.zeros((1, depth_y), F32)
    for x in range(width_x):
        for m in range(members):
            here = now[m, x]
            around = beside_y(here) + beside_rows(here, zero, zero)
            if x > 0:
                around = around + now[m, x - 1]
            if x < width_x - 1:
                around = around + now[m, x + 1]
            coef = cour[x] * planes[m]
            local[m, x] = 2.0 * here - prev[m, x] + coef * (around - 6.0 * here)
    for i, f in enumerate(faces_of(boxes, slabs, box, slab)):
        _, _, y = split_cell(cells[pl.ds(f, 1), :], total_z, depth_y)
        wide[i] = one_hot(y, depth_y)
    for i, f in enumerate((4, 5)):
        x, _, _ = split_cell(cells[f : f + 1, :], total_z, depth_y)
        narrow[i] = one_hot(extended_row(x, box * width_x, width_x), narrow.shape[1])


def extended_row(coordinate, start, width):
    d = coordinate - start
    edge = jnp.where(d == -1, width, jnp.where(d == width, width + 1, -1))
    return jnp.where((d >= 0) & (d < width), d, edge)


def three_parts(v):
    first = v.astype(BF16)
    rest = v - first.astype(F32)
    second = rest.astype(BF16)
    third = (rest - second.astype(F32)).astype(BF16)
    return first, second, third


def contract(lhs, rhs):
    return lax.dot_general(lhs, rhs, (((1,), (1,)), ((), ())), preferred_element_type=F32)


def face_source(values, row_index, rhs, high):
    hit = rows_of((high, row_index.shape[1]), 0) == row_index
    parts = []
    for v in values:
        for part in three_parts(v):
            parts.append(jnp.where(hit, part.astype(F32), 0.0).astype(BF16))
    out = contract(jnp.concatenate(parts, axis=0), rhs)
    sums = []
    for t in range(len(values)):
        one, two, three = (out[(3 * t + i) * high : (3 * t + i + 1) * high] for i in range(3))
        sums.append((three + two) + one)
    return sums


def first_kernel(
    boxes, slabs, total_z, received, planes, edges, cells, wide, narrow, now, local, cour,
    vals, za, zb, xa, xb, *rest,
):
    others, rest = rest[:received], rest[received:]
    one, hx, hz, src, xlo, xhi, zlo, zhi, value, xsrc, zsrc = rest
    members, width_x, width_z, depth_y = now.shape
    box, slab = lax.axis_index("box"), lax.axis_index("slab")
    start_x, start_z = box * width_x, slab * width_z
    face, side = lax.rem(box, 2), lax.rem(slab, 2)
    span_z = (2 * members + 1) * width_x
    low, high = (box > 0, slab > 0), (box < boxes - 1, slab < slabs - 1)
    xlo[...] = jnp.where(low[0], jnp.where(face == 0, xb[...], xa[...]), 0.0)
    xhi[...] = jnp.where(high[0], jnp.where(face == 0, xa[...], xb[...]), 0.0)
    zlo[...] = jnp.where(low[1], jnp.where(side == 0, zb[:span_z], za[:span_z]), 0.0)
    zhi[...] = jnp.where(high[1], jnp.where(side == 0, za[:span_z], zb[:span_z]), 0.0)
    total = vals[...] + za[span_z:]
    if slabs == 4:
        total = total + zb[span_z:]
    for other in others:
        total = total + other[...]
    value[...] = total

    faces = cells.shape[0]
    steps = xsrc.shape[0]
    chunks = value.shape[0] // steps
    per = chunks // faces

    def of_face(f):
        x, z, _ = split_cell(cells[pl.ds(f, 1), :], total_z, depth_y)
        vs = []
        for t in range(steps):
            pieces = [value[pl.ds(t * chunks + f * per + i, 1), :] for i in range(per)]
            vs.append(jnp.concatenate(pieces, axis=1))
        return extended_row(x, start_x, width_x), extended_row(z, start_z, width_z), vs

    on_x = (box == 0) | (box == boxes - 1)
    on_z = (slab == 0) | (slab == slabs - 1)
    face_x, face_z = faces_of(boxes, slabs, box, slab)
    _, at, vs = of_face(face_x)
    for t, s in enumerate(face_source(vs, jnp.where(on_x, at, -1), wide[0], xsrc.shape[1])):
        xsrc[t] = s
    at, _, vs = of_face(face_z)
    for t, s in enumerate(face_source(vs, jnp.where(on_z, at, -1), wide[1], zsrc.shape[1])):
        zsrc[t] = s
    ys = []
    for i, f in enumerate((4, 5)):
        _, at, vs = of_face(f)
        ys.append(face_source(vs, at, narrow[i], xsrc.shape[1]))

    lane = rows_of((width_z, depth_y), 1)
    row = rows_of((width_z, depth_y), 0)
    row_of_z = jnp.where(slab == 0, 0, jnp.where(slab == slabs - 1, width_z - 1, -1))
    row_of_x = jnp.where(box == 0, 0, jnp.where(box == boxes - 1, width_x - 1, -1))

    def plane_source(t, x):
        lo, hi = (y[t][:width_z, x : x + 1] for y in ys)
        out = jnp.where(lane == 0, lo, jnp.where(lane == depth_y - 1, hi, 0.0))
        out = out + jnp.where(row == row_of_z, zsrc[t, x : x + 1, :], 0.0)
        if x in (0, width_x - 1):
            out = out + jnp.where(row_of_x == x, xsrc[t, :width_z, :], 0.0)
        return out

    lane_x = rows_of((width_x, depth_y), 1)
    row_x = rows_of((width_x, depth_y), 0)
    turned = [jnp.transpose(y[0]) for y in ys]

    def row_source(z):
        lo, hi = (y[:width_x, z : z + 1] for y in turned)
        out = jnp.where(lane_x == 0, lo, jnp.where(lane_x == depth_y - 1, hi, 0.0))
        return out + jnp.where(row_x == row_of_x, xsrc[0, z : z + 1, :], 0.0)

    for s, (ref, x) in enumerate(((xlo, 0), (xhi, width_x - 1))):
        source = plane_source(0, width_x + s)
        for m in range(members):
            coef = ref[2 * members * width_z :] * planes[m]
            base = ref[(members + m) * width_z : (members + m + 1) * width_z]
            hx[s, m] = base + coef * now[m, x] + source
    for s, (ref, z) in enumerate(((zlo, 0), (zhi, width_z - 1))):
        source = row_source(width_z + s)
        for m in range(members):
            coef = ref[2 * members * width_x :] * edges[2 * m + s : 2 * m + s + 1]
            base = ref[(members + m) * width_x : (members + m + 1) * width_x]
            hz[s, m] = base + coef * now[m, :, z] + source
    for x in range(width_x):
        source = plane_source(0, x)
        src[x] = plane_source(1, x)
        for m in range(members):
            at = m * width_x + x
            more = jnp.where(row == 0, zlo[at : at + 1], 0.0)
            more = jnp.where(row == width_z - 1, zhi[at : at + 1], more)
            if x == 0:
                more = more + xlo[m * width_z : (m + 1) * width_z]
            if x == width_x - 1:
                more = more + xhi[m * width_z : (m + 1) * width_z]
            one[m, x] = local[m, x] + (cour[x] * planes[m]) * more + source


def second_kernel(
    boxes, slabs, planes, edges, now, one, cour, src, hx, hz, za, zb, xa, xb, ca, cb,
    out, last, nxt, sems,
):
    members, width_x, width_z, depth_y = now.shape
    box, slab = lax.axis_index("box"), lax.axis_index("slab")
    face, side = lax.rem(box, 2), lax.rem(slab, 2)
    open_x, open_z = (box > 0, box < boxes - 1), (slab > 0, slab < slabs - 1)
    row = rows_of((width_z, depth_y), 0)
    row_x = rows_of((width_x, depth_y), 0)
    tail_x, tail_z = 2 * members * width_z, 2 * members * width_x
    cour_x = [
        jnp.where(face == s, xb[tail_x : tail_x + width_z], xa[tail_x : tail_x + width_z])
        for s in (0, 1)
    ]
    cour_z = [
        jnp.where(side == s, zb[tail_z : tail_z + width_x], za[tail_z : tail_z + width_x])
        for s in (0, 1)
    ]

    def corner(m, sx, sz):
        at = 2 * m + sx
        got = jnp.where(side == sz, cb[at : at + 1], ca[at : at + 1])
        return jnp.where(open_x[sx] & open_z[sz], got, 0.0)

    copies = [pltpu.make_async_copy(one, last, sems.at[0])]
    copies[0].start()
    for m in range(members):
        corners = [[corner(m, sx, sz) for sz in (0, 1)] for sx in (0, 1)]
        halo_x, halo_z = [], []
        for s in (0, 1):
            d = jnp.where(row == 0, corners[s][0], 0.0)
            d = jnp.where(row == width_z - 1, corners[s][1], d)
            halo_x.append(hx[s, m] + cour_x[s] * planes[m] * d)
            d = jnp.where(row_x == 0, corners[0][s], 0.0)
            d = jnp.where(row_x == width_x - 1, corners[1][s], d)
            hz[s, m] = hz[s, m] + cour_z[s] * edges[2 * m + s : 2 * m + s + 1] * d
        for x in range(width_x):
            here = one[m, x]
            around = beside_rows(here, hz[0, m, x : x + 1], hz[1, m, x : x + 1]) + beside_y(here)
            around = around + (one[m, x - 1] if x > 0 else halo_x[0])
            around = around + (one[m, x + 1] if x < width_x - 1 else halo_x[1])
            coef = cour[x] * planes[m]
            nxt[m, x] = 2.0 * here - now[m, x] + coef * (around - 6.0 * here) + src[x]
            if x % 4 == 3:
                part = (m, pl.ds(x - 3, 4))
                copies.append(
                    pltpu.make_async_copy(nxt.at[part], out.at[part], sems.at[len(copies)])
                )
                copies[-1].start()
    for copy in copies:
        copy.wait()


def pairs_even(n):
    return [i ^ 1 for i in range(n)]


def pairs_odd(n):
    return [(i + 1) % n if i % 2 else (i - 1) % n for i in range(n)]


def on_device(
    boxes, slabs, pressure_now, pressure_prev, courant_sq, member_profiles, member_ids,
    stored_slabs, slab_home, interp_weights, surface_cells,
):
    members, width_x, width_z, depth_y = pressure_now.shape
    slots, samples, points = stored_slabs.shape
    steps = interp_weights.shape[0]
    total_z = width_z * slabs
    value_rows = steps * points // depth_y
    span_x = (2 * members + 1) * width_z
    span_z = (2 * members + 1) * width_x

    def shape(*dims):
        return jax.ShapeDtypeStruct(dims, F32)

    def inner(*dims):
        return pltpu.VMEM(dims, F32)

    def far(*arrays):
        return [pltpu.with_memory_space_constraint(a, pltpu.HBM) for a in arrays]

    def near(*arrays):
        return [pltpu.with_memory_space_constraint(a, pltpu.VMEM) for a in arrays]

    whole = pressure_now.shape
    now, prev, cour, cells, planes, edges, za, zb, vals, xa, xb = pl.pallas_call(
        functools.partial(pack_kernel, slots),
        out_shape=(
            inner(*whole),
            inner(*whole),
            inner(*courant_sq.shape),
            pltpu.VMEM(surface_cells.shape, jnp.int32),
            inner(members, width_z, depth_y),
            inner(2 * members, depth_y),
            inner(span_z + value_rows, depth_y),
            inner(span_z + value_rows, depth_y),
            inner(value_rows, depth_y),
            inner(span_x, depth_y),
            inner(span_x, depth_y),
        ),
        in_specs=[SMEM] + [HBM] * 8,
        out_specs=(VMEM,) * 11,
        scratch_shapes=[
            pltpu.SMEM(member_ids.shape, jnp.int32),
            pltpu.SMEM(interp_weights.shape, F32),
            pltpu.SMEM(member_profiles.shape, F32),
            pltpu.VMEM((samples, points), F32),
            pltpu.SemaphoreType.DMA((8,)),
        ],
        compiler_params=PARAMS,
        name="pack",
    )(
        slab_home, *far(member_ids, interp_weights, member_profiles),
        *far(pressure_now, pressure_prev, courant_sq, surface_cells, stored_slabs),
    )

    def over_slab(x, partner):
        return lax.ppermute(x, "slab", list(enumerate(partner)))

    def over_box(x, odd):
        pairs = []
        for b in range(boxes):
            other = b ^ 1
            if odd:
                other = b + 1 if b % 2 else b - 1
            for s in range(slabs):
                inside = 0 <= other < boxes
                to = other * slabs + s if inside else b * slabs + (s ^ 1)
                pairs.append((b * slabs + s, to))
        return lax.ppermute(x, ("box", "slab"), pairs)

    high_x, high_z = (width_x + 2 + 15) // 16 * 16, (width_z + 2 + 15) // 16 * 16
    per_face = surface_cells.shape[1]
    za = over_slab(za, pairs_even(slabs))
    zb = over_slab(zb, pairs_odd(slabs))
    xa, xb = over_box(xa, False), over_box(xb, True)
    others = [
        over_slab(vals, [i ^ k for i in range(slabs)])
        for k in range(2, slabs)
        if slabs != 4 or k != 3
    ]
    now, prev, cour, cells, vals, planes, edges = near(now, prev, cour, cells, vals, planes, edges)
    local, wide, narrow = pl.pallas_call(
        functools.partial(local_kernel, boxes, slabs, total_z),
        out_shape=(
            inner(*whole),
            pltpu.VMEM((2, depth_y, per_face), BF16),
            pltpu.VMEM((2, 128, per_face), BF16),
        ),
        in_specs=[VMEM] * 5,
        out_specs=(VMEM,) * 3,
        compiler_params=PARAMS,
        name="local",
    )(planes, cells, now, prev, cour)
    local, wide, narrow = near(local, wide, narrow)
    za, zb, xa, xb, *others = near(za, zb, xa, xb, *others)
    ca, cb = pl.pallas_call(
        functools.partial(corner_kernel, members, width_z),
        out_shape=(inner(2 * members, depth_y),) * 2,
        in_specs=[VMEM, VMEM, VMEM],
        out_specs=(VMEM, VMEM),
        compiler_params=PARAMS,
        name="corner",
    )(xa, xb, local)
    ca, cb = over_slab(ca, pairs_even(slabs)), over_slab(cb, pairs_odd(slabs))

    one, hx, hz, src = pl.pallas_call(
        functools.partial(first_kernel, boxes, slabs, total_z, len(others)),
        out_shape=(
            inner(*whole),
            inner(2, members, width_z, depth_y),
            inner(2, members, width_x, depth_y),
            inner(*courant_sq.shape),
        ),
        in_specs=[VMEM] * (13 + len(others)),
        out_specs=(VMEM,) * 4,
        scratch_shapes=[
            pltpu.VMEM((span_x, depth_y), F32),
            pltpu.VMEM((span_x, depth_y), F32),
            pltpu.VMEM((span_z, depth_y), F32),
            pltpu.VMEM((span_z, depth_y), F32),
            pltpu.VMEM((value_rows, depth_y), F32),
            pltpu.VMEM((steps, high_z, depth_y), F32),
            pltpu.VMEM((steps, high_x, depth_y), F32),
        ],
        compiler_params=PARAMS,
        name="first",
    )(
        planes, edges, cells, wide, narrow, now, local, cour,
        vals, za, zb, xa, xb, *others,
    )
    return pl.pallas_call(
        functools.partial(second_kernel, boxes, slabs),
        out_shape=(pltpu.HBM(whole, F32),) * 2,
        in_specs=[VMEM] * 14,
        out_specs=(HBM, HBM),
        scratch_shapes=[
            pltpu.VMEM(whole, F32),
            pltpu.SemaphoreType.DMA((1 + members * width_x // 4,)),
        ],
        compiler_params=PARAMS,
        name="second",
    )(
        planes, edges, now, *near(one), cour, *near(src, hx, hz),
        za, zb, xa, xb, *near(ca, cb),
    )


def solution(mesh):
    in_specs = (
        P("ens", "box", "slab", None),
        P("ens", "box", "slab", None),
        P("box", "slab", None),
        P(),
        P("ens"),
        P("slab", None, None),
        P("ens"),
        P(),
        P(),
    )
    out_specs = (P("ens", "box", "slab", None), P("ens", "box", "slab", None))
    boxes, slabs = mesh.shape["box"], mesh.shape["slab"]
    return jax.shard_map(
        functools.partial(on_device, boxes, slabs),
        mesh=mesh,
        in_specs=in_specs,
        out_specs=out_specs,
        check_vma=False,
    )
```

```python
import functools

import jax
import jax.numpy as jnp
from jax import lax
from jax.experimental import pallas as pl
from jax.experimental.pallas import tpu as pltpu
from jax.sharding import PartitionSpec as P


F32 = jnp.float32
BF16 = jnp.bfloat16
VMEM = pl.BlockSpec(memory_space=pltpu.VMEM)
SMEM = pl.BlockSpec(memory_space=pltpu.SMEM)
HBM = pl.BlockSpec(memory_space=pl.ANY)
CORNERS = 8
PARAMS = pltpu.CompilerParams(vmem_limit_bytes=16 * 1024 * 1024)


def rows_of(shape, axis):
    return lax.broadcasted_iota(jnp.int32, shape, axis)


def beside_y(v):
    length = v.shape[1]
    lane = rows_of(v.shape, 1)
    left = jnp.where(lane == 0, 0.0, pltpu.roll(v, 1, 1))
    right = jnp.where(lane == length - 1, 0.0, pltpu.roll(v, length - 1, 1))
    return left + right


def beside_rows(v, low, high):
    length = v.shape[0]
    row = rows_of(v.shape, 0)
    down = jnp.where(row == 0, low, pltpu.roll(v, 1, 0))
    up = jnp.where(row == length - 1, high, pltpu.roll(v, length - 1, 0))
    return down + up


def pack_kernel(
    slots, home, ids_in, weights_in, prof_in, now_in, prev_in, cour_in, cells_in, slabs,
    now, prev, cour, cells, planes, edges, za, zb, vals, xa, xb, ids, weights, prof, block, sems,
):
    members, width_x, width_z, depth_y = now.shape
    steps, samples = weights.shape
    box, slab = lax.axis_index("box"), lax.axis_index("slab")
    total_z = prof.shape[1]
    loads = [
        pltpu.make_async_copy(source, target, sems.at[i])
        for i, (source, target) in enumerate((
            (ids_in, ids),
            (prof_in, prof),
            (weights_in, weights),
            (now_in, now),
            (cour_in, cour),
            (prev_in, prev),
            (slabs.at[lax.rem(home[0], slots)], block),
            (cells_in, cells),
        ))
    ]
    for load in loads:
        load.start()
    start_z = slab * width_z
    for load in loads[:3]:
        load.wait()
    row = rows_of((width_z, depth_y), 0)
    for m in range(members):
        plane = jnp.zeros((width_z, depth_y), F32)
        for z in range(width_z):
            plane = jnp.where(row == z, 1.0 + prof[ids[m], start_z + z], plane)
        planes[m] = plane
        for s, z in ((0, start_z - 1), (1, start_z + width_z)):
            beyond = 1.0 + prof[ids[m], jnp.clip(z, 0, total_z - 1)]
            edges[2 * m + s : 2 * m + s + 1] = jnp.full((1, depth_y), beyond, F32)
    zero = jnp.zeros((1, depth_y), F32)
    for load in loads[3:6]:
        load.wait()
    face, side = lax.rem(box, 2), lax.rem(slab, 2)
    xs = []
    for x, inner in ((0, 1), (width_x - 1, width_x - 2)):
        rows = []
        for m in range(members):
            here = now[m, x]
            around = beside_y(here) + beside_rows(here, zero, zero) + now[m, inner]
            coef = cour[x] * planes[m]
            rows.append((here, 2.0 * here - prev[m, x] + coef * (around - 6.0 * here)))
        xs.append([r[0] for r in rows] + [r[1] for r in rows] + [cour[x]])
    for i, (low, high) in enumerate(zip(*xs)):
        at = slice(i * width_z, (i + 1) * width_z)
        xa[at] = jnp.where(face == 0, high, low)
        xb[at] = jnp.where(face == 1, high, low)
    zs = []
    for z, inner in ((0, 1), (width_z - 1, width_z - 2)):
        rows = []
        for m in range(members):
            here = now[m, :, z]
            around = beside_y(here) + beside_rows(here, zero, zero) + now[m, :, inner]
            coef = cour[:, z] * (1.0 + prof[ids[m], start_z + z])
            rows.append((here, 2.0 * here - prev[m, :, z] + coef * (around - 6.0 * here)))
        zs.append([r[0] for r in rows] + [r[1] for r in rows] + [cour[:, z]])
    for i, (low, high) in enumerate(zip(*zs)):
        at = slice(i * width_x, (i + 1) * width_x)
        za[at] = jnp.where(side == 0, high, low)
        zb[at] = jnp.where(side == 1, high, low)
    owner = slab == home[0] // slots
    points = block.shape[1]
    chunks = points // depth_y
    sample = rows_of((samples, depth_y), 0)
    columns = []
    for t in range(steps):
        column = jnp.zeros((samples, depth_y), F32)
        for k in range(samples):
            column = jnp.where(sample == k, weights[t, k], column)
        columns.append(jnp.where(owner, column, 0.0))
    loads[6].wait()
    for c in range(chunks):
        piece = block[:, c * depth_y : (c + 1) * depth_y]
        for t in range(steps):
            at = t * chunks + c
            vals[at : at + 1] = jnp.sum(columns[t] * piece, axis=0, keepdims=True)
    tail = (2 * members + 1) * width_x
    loads[7].wait()
    offered = vals[...]
    za[tail:] = offered
    zb[tail:] = offered


def corner_kernel(members, width_z, relay, xa, xb, zb, after, ca, cb):
    box, slab = lax.axis_index("box"), lax.axis_index("slab")
    face, side = lax.rem(box, 2), lax.rem(slab, 2)
    for out, last in ((ca, side == 0), (cb, side == 1)):
        for m in range(members):
            lo, hi = m * width_z, (m + 1) * width_z - 1
            a = jnp.where(last, xa[hi : hi + 1], xa[lo : lo + 1])
            b = jnp.where(last, xb[hi : hi + 1], xb[lo : lo + 1])
            out[2 * m : 2 * m + 1] = jnp.where(face == 0, b, a)
            out[2 * m + 1 : 2 * m + 2] = jnp.where(face == 0, a, b)
    if relay:
        ca[CORNERS:] = zb[zb.shape[0] - relay :]


def split_cell(cell, total_z, depth_y):
    plane = total_z * depth_y
    x = cell // plane
    rest = cell - x * plane
    z = rest // depth_y
    return x, z, rest - z * depth_y


def one_hot(index, high):
    rows = rows_of((high, index.shape[1]), 0)
    return jnp.where(rows == index, 1.0, 0.0).astype(BF16)


def faces_of(boxes, slabs, box, slab):
    return jnp.where(box == 0, 0, 1), jnp.where(slab == 0, 2, 3)


def local_kernel(boxes, slabs, total_z, planes, cells, now, prev, cour, local, wide, narrow):
    members, width_x, width_z, depth_y = now.shape
    box, slab = lax.axis_index("box"), lax.axis_index("slab")
    zero = jnp.zeros((1, depth_y), F32)
    for x in range(width_x):
        for m in range(members):
            here = now[m, x]
            around = beside_y(here) + beside_rows(here, zero, zero)
            if x > 0:
                around = around + now[m, x - 1]
            if x < width_x - 1:
                around = around + now[m, x + 1]
            coef = cour[x] * planes[m]
            local[m, x] = 2.0 * here - prev[m, x] + coef * (around - 6.0 * here)
    for i, f in enumerate(faces_of(boxes, slabs, box, slab)):
        _, _, y = split_cell(cells[pl.ds(f, 1), :], total_z, depth_y)
        wide[i] = one_hot(y, depth_y)
    for i, f in enumerate((4, 5)):
        x, _, _ = split_cell(cells[f : f + 1, :], total_z, depth_y)
        narrow[i] = one_hot(extended_row(x, box * width_x, width_x), narrow.shape[1])


def extended_row(coordinate, start, width):
    d = coordinate - start
    edge = jnp.where(d == -1, width, jnp.where(d == width, width + 1, -1))
    return jnp.where((d >= 0) & (d < width), d, edge)


def three_parts(v):
    first = v.astype(BF16)
    rest = v - first.astype(F32)
    second = rest.astype(BF16)
    third = (rest - second.astype(F32)).astype(BF16)
    return first, second, third


def contract(lhs, rhs):
    return lax.dot_general(lhs, rhs, (((1,), (1,)), ((), ())), preferred_element_type=F32)


def face_source(values, row_index, rhs, high):
    hit = rows_of((high, row_index.shape[1]), 0) == row_index
    parts = []
    for v in values:
        for part in three_parts(v):
            parts.append(jnp.where(hit, part.astype(F32), 0.0).astype(BF16))
    out = contract(jnp.concatenate(parts, axis=0), rhs)
    sums = []
    for t in range(len(values)):
        one, two, three = (out[(3 * t + i) * high : (3 * t + i + 1) * high] for i in range(3))
        sums.append((three + two) + one)
    return sums


def main_kernel(
    boxes, slabs, total_z, received, planes, edges, cells, wide, narrow, now, local, cour,
    vals, za, zb, xa, xb, ca, *rest,
):
    others, rest = rest[:received], rest[received:]
    out, last, ends, late, one, nxt, hz, src, xlo, xhi, zlo, zhi, value, xsrc, zsrc, sems = rest
    members, width_x, width_z, depth_y = now.shape
    box, slab = lax.axis_index("box"), lax.axis_index("slab")
    start_x, start_z = box * width_x, slab * width_z
    face, side = lax.rem(box, 2), lax.rem(slab, 2)
    span_z = (2 * members + 1) * width_x
    low, high = (box > 0, slab > 0), (box < boxes - 1, slab < slabs - 1)
    xlo[...] = jnp.where(low[0], jnp.where(face == 0, xb[...], xa[...]), 0.0)
    xhi[...] = jnp.where(high[0], jnp.where(face == 0, xa[...], xb[...]), 0.0)
    zlo[...] = jnp.where(low[1], jnp.where(side == 0, zb[:span_z], za[:span_z]), 0.0)
    zhi[...] = jnp.where(high[1], jnp.where(side == 0, za[:span_z], zb[:span_z]), 0.0)
    total = vals[...] + za[span_z:]
    if slabs == 4:
        total = total + (zb[span_z:] + ca[CORNERS:])
    for other in others:
        total = total + other[...]
    value[...] = total

    faces = cells.shape[0]
    steps = xsrc.shape[0]
    chunks = value.shape[0] // steps
    per = chunks // faces

    def of_face(f):
        x, z, _ = split_cell(cells[pl.ds(f, 1), :], total_z, depth_y)
        vs = []
        for t in range(steps):
            pieces = [value[pl.ds(t * chunks + f * per + i, 1), :] for i in range(per)]
            vs.append(jnp.concatenate(pieces, axis=1))
        return extended_row(x, start_x, width_x), extended_row(z, start_z, width_z), vs

    on_x = (box == 0) | (box == boxes - 1)
    on_z = (slab == 0) | (slab == slabs - 1)
    face_x, face_z = faces_of(boxes, slabs, box, slab)
    _, at, vs = of_face(face_x)
    for t, s in enumerate(face_source(vs, jnp.where(on_x, at, -1), wide[0], xsrc.shape[1])):
        xsrc[t] = s
    at, _, vs = of_face(face_z)
    for t, s in enumerate(face_source(vs, jnp.where(on_z, at, -1), wide[1], zsrc.shape[1])):
        zsrc[t] = s
    ys = []
    for i, f in enumerate((4, 5)):
        _, at, vs = of_face(f)
        ys.append(face_source(vs, at, narrow[i], xsrc.shape[1]))

    lane = rows_of((width_z, depth_y), 1)
    row = rows_of((width_z, depth_y), 0)
    row_of_z = jnp.where(slab == 0, 0, jnp.where(slab == slabs - 1, width_z - 1, -1))
    row_of_x = jnp.where(box == 0, 0, jnp.where(box == boxes - 1, width_x - 1, -1))

    def plane_source(t, x):
        lo, hi = (y[t][:width_z, x : x + 1] for y in ys)
        out = jnp.where(lane == 0, lo, jnp.where(lane == depth_y - 1, hi, 0.0))
        out = out + jnp.where(row == row_of_z, zsrc[t, x : x + 1, :], 0.0)
        if x in (0, width_x - 1):
            out = out + jnp.where(row_of_x == x, xsrc[t, :width_z, :], 0.0)
        return out

    lane_x = rows_of((width_x, depth_y), 1)
    row_x = rows_of((width_x, depth_y), 0)
    turned = [jnp.transpose(y[0]) for y in ys]

    def row_source(z):
        lo, hi = (y[:width_x, z : z + 1] for y in turned)
        out = jnp.where(lane_x == 0, lo, jnp.where(lane_x == depth_y - 1, hi, 0.0))
        return out + jnp.where(row_x == row_of_x, xsrc[0, z : z + 1, :], 0.0)

    open_x = (low[0], high[0])
    open_a = jnp.where(side == 0, high[1], low[1])
    row_a = jnp.where(side == 0, width_z - 1, 0)
    side_x, side_z = 2 * members * width_z, 2 * members * width_x

    def corner(m, sx):
        return jnp.where(open_x[sx] & open_a, ca[2 * m + sx : 2 * m + sx + 1], 0.0)

    halo_x = [[], []]
    coef_x = [[], []]
    for s, (ref, x) in enumerate(((xlo, 0), (xhi, width_x - 1))):
        source = plane_source(0, width_x + s)
        for m in range(members):
            coef = ref[side_x:] * planes[m]
            base = ref[(members + m) * width_z : (members + m + 1) * width_z]
            own = now[m, x] + jnp.where(row == row_a, corner(m, s), 0.0)
            halo_x[s].append(base + coef * own + source)
            coef_x[s].append(coef)
    coef_z = [[], []]
    for s, (ref, z) in enumerate(((zlo, 0), (zhi, width_z - 1))):
        source = row_source(width_z + s)
        for m in range(members):
            coef = ref[side_z:] * edges[2 * m + s : 2 * m + s + 1]
            base = ref[(members + m) * width_x : (members + m + 1) * width_x]
            more = jnp.where(row_x == 0, corner(m, 0), 0.0)
            more = jnp.where(row_x == width_x - 1, corner(m, 1), more)
            own = now[m, :, z] + jnp.where(side == 1 - s, more, 0.0)
            hz[s, m] = base + coef * own + source
            coef_z[s].append(coef)
    copies = []

    def send(scratch, target, m, first, count):
        part = (m, pl.ds(first, count))
        copies.append(pltpu.make_async_copy(scratch.at[part], target.at[part], sems.at[len(copies)]))
        copies[-1].start()

    for m in range(members):
        for x in range(width_x):
            if m == 0:
                src[0, x] = plane_source(0, x)
                src[1, x] = plane_source(1, x)
            at = m * width_x + x
            more = jnp.where(row == 0, zlo[at : at + 1], 0.0)
            more = jnp.where(row == width_z - 1, zhi[at : at + 1], more)
            if x == 0:
                more = more + xlo[m * width_z : (m + 1) * width_z]
            if x == width_x - 1:
                more = more + xhi[m * width_z : (m + 1) * width_z]
            one[m, x] = local[m, x] + (cour[x] * planes[m]) * more + src[0, x]
        send(one, last, m, 0, width_x)
        for x in range(width_x):
            here = one[m, x]
            around = beside_rows(here, hz[0, m, x : x + 1], hz[1, m, x : x + 1]) + beside_y(here)
            around = around + (one[m, x - 1] if x > 0 else halo_x[0][m])
            around = around + (one[m, x + 1] if x < width_x - 1 else halo_x[1][m])
            coef = cour[x] * planes[m]
            value_here = 2.0 * here - now[m, x] + coef * (around - 6.0 * here) + src[1, x]
            if x in (0, width_x - 1):
                s = 0 if x == 0 else 1
                ends[s, m] = value_here
                rows = []
                for z in (width_z - 1, 0):
                    beyond = coef_z[0 if z == 0 else 1][m][x : x + 1]
                    rows.append(coef[z : z + 1] * (beyond + coef_x[s][m][z : z + 1]))
                late[2 * m + s : 2 * m + s + 1] = jnp.where(side == 0, rows[1], rows[0])
            else:
                nxt[m, x] = value_here
        send(nxt, out, m, 1, width_x - 2)
    for copy in copies:
        copy.wait()


def fix_kernel(boxes, slabs, cb, ends, late, out_in, out, done, sems):
    _, members, width_z, depth_y = ends.shape
    width_x = out.shape[1]
    box, slab = lax.axis_index("box"), lax.axis_index("slab")
    side = lax.rem(slab, 2)
    open_x = (box > 0, box < boxes - 1)
    open_b = jnp.where(side == 0, slab > 0, slab < slabs - 1)
    row = rows_of((width_z, depth_y), 0)
    row_b = jnp.where(side == 0, 0, width_z - 1)
    copies = []
    for m in range(members):
        for s, x in ((0, 0), (1, width_x - 1)):
            at = 2 * m + s
            got = jnp.where(open_x[s] & open_b, cb[at : at + 1], 0.0)
            done[s, m] = ends[s, m] + jnp.where(row == row_b, late[at : at + 1] * got, 0.0)
            copies.append(pltpu.make_async_copy(done.at[s, m], out.at[m, x], sems.at[at]))
            copies[-1].start()
    for copy in copies:
        copy.wait()


def pairs_even(n):
    return [i ^ 1 for i in range(n)]


def pairs_odd(n):
    return [(i + 1) % n if i % 2 else (i - 1) % n for i in range(n)]


def on_device(
    boxes, slabs, pressure_now, pressure_prev, courant_sq, member_profiles, member_ids,
    stored_slabs, slab_home, interp_weights, surface_cells,
):
    members, width_x, width_z, depth_y = pressure_now.shape
    slots, samples, points = stored_slabs.shape
    steps = interp_weights.shape[0]
    total_z = width_z * slabs
    value_rows = steps * points // depth_y
    span_x = (2 * members + 1) * width_z
    span_z = (2 * members + 1) * width_x

    def shape(*dims):
        return jax.ShapeDtypeStruct(dims, F32)

    def inner(*dims):
        return pltpu.VMEM(dims, F32)

    def far(*arrays):
        return [pltpu.with_memory_space_constraint(a, pltpu.HBM) for a in arrays]

    def near(*arrays):
        return [pltpu.with_memory_space_constraint(a, pltpu.VMEM) for a in arrays]

    whole = pressure_now.shape
    now, prev, cour, cells, planes, edges, za, zb, vals, xa, xb = pl.pallas_call(
        functools.partial(pack_kernel, slots),
        out_shape=(
            inner(*whole),
            inner(*whole),
            inner(*courant_sq.shape),
            pltpu.VMEM(surface_cells.shape, jnp.int32),
            inner(members, width_z, depth_y),
            inner(2 * members, depth_y),
            inner(span_z + value_rows, depth_y),
            inner(span_z + value_rows, depth_y),
            inner(value_rows, depth_y),
            inner(span_x, depth_y),
            inner(span_x, depth_y),
        ),
        in_specs=[SMEM] + [HBM] * 8,
        out_specs=(VMEM,) * 11,
        scratch_shapes=[
            pltpu.SMEM(member_ids.shape, jnp.int32),
            pltpu.SMEM(interp_weights.shape, F32),
            pltpu.SMEM(member_profiles.shape, F32),
            pltpu.VMEM((samples, points), F32),
            pltpu.SemaphoreType.DMA((8,)),
        ],
        compiler_params=PARAMS,
        name="pack",
    )(
        slab_home, *far(member_ids, interp_weights, member_profiles),
        *far(pressure_now, pressure_prev, courant_sq, surface_cells, stored_slabs),
    )

    def over_slab(x, partner):
        return lax.ppermute(x, "slab", list(enumerate(partner)))

    def over_box(x, odd):
        pairs = []
        for b in range(boxes):
            other = b ^ 1
            if odd:
                other = b + 1 if b % 2 else b - 1
            for s in range(slabs):
                inside = 0 <= other < boxes
                to = other * slabs + s if inside else b * slabs + (s ^ 1)
                pairs.append((b * slabs + s, to))
        return lax.ppermute(x, ("box", "slab"), pairs)

    high_x, high_z = (width_x + 2 + 15) // 16 * 16, (width_z + 2 + 15) // 16 * 16
    per_face = surface_cells.shape[1]
    za = over_slab(za, pairs_even(slabs))
    zb = over_slab(zb, pairs_odd(slabs))
    xa, xb = over_box(xa, False), over_box(xb, True)
    others = [
        over_slab(vals, [i ^ k for i in range(slabs)])
        for k in range(2, slabs)
        if slabs != 4
    ]
    now, prev, cour, cells, vals, planes, edges = near(now, prev, cour, cells, vals, planes, edges)
    local, wide, narrow = pl.pallas_call(
        functools.partial(local_kernel, boxes, slabs, total_z),
        out_shape=(
            inner(*whole),
            pltpu.VMEM((2, depth_y, per_face), BF16),
            pltpu.VMEM((2, 128, per_face), BF16),
        ),
        in_specs=[VMEM] * 5,
        out_specs=(VMEM,) * 3,
        compiler_params=PARAMS,
        name="local",
    )(planes, cells, now, prev, cour)
    local, wide, narrow = near(local, wide, narrow)
    za, zb, xa, xb, *others = near(za, zb, xa, xb, *others)
    relay = value_rows if slabs == 4 else 0
    ca, cb = pl.pallas_call(
        functools.partial(corner_kernel, members, width_z, relay),
        out_shape=(inner(CORNERS + relay, depth_y), inner(CORNERS, depth_y)),
        in_specs=[VMEM] * 4,
        out_specs=(VMEM, VMEM),
        compiler_params=PARAMS,
        name="corner",
    )(xa, xb, zb, local)
    ca, cb = near(over_slab(ca, pairs_even(slabs)), over_slab(cb, pairs_odd(slabs)))

    out, last, ends, late = pl.pallas_call(
        functools.partial(main_kernel, boxes, slabs, total_z, len(others)),
        out_shape=(
            pltpu.HBM(whole, F32),
            pltpu.HBM(whole, F32),
            inner(2, members, width_z, depth_y),
            inner(2 * members, depth_y),
        ),
        in_specs=[VMEM] * (14 + len(others)),
        out_specs=(HBM, HBM, VMEM, VMEM),
        scratch_shapes=[
            pltpu.VMEM(whole, F32),
            pltpu.VMEM(whole, F32),
            pltpu.VMEM((2, members, width_x, depth_y), F32),
            pltpu.VMEM((steps,) + courant_sq.shape, F32),
            pltpu.VMEM((span_x, depth_y), F32),
            pltpu.VMEM((span_x, depth_y), F32),
            pltpu.VMEM((span_z, depth_y), F32),
            pltpu.VMEM((span_z, depth_y), F32),
            pltpu.VMEM((value_rows, depth_y), F32),
            pltpu.VMEM((steps, high_z, depth_y), F32),
            pltpu.VMEM((steps, high_x, depth_y), F32),
            pltpu.SemaphoreType.DMA((2 * members,)),
        ],
        compiler_params=PARAMS,
        name="main",
    )(
        planes, edges, cells, wide, narrow, now, local, cour,
        vals, za, zb, xa, xb, ca, *others,
    )
    ends, late = near(ends, late)
    out = pl.pallas_call(
        functools.partial(fix_kernel, boxes, slabs),
        out_shape=pltpu.HBM(whole, F32),
        in_specs=[VMEM, VMEM, VMEM, HBM],
        out_specs=HBM,
        input_output_aliases={3: 0},
        scratch_shapes=[
            pltpu.VMEM((2, members, width_z, depth_y), F32),
            pltpu.SemaphoreType.DMA((2 * members,)),
        ],
        compiler_params=PARAMS,
        name="fix",
    )(cb, ends, late, *far(out))
    return out, last


def solution(mesh):
    in_specs = (
        P("ens", "box", "slab", None),
        P("ens", "box", "slab", None),
        P("box", "slab", None),
        P(),
        P("ens"),
        P("slab", None, None),
        P("ens"),
        P(),
        P(),
    )
    out_specs = (P("ens", "box", "slab", None), P("ens", "box", "slab", None))
    boxes, slabs = mesh.shape["box"], mesh.shape["slab"]
    return jax.shard_map(
        functools.partial(on_device, boxes, slabs),
        mesh=mesh,
        in_specs=in_specs,
        out_specs=out_specs,
        check_vma=False,
    )
```

```python
import functools

import jax
import jax.numpy as jnp
from jax import lax
from jax.experimental import pallas as pl
from jax.experimental.pallas import tpu as pltpu
from jax.sharding import PartitionSpec as P


F32 = jnp.float32
BF16 = jnp.bfloat16
VMEM = pl.BlockSpec(memory_space=pltpu.VMEM)
SMEM = pl.BlockSpec(memory_space=pltpu.SMEM)
HBM = pl.BlockSpec(memory_space=pl.ANY)
CORNERS = 8
PARAMS = pltpu.CompilerParams(vmem_limit_bytes=16 * 1024 * 1024)


LANES = 128
STRIP = 8


def rows_of(shape, axis):
    return lax.broadcasted_iota(jnp.int32, shape, axis)


def up16(n):
    return (n + 15) // 16 * 16


def beside_y(tiles):
    lane = rows_of(tiles[0].shape, 1)
    right = [pltpu.roll(t, 1, 1) for t in tiles]
    left = [pltpu.roll(t, LANES - 1, 1) for t in tiles]
    before = [0.0] + right[:-1]
    after = left[1:] + [0.0]
    return [
        jnp.where(lane == 0, b, r) + jnp.where(lane == LANES - 1, a, l)
        for b, r, l, a in zip(before, right, left, after)
    ]


def beside_rows(tile, low, high):
    strips = [tile[i : i + STRIP] for i in range(0, tile.shape[0], STRIP)]
    row = rows_of(strips[0].shape, 0)
    down = [pltpu.roll(t, 1, 0) for t in strips]
    up = [pltpu.roll(t, STRIP - 1, 0) for t in strips]
    below = [low] + down[:-1]
    above = up[1:] + [high]
    sums = [
        jnp.where(row == 0, b, d) + jnp.where(row == STRIP - 1, a, u)
        for b, d, u, a in zip(below, down, up, above)
    ]
    return jnp.concatenate(sums, axis=0)


def halves(ref):
    return range(ref.shape[0])


def lanes(h):
    return slice(h * LANES, (h + 1) * LANES)


def depth_rows(ref, z, *lead):
    width_x, width_z = ref.shape[-3:-1]
    count = 1
    for n in ref.shape[:-3]:
        count = count * n
    at = 0
    for i, n in zip(lead, ref.shape[:-3]):
        at = at * n + i
    flat = ref.reshape(count * width_x * width_z, LANES)
    return flat[pl.ds(at * width_x * width_z + z, width_x, stride=width_z), :]


def pack_kernel(
    slots, home, ids_in, weights_in, prof_in, now_in, prev_in, cour_in, cells_in, slabs,
    now, prev, cour, cells, planes, edges, za, zb, vals, xa, xb, ids, weights, prof, block, sems,
):
    _, members, width_x, width_z, _ = now.shape
    steps, samples = weights.shape
    box, slab = lax.axis_index("box"), lax.axis_index("slab")
    total_z = prof.shape[1]
    pairs = [(ids_in, ids), (prof_in, prof), (weights_in, weights)]
    for h in halves(now):
        pairs.append((now_in.at[:, :, :, pl.ds(h * LANES, LANES)], now.at[h]))
    for h in halves(now):
        pairs.append((cour_in.at[:, :, pl.ds(h * LANES, LANES)], cour.at[h]))
        pairs.append((prev_in.at[:, :, :, pl.ds(h * LANES, LANES)], prev.at[h]))
    fields = len(pairs)
    pairs.append((slabs.at[lax.rem(home[0], slots)], block))
    pairs.append((cells_in, cells))
    loads = [pltpu.make_async_copy(a, b, sems.at[i]) for i, (a, b) in enumerate(pairs)]
    for load in loads:
        load.start()
    start_z = slab * width_z
    for load in loads[:3]:
        load.wait()
    row = rows_of((width_z, LANES), 0)
    for m in range(members):
        plane = jnp.zeros((width_z, LANES), F32)
        for z in range(width_z):
            plane = jnp.where(row == z, 1.0 + prof[ids[m], start_z + z], plane)
        planes[m] = plane
        for s, z in ((0, start_z - 1), (1, start_z + width_z)):
            beyond = 1.0 + prof[ids[m], jnp.clip(z, 0, total_z - 1)]
            edges[2 * m + s : 2 * m + s + 1] = jnp.full((1, LANES), beyond, F32)
    owner = slab == home[0] // slots
    points = block.shape[1]
    width = vals.shape[1]
    chunks = points // width
    sample = rows_of((samples, width), 0)
    columns = []
    for t in range(steps):
        column = jnp.zeros((samples, width), F32)
        for k in range(samples):
            column = jnp.where(sample == k, weights[t, k], column)
        columns.append(jnp.where(owner, column, 0.0))
    zero = jnp.zeros((1, LANES), F32)
    for load in loads[3:fields]:
        load.wait()
    face, side = lax.rem(box, 2), lax.rem(slab, 2)

    def local_step(heres, prevs, inners, coefs):
        near = beside_y(heres)
        out = []
        for here, prev_here, inner, coef, n in zip(heres, prevs, inners, coefs, near):
            around = n + beside_rows(here, zero, zero) + inner
            out.append(2.0 * here - prev_here + coef * (around - 6.0 * here))
        return out

    for a, b, at_high, get, length in (
        (za, zb, side == 0, "z", width_z),
        (xa, xb, face == 0, "x", width_x),
    ):
        ends = []
        for at, inner in ((0, 1), (length - 1, length - 2)):
            parts = [[] for _ in halves(now)]
            if get == "x":
                courant = [cour[h, at] for h in halves(now)]
            else:
                courant = [depth_rows(cour, at, h) for h in halves(now)]
            steps_here = []
            for m in range(members):
                if get == "x":
                    heres, prevs, inners = (
                        [ref[h, m, i] for h in halves(now)]
                        for ref, i in ((now, at), (prev, at), (now, inner))
                    )
                    coefs = [c * planes[m] for c in courant]
                else:
                    heres, prevs, inners = (
                        [depth_rows(ref, i, h, m) for h in halves(now)]
                        for ref, i in ((now, at), (prev, at), (now, inner))
                    )
                    coefs = [c * (1.0 + prof[ids[m], start_z + at]) for c in courant]
                steps_here.append(local_step(heres, prevs, inners, coefs))
                for h in halves(now):
                    parts[h].append(heres[h])
            for h in halves(now):
                ends.append(parts[h] + [r[h] for r in steps_here] + [courant[h]])
        count = len(ends) // 2
        for h in range(count):
            for i, (low, high) in enumerate(zip(ends[h], ends[count + h])):
                n = low.shape[0]
                a[i * n : (i + 1) * n, lanes(h)] = jnp.where(at_high, high, low)
                b[i * n : (i + 1) * n, lanes(h)] = jnp.where(at_high, low, high)
    loads[fields].wait()
    for c in range(chunks):
        piece = block[:, c * width : (c + 1) * width]
        for t in range(steps):
            at = t * chunks + c
            vals[at : at + 1] = jnp.sum(columns[t] * piece, axis=0, keepdims=True)
    loads[fields + 1].wait()
    tail = (2 * members + 1) * width_x
    offered = vals[...]
    za[tail:] = offered
    zb[tail:] = offered


def corner_kernel(members, width_z, relay, xa, xb, zb, after, ca, cb):
    box, slab = lax.axis_index("box"), lax.axis_index("slab")
    face, side = lax.rem(box, 2), lax.rem(slab, 2)
    for out, last in ((ca, side == 0), (cb, side == 1)):
        for m in range(members):
            lo, hi = m * width_z, (m + 1) * width_z - 1
            a = jnp.where(last, xa[hi : hi + 1], xa[lo : lo + 1])
            b = jnp.where(last, xb[hi : hi + 1], xb[lo : lo + 1])
            out[2 * m : 2 * m + 1] = jnp.where(face == 0, b, a)
            out[2 * m + 1 : 2 * m + 2] = jnp.where(face == 0, a, b)
    if relay:
        ca[CORNERS:] = zb[zb.shape[0] - relay :]


def split_cell(cell, total_z, depth_y):
    plane = total_z * depth_y
    x = cell // plane
    rest = cell - x * plane
    z = rest // depth_y
    return x, z, rest - z * depth_y


def extended_row(coordinate, start, width):
    d = coordinate - start
    edge = jnp.where(d == -1, width, jnp.where(d == width, width + 1, -1))
    return jnp.where((d >= 0) & (d < width), d, edge)


def one_hot(index, high):
    rows = rows_of((high, index.shape[1]), 0)
    return jnp.where(rows == index, 1.0, 0.0).astype(BF16)


def faces_of(box, slab):
    return jnp.where(box == 0, 0, 1), jnp.where(slab == 0, 2, 3), 4, 5


def local_kernel(
    boxes, slabs, total_z, planes, cells, now, prev, cour, local, wide, narrow, rows_x, rows_z,
):
    count, members, width_x, width_z, _ = now.shape
    depth_y = count * LANES
    box, slab = lax.axis_index("box"), lax.axis_index("slab")
    zero = jnp.zeros((1, LANES), F32)
    for x in range(width_x):
        for m in range(members):
            heres = [now[h, m, x] for h in range(count)]
            near = beside_y(heres)
            for h, here in enumerate(heres):
                around = near[h] + beside_rows(here, zero, zero)
                if x > 0:
                    around = around + now[h, m, x - 1]
                if x < width_x - 1:
                    around = around + now[h, m, x + 1]
                coef = cour[h, x] * planes[m]
                local[h, m, x] = 2.0 * here - prev[h, m, x] + coef * (around - 6.0 * here)
    on_x = (box == 0) | (box == boxes - 1)
    on_z = (slab == 0) | (slab == slabs - 1)
    for i, f in enumerate(faces_of(box, slab)):
        x, z, y = split_cell(cells[pl.ds(f, 1), :], total_z, depth_y)
        x = extended_row(x, box * width_x, width_x)
        z = extended_row(z, slab * width_z, width_z)
        if i == 0:
            rows_z[0] = one_hot(jnp.where(on_x, z, -1), rows_z.shape[1])
            wide[0] = one_hot(y, depth_y)
        elif i == 1:
            rows_x[...] = one_hot(jnp.where(on_z, x, -1), rows_x.shape[0])
            wide[1] = one_hot(y, depth_y)
        else:
            rows_z[i - 1] = one_hot(z, rows_z.shape[1])
            narrow[i - 2] = one_hot(x, narrow.shape[1])


def three_parts(v):
    first = v.astype(BF16)
    rest = v - first.astype(F32)
    second = rest.astype(BF16)
    third = (rest - second.astype(F32)).astype(BF16)
    return first, second, third


def face_source(values, rows, rhs, width):
    heights = [rows.shape[0]] + [up16(width)] * (len(values) - 1)
    parts = []
    for v, high in zip(values, heights):
        for part in three_parts(v):
            parts.append(rows[:high] * jnp.broadcast_to(part, (high, part.shape[1])))
    out = lax.dot_general(
        jnp.concatenate(parts, axis=0), rhs, (((1,), (1,)), ((), ())), preferred_element_type=F32
    )
    sums, at = [], 0
    for high in heights:
        one, two, three = (out[at + i * high : at + (i + 1) * high] for i in range(3))
        sums.append((three + two) + one)
        at = at + 3 * high
    return sums


def main_kernel(
    boxes, slabs, received, planes, edges, wide, narrow, rows_x, rows_z, now, local, cour,
    vals, za, zb, xa, xb, ca, *rest,
):
    others, rest = rest[:received], rest[received:]
    last, nxt, late, one, hz, xlo, xhi, zlo, zhi, value, xsrc, zsrc, sems = rest
    count, members, width_x, width_z, _ = now.shape
    depth_y = count * LANES
    box, slab = lax.axis_index("box"), lax.axis_index("slab")
    face, side = lax.rem(box, 2), lax.rem(slab, 2)
    span_z = (2 * members + 1) * width_x
    low, high = (box > 0, slab > 0), (box < boxes - 1, slab < slabs - 1)
    xlo[...] = jnp.where(low[0], jnp.where(face == 0, xb[...], xa[...]), 0.0)
    xhi[...] = jnp.where(high[0], jnp.where(face == 0, xa[...], xb[...]), 0.0)
    zlo[...] = jnp.where(low[1], jnp.where(side == 0, zb[:span_z], za[:span_z]), 0.0)
    zhi[...] = jnp.where(high[1], jnp.where(side == 0, za[:span_z], zb[:span_z]), 0.0)
    total = vals[...] + za[span_z:]
    if slabs == 4:
        total = total + (zb[span_z:] + ca[CORNERS:])
    for other in others:
        total = total + other[...]
    value[...] = total

    steps = xsrc.shape[0]
    chunks = value.shape[0] // steps
    per = wide.shape[2] // depth_y
    faces = faces_of(box, slab)

    def of_face(f):
        vs = []
        for t in range(steps):
            pieces = [value[pl.ds(t * chunks + f * per + i, 1), :] for i in range(per)]
            vs.append(jnp.concatenate(pieces, axis=1))
        return vs

    for t, s in enumerate(face_source(of_face(faces[0]), rows_z[0], wide[0], width_z)):
        xsrc[t, : s.shape[0]] = s
    for t, s in enumerate(face_source(of_face(faces[1]), rows_x[...], wide[1], width_x)):
        zsrc[t, : s.shape[0]] = s
    ys = [
        face_source(of_face(faces[2 + i]), rows_z[1 + i], narrow[i], width_z) for i in range(2)
    ]

    lane = rows_of((width_z, LANES), 1)
    row = rows_of((width_z, LANES), 0)
    row_of_z = jnp.where(slab == 0, 0, jnp.where(slab == slabs - 1, width_z - 1, -1))
    row_of_x = jnp.where(box == 0, 0, jnp.where(box == boxes - 1, width_x - 1, -1))

    def plane_source(t, x):
        out = []
        for h in range(count):
            part = jnp.where(row == row_of_z, zsrc[t, x : x + 1, lanes(h)], 0.0)
            if h == 0:
                part = part + jnp.where(lane == 0, ys[0][t][:width_z, x : x + 1], 0.0)
            if h == count - 1:
                part = part + jnp.where(lane == LANES - 1, ys[1][t][:width_z, x : x + 1], 0.0)
            if x in (0, width_x - 1):
                part = part + jnp.where(row_of_x == x, xsrc[t, :width_z, lanes(h)], 0.0)
            out.append(part)
        return out

    lane_x = rows_of((width_x, LANES), 1)
    row_x = rows_of((width_x, LANES), 0)
    turned = [jnp.transpose(y[0]) for y in ys]

    def row_source(z):
        out = []
        for h in range(count):
            part = jnp.where(row_x == row_of_x, xsrc[0, z : z + 1, lanes(h)], 0.0)
            if h == 0:
                part = part + jnp.where(lane_x == 0, turned[0][:width_x, z : z + 1], 0.0)
            if h == count - 1:
                part = part + jnp.where(lane_x == LANES - 1, turned[1][:width_x, z : z + 1], 0.0)
            out.append(part)
        return out

    open_x = (low[0], high[0])
    open_a = jnp.where(side == 0, high[1], low[1])
    row_a = jnp.where(side == 0, width_z - 1, 0)
    side_x, side_z = 2 * members * width_z, 2 * members * width_x

    def corner(m, sx, h):
        return jnp.where(open_x[sx] & open_a, ca[2 * m + sx : 2 * m + sx + 1, lanes(h)], 0.0)

    halo_x, coef_x, coef_z = {}, {}, {}
    for s, (ref, x) in enumerate(((xlo, 0), (xhi, width_x - 1))):
        source = plane_source(0, width_x + s)
        for m in range(members):
            for h in range(count):
                coef = ref[side_x:, lanes(h)] * planes[m]
                base = ref[(members + m) * width_z : (members + m + 1) * width_z, lanes(h)]
                own = now[h, m, x] + jnp.where(row == row_a, corner(m, s, h), 0.0)
                halo_x[s, m, h] = base + coef * own + source[h]
                coef_x[s, m, h] = coef
    for s, (ref, z) in enumerate(((zlo, 0), (zhi, width_z - 1))):
        source = row_source(width_z + s)
        for m in range(members):
            for h in range(count):
                coef = ref[side_z:, lanes(h)] * edges[2 * m + s : 2 * m + s + 1]
                base = ref[(members + m) * width_x : (members + m + 1) * width_x, lanes(h)]
                more = jnp.where(row_x == 0, corner(m, 0, h), 0.0)
                more = jnp.where(row_x == width_x - 1, corner(m, 1, h), more)
                own = depth_rows(now, z, h, m) + jnp.where(side == 1 - s, more, 0.0)
                hz[s, h, m] = base + coef * own + source[h]
                coef_z[s, m, h] = coef
    copies = []
    for x in range(width_x):
        source = plane_source(0, x)
        for m in range(members):
            at = m * width_x + x
            for h in range(count):
                low_row, high_row = zlo[at : at + 1, lanes(h)], zhi[at : at + 1, lanes(h)]
                more = jnp.where(row == 0, low_row, jnp.where(row == width_z - 1, high_row, 0.0))
                if x == 0:
                    more = more + xlo[m * width_z : (m + 1) * width_z, lanes(h)]
                if x == width_x - 1:
                    more = more + xhi[m * width_z : (m + 1) * width_z, lanes(h)]
                one[h, m, x] = local[h, m, x] + (cour[h, x] * planes[m]) * more + source[h]
    for h in range(count):
        copies.append(
            pltpu.make_async_copy(
                one.at[h], last.at[:, :, :, pl.ds(h * LANES, LANES)], sems.at[h]
            )
        )
        copies[-1].start()
    for x in range(width_x):
        source = plane_source(1, x)
        for m in range(members):
            heres = [one[h, m, x] for h in range(count)]
            near = beside_y(heres)
            for h, here in enumerate(heres):
                rows = beside_rows(here, hz[0, h, m, x : x + 1], hz[1, h, m, x : x + 1])
                around = near[h] + rows
                around = around + (one[h, m, x - 1] if x > 0 else halo_x[0, m, h])
                around = around + (one[h, m, x + 1] if x < width_x - 1 else halo_x[1, m, h])
                coef = cour[h, x] * planes[m]
                nxt[h, m, x] = 2.0 * here - now[h, m, x] + coef * (around - 6.0 * here) + source[h]
                if x in (0, width_x - 1):
                    s = 0 if x == 0 else 1
                    terms = []
                    for z in (width_z - 1, 0):
                        beyond = coef_z[0 if z == 0 else 1, m, h][x : x + 1]
                        terms.append(coef[z : z + 1] * (beyond + coef_x[s, m, h][z : z + 1]))
                    late[2 * m + s : 2 * m + s + 1, lanes(h)] = jnp.where(
                        side == 0, terms[1], terms[0]
                    )
    for copy in copies:
        copy.wait()


def fix_kernel(boxes, slabs, cb, nxt, late, out, done, sems):
    count, members, width_x, width_z, _ = nxt.shape
    box, slab = lax.axis_index("box"), lax.axis_index("slab")
    side = lax.rem(slab, 2)
    open_x = (box > 0, box < boxes - 1)
    open_b = jnp.where(side == 0, slab > 0, slab < slabs - 1)
    row = rows_of((width_z, LANES), 0)
    row_b = jnp.where(side == 0, 0, width_z - 1)
    copies = []

    def send(source, target):
        copies.append(pltpu.make_async_copy(source, target, sems.at[len(copies)]))
        copies[-1].start()

    for h in range(count):
        inside = pl.ds(1, width_x - 2)
        for m in range(members):
            send(nxt.at[h, m, inside], out.at[m, inside, :, pl.ds(h * LANES, LANES)])
    for h in range(count):
        for m in range(members):
            for s, x in ((0, 0), (1, width_x - 1)):
                at = 2 * m + s
                got = jnp.where(open_x[s] & open_b, cb[at : at + 1, lanes(h)], 0.0)
                add = jnp.where(row == row_b, late[at : at + 1, lanes(h)] * got, 0.0)
                done[h, s, m] = nxt[h, m, x] + add
                send(done.at[h, s, m], out.at[m, x, :, pl.ds(h * LANES, LANES)])
    for copy in copies:
        copy.wait()


def pairs_even(n):
    return [i ^ 1 for i in range(n)]


def pairs_odd(n):
    return [(i + 1) % n if i % 2 else (i - 1) % n for i in range(n)]


def on_device(
    boxes, slabs, pressure_now, pressure_prev, courant_sq, member_profiles, member_ids,
    stored_slabs, slab_home, interp_weights, surface_cells,
):
    members, width_x, width_z, depth_y = pressure_now.shape
    slots, samples, points = stored_slabs.shape
    steps = interp_weights.shape[0]
    total_z = width_z * slabs
    value_rows = steps * points // depth_y
    span_x = (2 * members + 1) * width_z
    span_z = (2 * members + 1) * width_x
    count = depth_y // LANES

    def inner(*dims, dtype=F32):
        return pltpu.VMEM(dims, dtype)

    def far(*arrays):
        return [pltpu.with_memory_space_constraint(a, pltpu.HBM) for a in arrays]

    def near(*arrays):
        return [pltpu.with_memory_space_constraint(a, pltpu.VMEM) for a in arrays]

    def over_slab(x, partner):
        return lax.ppermute(x, "slab", list(enumerate(partner)))

    def over_box(x, odd):
        pairs = []
        for b in range(boxes):
            other = b ^ 1
            if odd:
                other = b + 1 if b % 2 else b - 1
            for s in range(slabs):
                inside = 0 <= other < boxes
                to = other * slabs + s if inside else b * slabs + (s ^ 1)
                pairs.append((b * slabs + s, to))
        return lax.ppermute(x, ("box", "slab"), pairs)

    whole = pressure_now.shape
    half = (count,) + whole[:3] + (LANES,)
    now, prev, cour, cells, planes, edges, za, zb, vals, xa, xb = pl.pallas_call(
        functools.partial(pack_kernel, slots),
        out_shape=(
            inner(*half),
            inner(*half),
            inner(count, width_x, width_z, LANES),
            inner(*surface_cells.shape, dtype=jnp.int32),
            inner(members, width_z, LANES),
            inner(2 * members, LANES),
            inner(span_z + value_rows, depth_y),
            inner(span_z + value_rows, depth_y),
            inner(value_rows, depth_y),
            inner(span_x, depth_y),
            inner(span_x, depth_y),
        ),
        in_specs=[SMEM] + [HBM] * 8,
        out_specs=(VMEM,) * 11,
        scratch_shapes=[
            pltpu.SMEM(member_ids.shape, jnp.int32),
            pltpu.SMEM(interp_weights.shape, F32),
            pltpu.SMEM(member_profiles.shape, F32),
            pltpu.VMEM((samples, points), F32),
            pltpu.SemaphoreType.DMA((5 + 3 * count,)),
        ],
        compiler_params=PARAMS,
        name="pack",
    )(
        slab_home, *far(member_ids, interp_weights, member_profiles),
        *far(pressure_now, pressure_prev, courant_sq, surface_cells, stored_slabs),
    )

    per_face = surface_cells.shape[1]
    za = over_slab(za, pairs_even(slabs))
    zb = over_slab(zb, pairs_odd(slabs))
    xa, xb = over_box(xa, False), over_box(xb, True)
    others = [
        over_slab(vals, [i ^ k for i in range(slabs)])
        for k in range(2, slabs)
        if slabs != 4
    ]
    now, prev, cour, cells, vals, planes, edges = near(
        now, prev, cour, cells, vals, planes, edges
    )
    high_x, high_z = up16(width_x + 2), up16(width_z + 2)
    local, wide, narrow, rows_x, rows_z = near(
        *pl.pallas_call(
            functools.partial(local_kernel, boxes, slabs, total_z),
            out_shape=(
                inner(*half),
                inner(2, depth_y, per_face, dtype=BF16),
                inner(2, high_x, per_face, dtype=BF16),
                inner(high_x, per_face, dtype=BF16),
                inner(3, high_z, per_face, dtype=BF16),
            ),
            in_specs=[VMEM] * 5,
            out_specs=(VMEM,) * 5,
            compiler_params=PARAMS,
            name="local",
        )(planes, cells, now, prev, cour)
    )
    za, zb, xa, xb, *others = near(za, zb, xa, xb, *others)
    relay = value_rows if slabs == 4 else 0
    ca, cb = pl.pallas_call(
        functools.partial(corner_kernel, members, width_z, relay),
        out_shape=(inner(CORNERS + relay, depth_y), inner(CORNERS, depth_y)),
        in_specs=[VMEM] * 4,
        out_specs=(VMEM, VMEM),
        compiler_params=PARAMS,
        name="corner",
    )(xa, xb, zb, local)
    ca, cb = near(over_slab(ca, pairs_even(slabs)), over_slab(cb, pairs_odd(slabs)))

    last, nxt, late = pl.pallas_call(
        functools.partial(main_kernel, boxes, slabs, len(others)),
        out_shape=(pltpu.HBM(whole, F32), inner(*half), inner(2 * members, depth_y)),
        in_specs=[VMEM] * (15 + len(others)),
        out_specs=(HBM, VMEM, VMEM),
        scratch_shapes=[
            inner(*half),
            inner(2, count, members, width_x, LANES),
            inner(span_x, depth_y),
            inner(span_x, depth_y),
            inner(span_z, depth_y),
            inner(span_z, depth_y),
            inner(value_rows, depth_y),
            inner(steps, high_z, depth_y),
            inner(steps, high_x, depth_y),
            pltpu.SemaphoreType.DMA((count,)),
        ],
        compiler_params=PARAMS,
        name="main",
    )(
        planes, edges, wide, narrow, rows_x, rows_z, now, local, cour,
        vals, za, zb, xa, xb, ca, *others,
    )
    out = pl.pallas_call(
        functools.partial(fix_kernel, boxes, slabs),
        out_shape=pltpu.HBM(whole, F32),
        in_specs=[VMEM] * 3,
        out_specs=HBM,
        scratch_shapes=[
            inner(count, 2, members, width_z, LANES),
            pltpu.SemaphoreType.DMA((3 * count * members,)),
        ],
        compiler_params=PARAMS,
        name="fix",
    )(cb, *near(nxt, late))
    return out, last


def solution(mesh):
    in_specs = (
        P("ens", "box", "slab", None),
        P("ens", "box", "slab", None),
        P("box", "slab", None),
        P(),
        P("ens"),
        P("slab", None, None),
        P("ens"),
        P(),
        P(),
    )
    out_specs = (P("ens", "box", "slab", None), P("ens", "box", "slab", None))
    boxes, slabs = mesh.shape["box"], mesh.shape["slab"]
    return jax.shard_map(
        functools.partial(on_device, boxes, slabs),
        mesh=mesh,
        in_specs=in_specs,
        out_specs=out_specs,
        check_vma=False,
    )
```

```python
import functools

import jax
import jax.numpy as jnp
from jax import lax
from jax.experimental import pallas as pl
from jax.experimental.pallas import tpu as pltpu
from jax.sharding import PartitionSpec as P


F32 = jnp.float32
BF16 = jnp.bfloat16
VMEM = pl.BlockSpec(memory_space=pltpu.VMEM)
SMEM = pl.BlockSpec(memory_space=pltpu.SMEM)
HBM = pl.BlockSpec(memory_space=pl.ANY)
CORNERS = 8
PARAMS = pltpu.CompilerParams(vmem_limit_bytes=16 * 1024 * 1024)


LANES = 128
STRIP = 8


def rows_of(shape, axis):
    return lax.broadcasted_iota(jnp.int32, shape, axis)


def up16(n):
    return (n + 15) // 16 * 16


def beside_y(tiles):
    lane = rows_of(tiles[0].shape, 1)
    right = [pltpu.roll(t, 1, 1) for t in tiles]
    left = [pltpu.roll(t, LANES - 1, 1) for t in tiles]
    before = [0.0] + right[:-1]
    after = left[1:] + [0.0]
    return [
        jnp.where(lane == 0, b, r) + jnp.where(lane == LANES - 1, a, l)
        for b, r, l, a in zip(before, right, left, after)
    ]


def beside_rows(tile, low, high):
    strips = [tile[i : i + STRIP] for i in range(0, tile.shape[0], STRIP)]
    row = rows_of(strips[0].shape, 0)
    down = [pltpu.roll(t, 1, 0) for t in strips]
    up = [pltpu.roll(t, STRIP - 1, 0) for t in strips]
    below = [low] + down[:-1]
    above = up[1:] + [high]
    sums = [
        jnp.where(row == 0, b, d) + jnp.where(row == STRIP - 1, a, u)
        for b, d, u, a in zip(below, down, up, above)
    ]
    return jnp.concatenate(sums, axis=0)


def halves(ref):
    return range(ref.shape[0])


def lanes(h):
    return slice(h * LANES, (h + 1) * LANES)


def depth_rows(ref, z, *lead):
    width_x, width_z = ref.shape[-3:-1]
    count = 1
    for n in ref.shape[:-3]:
        count = count * n
    at = 0
    for i, n in zip(lead, ref.shape[:-3]):
        at = at * n + i
    flat = ref.reshape(count * width_x * width_z, LANES)
    return flat[pl.ds(at * width_x * width_z + z, width_x, stride=width_z), :]


def pack_kernel(
    slots, home, ids_in, weights_in, prof_in, now_in, prev_in, cour_in, cells_in, slabs,
    now, prev, cour, cells, planes, edges, za, zb, vals, xa, xb, ids, weights, prof, block, sems,
):
    _, members, width_x, width_z, _ = now.shape
    steps, samples = weights.shape
    box, slab = lax.axis_index("box"), lax.axis_index("slab")
    total_z = prof.shape[1]
    pairs = [(ids_in, ids), (prof_in, prof), (weights_in, weights)]
    for h in halves(now):
        pairs.append((now_in.at[:, :, :, pl.ds(h * LANES, LANES)], now.at[h]))
    for h in halves(now):
        pairs.append((cour_in.at[:, :, pl.ds(h * LANES, LANES)], cour.at[h]))
        pairs.append((prev_in.at[:, :, :, pl.ds(h * LANES, LANES)], prev.at[h]))
    fields = len(pairs)
    pairs.append((slabs.at[lax.rem(home[0], slots)], block))
    pairs.append((cells_in, cells))
    loads = [pltpu.make_async_copy(a, b, sems.at[i]) for i, (a, b) in enumerate(pairs)]
    for load in loads:
        load.start()
    start_z = slab * width_z
    for load in loads[:3]:
        load.wait()
    row = rows_of((width_z, LANES), 0)
    for m in range(members):
        plane = jnp.zeros((width_z, LANES), F32)
        for z in range(width_z):
            plane = jnp.where(row == z, 1.0 + prof[ids[m], start_z + z], plane)
        planes[m] = plane
        for s, z in ((0, start_z - 1), (1, start_z + width_z)):
            beyond = 1.0 + prof[ids[m], jnp.clip(z, 0, total_z - 1)]
            edges[2 * m + s : 2 * m + s + 1] = jnp.full((1, LANES), beyond, F32)
    owner = slab == home[0] // slots
    points = block.shape[1]
    width = vals.shape[1]
    chunks = points // width
    sample = rows_of((samples, width), 0)
    columns = []
    for t in range(steps):
        column = jnp.zeros((samples, width), F32)
        for k in range(samples):
            column = jnp.where(sample == k, weights[t, k], column)
        columns.append(jnp.where(owner, column, 0.0))
    zero = jnp.zeros((1, LANES), F32)
    for load in loads[3:fields]:
        load.wait()
    face, side = lax.rem(box, 2), lax.rem(slab, 2)

    def local_step(heres, prevs, inners, coefs):
        near = beside_y(heres)
        out = []
        for here, prev_here, inner, coef, n in zip(heres, prevs, inners, coefs, near):
            around = n + beside_rows(here, zero, zero) + inner
            out.append(2.0 * here - prev_here + coef * (around - 6.0 * here))
        return out

    for a, b, at_high, get, length in (
        (za, zb, side == 0, "z", width_z),
        (xa, xb, face == 0, "x", width_x),
    ):
        ends = []
        for at, inner in ((0, 1), (length - 1, length - 2)):
            parts = [[] for _ in halves(now)]
            if get == "x":
                courant = [cour[h, at] for h in halves(now)]
            else:
                courant = [depth_rows(cour, at, h) for h in halves(now)]
            steps_here = []
            for m in range(members):
                if get == "x":
                    heres, prevs, inners = (
                        [ref[h, m, i] for h in halves(now)]
                        for ref, i in ((now, at), (prev, at), (now, inner))
                    )
                    coefs = [c * planes[m] for c in courant]
                else:
                    heres, prevs, inners = (
                        [depth_rows(ref, i, h, m) for h in halves(now)]
                        for ref, i in ((now, at), (prev, at), (now, inner))
                    )
                    coefs = [c * (1.0 + prof[ids[m], start_z + at]) for c in courant]
                steps_here.append(local_step(heres, prevs, inners, coefs))
                for h in halves(now):
                    parts[h].append(heres[h])
            for h in halves(now):
                ends.append(parts[h] + [r[h] for r in steps_here] + [courant[h]])
        count = len(ends) // 2
        for h in range(count):
            for i, (low, high) in enumerate(zip(ends[h], ends[count + h])):
                n = low.shape[0]
                a[i * n : (i + 1) * n, lanes(h)] = jnp.where(at_high, high, low)
                b[i * n : (i + 1) * n, lanes(h)] = jnp.where(at_high, low, high)
    loads[fields].wait()
    for c in range(chunks):
        piece = block[:, c * width : (c + 1) * width]
        for t in range(steps):
            at = t * chunks + c
            vals[at : at + 1] = jnp.sum(columns[t] * piece, axis=0, keepdims=True)
    loads[fields + 1].wait()
    tail = (2 * members + 1) * width_x
    offered = vals[...]
    zb[tail:] = offered


def relay_kernel(relay, face, vals, zb, after, za):
    tail = face.shape[0]
    za[:tail] = face[...]
    za[tail:] = vals[...] + zb[tail:] if relay else vals[...]


def corner_kernel(members, width_z, xa, xb, after, ca, cb):
    box, slab = lax.axis_index("box"), lax.axis_index("slab")
    face, side = lax.rem(box, 2), lax.rem(slab, 2)
    for out, last in ((ca, side == 0), (cb, side == 1)):
        for m in range(members):
            lo, hi = m * width_z, (m + 1) * width_z - 1
            a = jnp.where(last, xa[hi : hi + 1], xa[lo : lo + 1])
            b = jnp.where(last, xb[hi : hi + 1], xb[lo : lo + 1])
            out[2 * m : 2 * m + 1] = jnp.where(face == 0, b, a)
            out[2 * m + 1 : 2 * m + 2] = jnp.where(face == 0, a, b)


def split_cell(cell, total_z, depth_y):
    plane = total_z * depth_y
    x = cell // plane
    rest = cell - x * plane
    z = rest // depth_y
    return x, z, rest - z * depth_y


def extended_row(coordinate, start, width):
    d = coordinate - start
    edge = jnp.where(d == -1, width, jnp.where(d == width, width + 1, -1))
    return jnp.where((d >= 0) & (d < width), d, edge)


def one_hot(index, high):
    rows = rows_of((high, index.shape[1]), 0)
    return jnp.where(rows == index, 1.0, 0.0).astype(BF16)


def faces_of(box, slab):
    return jnp.where(box == 0, 0, 1), jnp.where(slab == 0, 2, 3), 4, 5


def local_kernel(
    boxes, slabs, total_z, planes, cells, now, prev, cour, local, wide, narrow, rows_x, rows_z,
):
    count, members, width_x, width_z, _ = now.shape
    depth_y = count * LANES
    box, slab = lax.axis_index("box"), lax.axis_index("slab")
    zero = jnp.zeros((1, LANES), F32)
    for x in range(width_x):
        for m in range(members):
            heres = [now[h, m, x] for h in range(count)]
            near = beside_y(heres)
            for h, here in enumerate(heres):
                around = near[h] + beside_rows(here, zero, zero)
                if x > 0:
                    around = around + now[h, m, x - 1]
                if x < width_x - 1:
                    around = around + now[h, m, x + 1]
                coef = cour[h, x] * planes[m]
                local[h, m, x] = 2.0 * here - prev[h, m, x] + coef * (around - 6.0 * here)
    on_x = (box == 0) | (box == boxes - 1)
    on_z = (slab == 0) | (slab == slabs - 1)
    for i, f in enumerate(faces_of(box, slab)):
        x, z, y = split_cell(cells[pl.ds(f, 1), :], total_z, depth_y)
        x = extended_row(x, box * width_x, width_x)
        z = extended_row(z, slab * width_z, width_z)
        if i == 0:
            rows_z[0] = one_hot(jnp.where(on_x, z, -1), rows_z.shape[1])
            wide[0] = one_hot(y, depth_y)
        elif i == 1:
            rows_x[...] = one_hot(jnp.where(on_z, x, -1), rows_x.shape[0])
            wide[1] = one_hot(y, depth_y)
        else:
            rows_z[i - 1] = one_hot(z, rows_z.shape[1])
            narrow[i - 2] = one_hot(x, narrow.shape[1])


def three_parts(v):
    first = v.astype(BF16)
    rest = v - first.astype(F32)
    second = rest.astype(BF16)
    third = (rest - second.astype(F32)).astype(BF16)
    return first, second, third


def face_source(values, rows, rhs, width):
    heights = [rows.shape[0]] + [up16(width)] * (len(values) - 1)
    parts = []
    for v, high in zip(values, heights):
        for part in three_parts(v):
            parts.append(rows[:high] * jnp.broadcast_to(part, (high, part.shape[1])))
    out = lax.dot_general(
        jnp.concatenate(parts, axis=0), rhs, (((1,), (1,)), ((), ())), preferred_element_type=F32
    )
    sums, at = [], 0
    for high in heights:
        one, two, three = (out[at + i * high : at + (i + 1) * high] for i in range(3))
        sums.append((three + two) + one)
        at = at + 3 * high
    return sums


def main_kernel(
    boxes, slabs, received, planes, edges, wide, narrow, rows_x, rows_z, now, local, cour,
    vals, za, zb, xa, xb, *rest,
):
    others, rest = rest[:received], rest[received:]
    one, nxt, late, hz, xlo, xhi, zlo, zhi, value, xsrc, zsrc = rest
    count, members, width_x, width_z, _ = now.shape
    depth_y = count * LANES
    box, slab = lax.axis_index("box"), lax.axis_index("slab")
    face, side = lax.rem(box, 2), lax.rem(slab, 2)
    span_z = (2 * members + 1) * width_x
    low, high = (box > 0, slab > 0), (box < boxes - 1, slab < slabs - 1)
    xlo[...] = jnp.where(low[0], jnp.where(face == 0, xb[...], xa[...]), 0.0)
    xhi[...] = jnp.where(high[0], jnp.where(face == 0, xa[...], xb[...]), 0.0)
    zlo[...] = jnp.where(low[1], jnp.where(side == 0, zb[:span_z], za[:span_z]), 0.0)
    zhi[...] = jnp.where(high[1], jnp.where(side == 0, za[:span_z], zb[:span_z]), 0.0)
    total = vals[...] + za[span_z:]
    if slabs == 4:
        total = total + zb[span_z:]
    for other in others:
        total = total + other[...]
    value[...] = total

    steps = xsrc.shape[0]
    chunks = value.shape[0] // steps
    per = wide.shape[2] // depth_y
    faces = faces_of(box, slab)

    def of_face(f):
        vs = []
        for t in range(steps):
            pieces = [value[pl.ds(t * chunks + f * per + i, 1), :] for i in range(per)]
            vs.append(jnp.concatenate(pieces, axis=1))
        return vs

    for t, s in enumerate(face_source(of_face(faces[0]), rows_z[0], wide[0], width_z)):
        xsrc[t, : s.shape[0]] = s
    for t, s in enumerate(face_source(of_face(faces[1]), rows_x[...], wide[1], width_x)):
        zsrc[t, : s.shape[0]] = s
    ys = [
        face_source(of_face(faces[2 + i]), rows_z[1 + i], narrow[i], width_z) for i in range(2)
    ]

    lane = rows_of((width_z, LANES), 1)
    row = rows_of((width_z, LANES), 0)
    row_of_z = jnp.where(slab == 0, 0, jnp.where(slab == slabs - 1, width_z - 1, -1))
    row_of_x = jnp.where(box == 0, 0, jnp.where(box == boxes - 1, width_x - 1, -1))

    def plane_source(t, x):
        out = []
        for h in range(count):
            part = jnp.where(row == row_of_z, zsrc[t, x : x + 1, lanes(h)], 0.0)
            if h == 0:
                part = part + jnp.where(lane == 0, ys[0][t][:width_z, x : x + 1], 0.0)
            if h == count - 1:
                part = part + jnp.where(lane == LANES - 1, ys[1][t][:width_z, x : x + 1], 0.0)
            if x in (0, width_x - 1):
                part = part + jnp.where(row_of_x == x, xsrc[t, :width_z, lanes(h)], 0.0)
            out.append(part)
        return out

    lane_x = rows_of((width_x, LANES), 1)
    row_x = rows_of((width_x, LANES), 0)
    turned = [jnp.transpose(y[0]) for y in ys]

    def row_source(z):
        out = []
        for h in range(count):
            part = jnp.where(row_x == row_of_x, xsrc[0, z : z + 1, lanes(h)], 0.0)
            if h == 0:
                part = part + jnp.where(lane_x == 0, turned[0][:width_x, z : z + 1], 0.0)
            if h == count - 1:
                part = part + jnp.where(lane_x == LANES - 1, turned[1][:width_x, z : z + 1], 0.0)
            out.append(part)
        return out

    side_x, side_z = 2 * members * width_z, 2 * members * width_x
    halo_x, coef_x, coef_z = {}, {}, {}
    for s, (ref, x) in enumerate(((xlo, 0), (xhi, width_x - 1))):
        source = plane_source(0, width_x + s)
        for m in range(members):
            for h in range(count):
                coef = ref[side_x:, lanes(h)] * planes[m]
                base = ref[(members + m) * width_z : (members + m + 1) * width_z, lanes(h)]
                halo_x[s, m, h] = base + coef * now[h, m, x] + source[h]
                coef_x[s, m, h] = coef
    for s, (ref, z) in enumerate(((zlo, 0), (zhi, width_z - 1))):
        source = row_source(width_z + s)
        for m in range(members):
            for h in range(count):
                coef = ref[side_z:, lanes(h)] * edges[2 * m + s : 2 * m + s + 1]
                base = ref[(members + m) * width_x : (members + m + 1) * width_x, lanes(h)]
                hz[s, h, m] = base + coef * depth_rows(now, z, h, m) + source[h]
                coef_z[s, m, h] = coef
    for x in range(width_x):
        source = plane_source(0, x)
        for m in range(members):
            at = m * width_x + x
            for h in range(count):
                low_row, high_row = zlo[at : at + 1, lanes(h)], zhi[at : at + 1, lanes(h)]
                more = jnp.where(row == 0, low_row, jnp.where(row == width_z - 1, high_row, 0.0))
                if x == 0:
                    more = more + xlo[m * width_z : (m + 1) * width_z, lanes(h)]
                if x == width_x - 1:
                    more = more + xhi[m * width_z : (m + 1) * width_z, lanes(h)]
                one[h, m, x] = local[h, m, x] + (cour[h, x] * planes[m]) * more + source[h]
    for x in range(width_x):
        source = plane_source(1, x)
        for m in range(members):
            heres = [one[h, m, x] for h in range(count)]
            near = beside_y(heres)
            for h, here in enumerate(heres):
                rows = beside_rows(here, hz[0, h, m, x : x + 1], hz[1, h, m, x : x + 1])
                around = near[h] + rows
                around = around + (one[h, m, x - 1] if x > 0 else halo_x[0, m, h])
                around = around + (one[h, m, x + 1] if x < width_x - 1 else halo_x[1, m, h])
                coef = cour[h, x] * planes[m]
                nxt[h, m, x] = 2.0 * here - now[h, m, x] + coef * (around - 6.0 * here) + source[h]
                if x in (0, width_x - 1):
                    s = 0 if x == 0 else 1
                    for e, z in ((0, 0), (1, width_z - 1)):
                        beyond = coef_z[e, m, h][x : x + 1] + coef_x[s, m, h][z : z + 1]
                        at = 2 * (members * e + m) + s
                        late[at : at + 1, lanes(h)] = coef[z : z + 1] * beyond


def fix_kernel(boxes, slabs, ca, cb, one, nxt, late, out, last, done, sems):
    count, members, width_x, width_z, _ = nxt.shape
    box, slab = lax.axis_index("box"), lax.axis_index("slab")
    side = lax.rem(slab, 2)
    open_x = (box > 0, box < boxes - 1)
    open_z = (slab > 0, slab < slabs - 1)
    row = rows_of((width_z, LANES), 0)
    copies = []

    def send(source, target):
        copies.append(pltpu.make_async_copy(source, target, sems.at[len(copies)]))
        copies[-1].start()

    for h in range(count):
        inside = pl.ds(1, width_x - 2)
        for m in range(members):
            send(nxt.at[h, m, inside], out.at[m, inside, :, pl.ds(h * LANES, LANES)])
            send(one.at[h, m], last.at[m, :, :, pl.ds(h * LANES, LANES)])
    for h in range(count):
        for m in range(members):
            for s, x in ((0, 0), (1, width_x - 1)):
                at = 2 * m + s
                add = 0.0
                for e, z in ((0, 0), (1, width_z - 1)):
                    got = jnp.where(
                        side == e, cb[at : at + 1, lanes(h)], ca[at : at + 1, lanes(h)]
                    )
                    got = jnp.where(open_x[s] & open_z[e], got, 0.0)
                    k = 2 * members * e + at
                    add = jnp.where(row == z, late[k : k + 1, lanes(h)] * got, add)
                done[h, s, m] = nxt[h, m, x] + add
                send(done.at[h, s, m], out.at[m, x, :, pl.ds(h * LANES, LANES)])
    for copy in copies:
        copy.wait()


def pairs_even(n):
    return [i ^ 1 for i in range(n)]


def pairs_odd(n):
    return [(i + 1) % n if i % 2 else (i - 1) % n for i in range(n)]


def on_device(
    boxes, slabs, pressure_now, pressure_prev, courant_sq, member_profiles, member_ids,
    stored_slabs, slab_home, interp_weights, surface_cells,
):
    members, width_x, width_z, depth_y = pressure_now.shape
    slots, samples, points = stored_slabs.shape
    steps = interp_weights.shape[0]
    total_z = width_z * slabs
    value_rows = steps * points // depth_y
    span_x = (2 * members + 1) * width_z
    span_z = (2 * members + 1) * width_x
    count = depth_y // LANES

    def inner(*dims, dtype=F32):
        return pltpu.VMEM(dims, dtype)

    def far(*arrays):
        return [pltpu.with_memory_space_constraint(a, pltpu.HBM) for a in arrays]

    def near(*arrays):
        return [pltpu.with_memory_space_constraint(a, pltpu.VMEM) for a in arrays]

    def over_slab(x, partner):
        return lax.ppermute(x, "slab", list(enumerate(partner)))

    def over_box(x, odd):
        pairs = []
        for b in range(boxes):
            other = b ^ 1
            if odd:
                other = b + 1 if b % 2 else b - 1
            for s in range(slabs):
                inside = 0 <= other < boxes
                to = other * slabs + s if inside else b * slabs + (s ^ 1)
                pairs.append((b * slabs + s, to))
        return lax.ppermute(x, ("box", "slab"), pairs)

    whole = pressure_now.shape
    half = (count,) + whole[:3] + (LANES,)
    now, prev, cour, cells, planes, edges, za, zb, vals, xa, xb = pl.pallas_call(
        functools.partial(pack_kernel, slots),
        out_shape=(
            inner(*half),
            inner(*half),
            inner(count, width_x, width_z, LANES),
            inner(*surface_cells.shape, dtype=jnp.int32),
            inner(members, width_z, LANES),
            inner(2 * members, LANES),
            inner(span_z, depth_y),
            inner(span_z + value_rows, depth_y),
            inner(value_rows, depth_y),
            inner(span_x, depth_y),
            inner(span_x, depth_y),
        ),
        in_specs=[SMEM] + [HBM] * 8,
        out_specs=(VMEM,) * 11,
        scratch_shapes=[
            pltpu.SMEM(member_ids.shape, jnp.int32),
            pltpu.SMEM(interp_weights.shape, F32),
            pltpu.SMEM(member_profiles.shape, F32),
            pltpu.VMEM((samples, points), F32),
            pltpu.SemaphoreType.DMA((5 + 3 * count,)),
        ],
        compiler_params=PARAMS,
        name="pack",
    )(
        slab_home, *far(member_ids, interp_weights, member_profiles),
        *far(pressure_now, pressure_prev, courant_sq, surface_cells, stored_slabs),
    )

    per_face = surface_cells.shape[1]
    zb = over_slab(zb, pairs_odd(slabs))
    xa = over_box(xa, False)
    xb = over_box(xb, True)
    others = [
        over_slab(vals, [i ^ k for i in range(slabs)])
        for k in range(2, slabs)
        if slabs != 4
    ]
    now, prev, cour, cells, vals, planes, edges = near(
        now, prev, cour, cells, vals, planes, edges
    )
    high_x, high_z = up16(width_x + 2), up16(width_z + 2)
    local, wide, narrow, rows_x, rows_z = near(
        *pl.pallas_call(
            functools.partial(local_kernel, boxes, slabs, total_z),
            out_shape=(
                inner(*half),
                inner(2, depth_y, per_face, dtype=BF16),
                inner(2, high_x, per_face, dtype=BF16),
                inner(high_x, per_face, dtype=BF16),
                inner(3, high_z, per_face, dtype=BF16),
            ),
            in_specs=[VMEM] * 5,
            out_specs=(VMEM,) * 5,
            compiler_params=PARAMS,
            name="local",
        )(planes, cells, now, prev, cour)
    )
    za, zb, xa, xb, *others = near(za, zb, xa, xb, *others)
    za = pl.pallas_call(
        functools.partial(relay_kernel, slabs == 4),
        out_shape=inner(span_z + value_rows, depth_y),
        in_specs=[VMEM] * 4,
        out_specs=VMEM,
        compiler_params=PARAMS,
        name="relay",
    )(za, vals, zb, local)
    ca, cb = pl.pallas_call(
        functools.partial(corner_kernel, members, width_z),
        out_shape=(inner(CORNERS, depth_y),) * 2,
        in_specs=[VMEM] * 3,
        out_specs=(VMEM, VMEM),
        compiler_params=PARAMS,
        name="corner",
    )(xa, xb, *near(za))
    za = over_slab(za, pairs_even(slabs))
    ca = over_slab(ca, pairs_even(slabs))
    cb = over_slab(cb, pairs_odd(slabs))
    za, ca, cb = near(za, ca, cb)

    one, nxt, late = pl.pallas_call(
        functools.partial(main_kernel, boxes, slabs, len(others)),
        out_shape=(inner(*half), inner(*half), inner(4 * members, depth_y)),
        in_specs=[VMEM] * (14 + len(others)),
        out_specs=(VMEM, VMEM, VMEM),
        scratch_shapes=[
            inner(2, count, members, width_x, LANES),
            inner(span_x, depth_y),
            inner(span_x, depth_y),
            inner(span_z, depth_y),
            inner(span_z, depth_y),
            inner(value_rows, depth_y),
            inner(steps, high_z, depth_y),
            inner(steps, high_x, depth_y),
        ],
        compiler_params=PARAMS,
        name="main",
    )(
        planes, edges, wide, narrow, rows_x, rows_z, now, local, cour,
        vals, za, zb, xa, xb, *others,
    )
    return pl.pallas_call(
        functools.partial(fix_kernel, boxes, slabs),
        out_shape=(pltpu.HBM(whole, F32),) * 2,
        in_specs=[VMEM] * 5,
        out_specs=(HBM, HBM),
        scratch_shapes=[
            inner(count, 2, members, width_z, LANES),
            pltpu.SemaphoreType.DMA((4 * count * members,)),
        ],
        compiler_params=PARAMS,
        name="fix",
    )(ca, cb, *near(one, nxt, late))


def solution(mesh):
    in_specs = (
        P("ens", "box", "slab", None),
        P("ens", "box", "slab", None),
        P("box", "slab", None),
        P(),
        P("ens"),
        P("slab", None, None),
        P("ens"),
        P(),
        P(),
    )
    out_specs = (P("ens", "box", "slab", None), P("ens", "box", "slab", None))
    boxes, slabs = mesh.shape["box"], mesh.shape["slab"]
    return jax.shard_map(
        functools.partial(on_device, boxes, slabs),
        mesh=mesh,
        in_specs=in_specs,
        out_specs=out_specs,
        check_vma=False,
    )
```

```python
import functools

import jax
import jax.numpy as jnp
from jax import lax
from jax.experimental import pallas as pl
from jax.experimental.pallas import tpu as pltpu
from jax.sharding import PartitionSpec as P


F32 = jnp.float32
BF16 = jnp.bfloat16
VMEM = pl.BlockSpec(memory_space=pltpu.VMEM)
SMEM = pl.BlockSpec(memory_space=pltpu.SMEM)
HBM = pl.BlockSpec(memory_space=pl.ANY)
CORNERS = 8
VALUE_FACES = 4
PARAMS = pltpu.CompilerParams(vmem_limit_bytes=16 * 1024 * 1024)


LANES = 128
STRIP = 8


def rows_of(shape, axis):
    return lax.broadcasted_iota(jnp.int32, shape, axis)


def up16(n):
    return (n + 15) // 16 * 16


def beside_y(tiles):
    lane = rows_of(tiles[0].shape, 1)
    right = [pltpu.roll(t, 1, 1) for t in tiles]
    left = [pltpu.roll(t, LANES - 1, 1) for t in tiles]
    before = [0.0] + right[:-1]
    after = left[1:] + [0.0]
    return [
        jnp.where(lane == 0, b, r) + jnp.where(lane == LANES - 1, a, l)
        for b, r, l, a in zip(before, right, left, after)
    ]


def beside_rows(tile, low, high):
    strips = [tile[i : i + STRIP] for i in range(0, tile.shape[0], STRIP)]
    row = rows_of(strips[0].shape, 0)
    down = [pltpu.roll(t, 1, 0) for t in strips]
    up = [pltpu.roll(t, STRIP - 1, 0) for t in strips]
    below = [low] + down[:-1]
    above = up[1:] + [high]
    sums = [
        jnp.where(row == 0, b, d) + jnp.where(row == STRIP - 1, a, u)
        for b, d, u, a in zip(below, down, up, above)
    ]
    return jnp.concatenate(sums, axis=0)


def halves(ref):
    return range(ref.shape[0])


def lanes(h):
    return slice(h * LANES, (h + 1) * LANES)


def depth_rows(ref, z, *lead):
    width_x, width_z = ref.shape[-3:-1]
    count = 1
    for n in ref.shape[:-3]:
        count = count * n
    at = 0
    for i, n in zip(lead, ref.shape[:-3]):
        at = at * n + i
    flat = ref.reshape(count * width_x * width_z, LANES)
    return flat[pl.ds(at * width_x * width_z + z, width_x, stride=width_z), :]


def pack_kernel(
    slots, depth_devices, home, ids_in, weights_in, prof_in, now_in, prev_in, cour_in, cells_in, slabs,
    now, prev, cour, cells, planes, edges, za, zb, vals, xa, xb, ids, weights, prof, block, sems,
):
    _, members, width_x, width_z, _ = now.shape
    steps, samples = weights.shape
    box, slab = lax.axis_index("box"), lax.axis_index("slab")
    total_z = prof.shape[1]
    pairs = [(ids_in, ids), (prof_in, prof), (weights_in, weights)]
    for h in halves(now):
        pairs.append((cour_in.at[:, :, pl.ds(h * LANES, LANES)], cour.at[h]))
    groups = [len(pairs)]
    for h in halves(now):
        pairs.append((now_in.at[:, :, :, pl.ds(h * LANES, LANES)], now.at[h]))
        pairs.append((prev_in.at[:, :, :, pl.ds(h * LANES, LANES)], prev.at[h]))
    groups = groups + [len(pairs)] * members
    fields = len(pairs)
    pairs.append((slabs.at[lax.rem(home[0], slots)], block))
    pairs.append((cells_in, cells))
    loads = [pltpu.make_async_copy(a, b, sems.at[i]) for i, (a, b) in enumerate(pairs)]
    for load in loads:
        load.start()
    start_z = slab * width_z
    for load in loads[:3]:
        load.wait()
    row = rows_of((width_z, LANES), 0)
    for m in range(members):
        plane = jnp.zeros((width_z, LANES), F32)
        for z in range(width_z):
            plane = jnp.where(row == z, 1.0 + prof[ids[m], start_z + z], plane)
        planes[m] = plane
        for s, z in ((0, start_z - 1), (1, start_z + width_z)):
            beyond = 1.0 + prof[ids[m], jnp.clip(z, 0, total_z - 1)]
            edges[2 * m + s : 2 * m + s + 1] = jnp.full((1, LANES), beyond, F32)
    owner = slab == home[0] // slots
    width = vals.shape[1]
    sample = rows_of((samples, width), 0)
    columns = []
    for t in range(steps):
        column = jnp.zeros((samples, width), F32)
        for k in range(samples):
            column = jnp.where(sample == k, weights[t, k], column)
        columns.append(jnp.where(owner, column, 0.0))
    zero = jnp.zeros((1, LANES), F32)
    for load in loads[3 : groups[0]]:
        load.wait()
    face, side = lax.rem(box, 2), lax.rem(slab, 2)

    def local_step(heres, prevs, inners, coefs):
        near = beside_y(heres)
        out = []
        for here, prev_here, inner, coef, n in zip(heres, prevs, inners, coefs, near):
            around = n + beside_rows(here, zero, zero) + inner
            out.append(2.0 * here - prev_here + coef * (around - 6.0 * here))
        return out

    sides = (
        (za, zb, side == 0, width_x, (0, 1), (width_z - 1, width_z - 2), True),
        (xa, xb, face == 0, width_z, (0, 1), (width_x - 1, width_x - 2), False),
    )

    def plane(ref, at, deep, *lead):
        return depth_rows(ref, at, *lead) if deep else ref[lead + (at,)]

    def put(a, b, at_high, at, h, low, high):
        n = low.shape[0]
        a[at * n : (at + 1) * n, lanes(h)] = jnp.where(at_high, high, low)
        b[at * n : (at + 1) * n, lanes(h)] = jnp.where(at_high, low, high)

    for a, b, at_high, _, (low, _), (high, _), deep in sides:
        for h in halves(now):
            courant = [plane(cour, at, deep, h) for at in (low, high)]
            put(a, b, at_high, 2 * members, h, *courant)
    for m in range(members):
        for load in loads[groups[m] : groups[m + 1]]:
            load.wait()
        for a, b, at_high, _, low, high, deep in sides:
            ends = []
            for at, inner in (low, high):
                heres, prevs, inners = (
                    [plane(ref, i, deep, h, m) for h in halves(now)]
                    for ref, i in ((now, at), (prev, at), (now, inner))
                )
                scale = 1.0 + prof[ids[m], start_z + at] if deep else planes[m]
                coefs = [plane(cour, at, deep, h) * scale for h in halves(now)]
                ends.append((heres, local_step(heres, prevs, inners, coefs)))
            for h in halves(now):
                put(a, b, at_high, m, h, ends[0][0][h], ends[1][0][h])
                put(a, b, at_high, members + m, h, ends[0][1][h], ends[1][1][h])
    per_face = cells.shape[1]
    per = per_face // width
    low_half = slab < depth_devices // 2
    tail = (2 * members + 1) * width_x
    loads[fields].wait()
    picks = (
        (0, jnp.where(box == 0, 0, 1), True, True),
        (1, jnp.where(low_half, 2, 3), True, False),
        (1, jnp.where(low_half, 3, 2), False, True),
        (2, 4, True, True),
        (3, 5, True, True),
    )
    for slot, f, for_near, for_far in picks:
        for i in range(per):
            start = pl.multiple_of(f * per_face + i * width, width)
            piece = block[:, pl.ds(start, width)]
            for t in range(steps):
                at = (t * VALUE_FACES + slot) * per + i
                row_value = jnp.sum(columns[t] * piece, axis=0, keepdims=True)
                if for_near:
                    vals[at : at + 1] = row_value
                if for_far:
                    zb[tail + at : tail + at + 1] = row_value
    loads[fields + 1].wait()


def relay_kernel(relay, face, vals, zb, after, za):
    tail = face.shape[0]
    za[:tail] = face[...]
    za[tail:] = vals[...] + zb[tail:] if relay else vals[...]


def corner_kernel(members, width_z, xa, xb, after, ca, cb):
    box, slab = lax.axis_index("box"), lax.axis_index("slab")
    face, side = lax.rem(box, 2), lax.rem(slab, 2)
    for out, last in ((ca, side == 0), (cb, side == 1)):
        for m in range(members):
            lo, hi = m * width_z, (m + 1) * width_z - 1
            a = jnp.where(last, xa[hi : hi + 1], xa[lo : lo + 1])
            b = jnp.where(last, xb[hi : hi + 1], xb[lo : lo + 1])
            out[2 * m : 2 * m + 1] = jnp.where(face == 0, b, a)
            out[2 * m + 1 : 2 * m + 2] = jnp.where(face == 0, a, b)


def split_cell(cell, total_z, depth_y):
    plane = total_z * depth_y
    x = cell // plane
    rest = cell - x * plane
    z = rest // depth_y
    return x, z, rest - z * depth_y


def extended_row(coordinate, start, width):
    d = coordinate - start
    edge = jnp.where(d == -1, width, jnp.where(d == width, width + 1, -1))
    return jnp.where((d >= 0) & (d < width), d, edge)


def one_hot(index, high):
    rows = rows_of((high, index.shape[1]), 0)
    return jnp.where(rows == index, 1.0, 0.0).astype(BF16)


def faces_of(box, slab):
    return jnp.where(box == 0, 0, 1), jnp.where(slab == 0, 2, 3), 4, 5


def local_kernel(
    boxes, slabs, total_z, planes, cells, now, prev, cour, local, wide, narrow, rows_x, rows_z,
):
    count, members, width_x, width_z, _ = now.shape
    depth_y = count * LANES
    box, slab = lax.axis_index("box"), lax.axis_index("slab")
    zero = jnp.zeros((1, LANES), F32)
    for x in range(width_x):
        for m in range(members):
            heres = [now[h, m, x] for h in range(count)]
            near = beside_y(heres)
            for h, here in enumerate(heres):
                around = near[h] + beside_rows(here, zero, zero)
                if x > 0:
                    around = around + now[h, m, x - 1]
                if x < width_x - 1:
                    around = around + now[h, m, x + 1]
                coef = cour[h, x] * planes[m]
                local[h, m, x] = 2.0 * here - prev[h, m, x] + coef * (around - 6.0 * here)
    on_x = (box == 0) | (box == boxes - 1)
    on_z = (slab == 0) | (slab == slabs - 1)
    for i, f in enumerate(faces_of(box, slab)):
        x, z, y = split_cell(cells[pl.ds(f, 1), :], total_z, depth_y)
        x = extended_row(x, box * width_x, width_x)
        z = extended_row(z, slab * width_z, width_z)
        if i == 0:
            rows_z[0] = one_hot(jnp.where(on_x, z, -1), rows_z.shape[1])
            wide[0] = one_hot(y, depth_y)
        elif i == 1:
            rows_x[...] = one_hot(jnp.where(on_z, x, -1), rows_x.shape[0])
            wide[1] = one_hot(y, depth_y)
        else:
            rows_z[i - 1] = one_hot(z, rows_z.shape[1])
            narrow[i - 2] = one_hot(x, narrow.shape[1])


def three_parts(v):
    first = v.astype(BF16)
    rest = v - first.astype(F32)
    second = rest.astype(BF16)
    third = (rest - second.astype(F32)).astype(BF16)
    return first, second, third


def face_source(values, rows, rhs, width):
    heights = [rows.shape[0]] + [up16(width)] * (len(values) - 1)
    parts = []
    for v, high in zip(values, heights):
        for part in three_parts(v):
            parts.append(rows[:high] * jnp.broadcast_to(part, (high, part.shape[1])))
    out = lax.dot_general(
        jnp.concatenate(parts, axis=0), rhs, (((1,), (1,)), ((), ())), preferred_element_type=F32
    )
    sums, at = [], 0
    for high in heights:
        one, two, three = (out[at + i * high : at + (i + 1) * high] for i in range(3))
        sums.append((three + two) + one)
        at = at + 3 * high
    return sums


def main_kernel(
    boxes, slabs, received, planes, edges, wide, narrow, rows_x, rows_z, now, local, cour,
    vals, za, zb, xa, xb, *rest,
):
    others, rest = rest[:received], rest[received:]
    one, nxt, late, hz, xlo, xhi, zlo, zhi, value, xsrc, zsrc = rest
    count, members, width_x, width_z, _ = now.shape
    depth_y = count * LANES
    box, slab = lax.axis_index("box"), lax.axis_index("slab")
    face, side = lax.rem(box, 2), lax.rem(slab, 2)
    span_z = (2 * members + 1) * width_x
    low, high = (box > 0, slab > 0), (box < boxes - 1, slab < slabs - 1)
    xlo[...] = jnp.where(low[0], jnp.where(face == 0, xb[...], xa[...]), 0.0)
    xhi[...] = jnp.where(high[0], jnp.where(face == 0, xa[...], xb[...]), 0.0)
    zlo[...] = jnp.where(low[1], jnp.where(side == 0, zb[:span_z], za[:span_z]), 0.0)
    zhi[...] = jnp.where(high[1], jnp.where(side == 0, za[:span_z], zb[:span_z]), 0.0)
    total = vals[...] + za[span_z:]
    if slabs == 4:
        total = total + zb[span_z:]
    for other in others:
        total = total + other[...]
    value[...] = total

    steps = xsrc.shape[0]
    chunks = value.shape[0] // steps
    per = wide.shape[2] // depth_y

    def of_face(f):
        vs = []
        for t in range(steps):
            pieces = [value[t * chunks + f * per + i : t * chunks + f * per + i + 1, :] for i in range(per)]
            vs.append(jnp.concatenate(pieces, axis=1))
        return vs

    for t, s in enumerate(face_source(of_face(0), rows_z[0], wide[0], width_z)):
        xsrc[t, : s.shape[0]] = s
    for t, s in enumerate(face_source(of_face(1), rows_x[...], wide[1], width_x)):
        zsrc[t, : s.shape[0]] = s
    ys = [
        face_source(of_face(2 + i), rows_z[1 + i], narrow[i], width_z) for i in range(2)
    ]

    lane = rows_of((width_z, LANES), 1)
    row = rows_of((width_z, LANES), 0)
    row_of_z = jnp.where(slab == 0, 0, jnp.where(slab == slabs - 1, width_z - 1, -1))
    row_of_x = jnp.where(box == 0, 0, jnp.where(box == boxes - 1, width_x - 1, -1))

    def plane_source(t, x):
        out = []
        for h in range(count):
            part = jnp.where(row == row_of_z, zsrc[t, x : x + 1, lanes(h)], 0.0)
            if h == 0:
                part = part + jnp.where(lane == 0, ys[0][t][:width_z, x : x + 1], 0.0)
            if h == count - 1:
                part = part + jnp.where(lane == LANES - 1, ys[1][t][:width_z, x : x + 1], 0.0)
            if x in (0, width_x - 1):
                part = part + jnp.where(row_of_x == x, xsrc[t, :width_z, lanes(h)], 0.0)
            out.append(part)
        return out

    lane_x = rows_of((width_x, LANES), 1)
    row_x = rows_of((width_x, LANES), 0)
    turned = [jnp.transpose(y[0]) for y in ys]

    def row_source(z):
        out = []
        for h in range(count):
            part = jnp.where(row_x == row_of_x, xsrc[0, z : z + 1, lanes(h)], 0.0)
            if h == 0:
                part = part + jnp.where(lane_x == 0, turned[0][:width_x, z : z + 1], 0.0)
            if h == count - 1:
                part = part + jnp.where(lane_x == LANES - 1, turned[1][:width_x, z : z + 1], 0.0)
            out.append(part)
        return out

    side_x, side_z = 2 * members * width_z, 2 * members * width_x
    halo_x, coef_x, coef_z = {}, {}, {}
    for s, (ref, x) in enumerate(((xlo, 0), (xhi, width_x - 1))):
        source = plane_source(0, width_x + s)
        for m in range(members):
            for h in range(count):
                coef = ref[side_x:, lanes(h)] * planes[m]
                base = ref[(members + m) * width_z : (members + m + 1) * width_z, lanes(h)]
                halo_x[s, m, h] = base + coef * now[h, m, x] + source[h]
                coef_x[s, m, h] = coef
    for s, (ref, z) in enumerate(((zlo, 0), (zhi, width_z - 1))):
        source = row_source(width_z + s)
        for m in range(members):
            for h in range(count):
                coef = ref[side_z:, lanes(h)] * edges[2 * m + s : 2 * m + s + 1]
                base = ref[(members + m) * width_x : (members + m + 1) * width_x, lanes(h)]
                hz[s, h, m] = base + coef * depth_rows(now, z, h, m) + source[h]
                coef_z[s, m, h] = coef
    for x in range(width_x):
        source = plane_source(0, x)
        for m in range(members):
            at = m * width_x + x
            for h in range(count):
                low_row, high_row = zlo[at : at + 1, lanes(h)], zhi[at : at + 1, lanes(h)]
                more = jnp.where(row == 0, low_row, jnp.where(row == width_z - 1, high_row, 0.0))
                if x == 0:
                    more = more + xlo[m * width_z : (m + 1) * width_z, lanes(h)]
                if x == width_x - 1:
                    more = more + xhi[m * width_z : (m + 1) * width_z, lanes(h)]
                one[h, m, x] = local[h, m, x] + (cour[h, x] * planes[m]) * more + source[h]
    for x in range(width_x):
        source = plane_source(1, x)
        for m in range(members):
            heres = [one[h, m, x] for h in range(count)]
            near = beside_y(heres)
            for h, here in enumerate(heres):
                rows = beside_rows(here, hz[0, h, m, x : x + 1], hz[1, h, m, x : x + 1])
                around = near[h] + rows
                around = around + (one[h, m, x - 1] if x > 0 else halo_x[0, m, h])
                around = around + (one[h, m, x + 1] if x < width_x - 1 else halo_x[1, m, h])
                coef = cour[h, x] * planes[m]
                nxt[h, m, x] = 2.0 * here - now[h, m, x] + coef * (around - 6.0 * here) + source[h]
                if x in (0, width_x - 1):
                    s = 0 if x == 0 else 1
                    for e, z in ((0, 0), (1, width_z - 1)):
                        beyond = coef_z[e, m, h][x : x + 1] + coef_x[s, m, h][z : z + 1]
                        at = 2 * (members * e + m) + s
                        late[at : at + 1, lanes(h)] = coef[z : z + 1] * beyond


def fix_kernel(boxes, slabs, ca, cb, one, nxt, late, out, last, done, sems):
    count, members, width_x, width_z, _ = nxt.shape
    box, slab = lax.axis_index("box"), lax.axis_index("slab")
    side = lax.rem(slab, 2)
    open_x = (box > 0, box < boxes - 1)
    open_z = (slab > 0, slab < slabs - 1)
    row = rows_of((width_z, LANES), 0)
    copies = []

    def send(source, target):
        copies.append(pltpu.make_async_copy(source, target, sems.at[len(copies)]))
        copies[-1].start()

    for h in range(count):
        inside = pl.ds(1, width_x - 2)
        for m in range(members):
            send(nxt.at[h, m, inside], out.at[m, inside, :, pl.ds(h * LANES, LANES)])
            send(one.at[h, m], last.at[m, :, :, pl.ds(h * LANES, LANES)])
    for h in range(count):
        for m in range(members):
            for s, x in ((0, 0), (1, width_x - 1)):
                at = 2 * m + s
                add = 0.0
                for e, z in ((0, 0), (1, width_z - 1)):
                    got = jnp.where(
                        side == e, cb[at : at + 1, lanes(h)], ca[at : at + 1, lanes(h)]
                    )
                    got = jnp.where(open_x[s] & open_z[e], got, 0.0)
                    k = 2 * members * e + at
                    add = jnp.where(row == z, late[k : k + 1, lanes(h)] * got, add)
                done[h, s, m] = nxt[h, m, x] + add
                send(done.at[h, s, m], out.at[m, x, :, pl.ds(h * LANES, LANES)])
    for copy in copies:
        copy.wait()


def pairs_even(n):
    return [i ^ 1 for i in range(n)]


def pairs_odd(n):
    return [(i + 1) % n if i % 2 else (i - 1) % n for i in range(n)]


def on_device(
    boxes, slabs, pressure_now, pressure_prev, courant_sq, member_profiles, member_ids,
    stored_slabs, slab_home, interp_weights, surface_cells,
):
    members, width_x, width_z, depth_y = pressure_now.shape
    slots, samples, points = stored_slabs.shape
    steps = interp_weights.shape[0]
    total_z = width_z * slabs
    value_rows = steps * VALUE_FACES * surface_cells.shape[1] // depth_y
    span_x = (2 * members + 1) * width_z
    span_z = (2 * members + 1) * width_x
    count = depth_y // LANES

    def inner(*dims, dtype=F32):
        return pltpu.VMEM(dims, dtype)

    def far(*arrays):
        return [pltpu.with_memory_space_constraint(a, pltpu.HBM) for a in arrays]

    def near(*arrays):
        return [pltpu.with_memory_space_constraint(a, pltpu.VMEM) for a in arrays]

    def over_slab(x, partner):
        return lax.ppermute(x, "slab", list(enumerate(partner)))

    def over_box(x, odd):
        pairs = []
        for b in range(boxes):
            other = b ^ 1
            if odd:
                other = b + 1 if b % 2 else b - 1
            for s in range(slabs):
                inside = 0 <= other < boxes
                to = other * slabs + s if inside else b * slabs + (s ^ 1)
                pairs.append((b * slabs + s, to))
        return lax.ppermute(x, ("box", "slab"), pairs)

    whole = pressure_now.shape
    half = (count,) + whole[:3] + (LANES,)
    now, prev, cour, cells, planes, edges, za, zb, vals, xa, xb = pl.pallas_call(
        functools.partial(pack_kernel, slots, slabs),
        out_shape=(
            inner(*half),
            inner(*half),
            inner(count, width_x, width_z, LANES),
            inner(*surface_cells.shape, dtype=jnp.int32),
            inner(members, width_z, LANES),
            inner(2 * members, LANES),
            inner(span_z, depth_y),
            inner(span_z + value_rows, depth_y),
            inner(value_rows, depth_y),
            inner(span_x, depth_y),
            inner(span_x, depth_y),
        ),
        in_specs=[SMEM] + [HBM] * 8,
        out_specs=(VMEM,) * 11,
        scratch_shapes=[
            pltpu.SMEM(member_ids.shape, jnp.int32),
            pltpu.SMEM(interp_weights.shape, F32),
            pltpu.SMEM(member_profiles.shape, F32),
            pltpu.VMEM((samples, points), F32),
            pltpu.SemaphoreType.DMA((5 + 3 * count,)),
        ],
        compiler_params=PARAMS,
        name="pack",
    )(
        slab_home, *far(member_ids, interp_weights, member_profiles),
        *far(pressure_now, pressure_prev, courant_sq, surface_cells, stored_slabs),
    )

    per_face = surface_cells.shape[1]
    away = zb[span_z:]
    zb = over_slab(zb, pairs_odd(slabs))
    xa = over_box(xa, False)
    xb = over_box(xb, True)
    others = [
        over_slab(vals if k < slabs // 2 else away, [i ^ k for i in range(slabs)])
        for k in range(2, slabs)
        if slabs != 4
    ]
    now, prev, cour, cells, vals, planes, edges = near(
        now, prev, cour, cells, vals, planes, edges
    )
    high_x, high_z = up16(width_x + 2), up16(width_z + 2)
    local, wide, narrow, rows_x, rows_z = near(
        *pl.pallas_call(
            functools.partial(local_kernel, boxes, slabs, total_z),
            out_shape=(
                inner(*half),
                inner(2, depth_y, per_face, dtype=BF16),
                inner(2, high_x, per_face, dtype=BF16),
                inner(high_x, per_face, dtype=BF16),
                inner(3, high_z, per_face, dtype=BF16),
            ),
            in_specs=[VMEM] * 5,
            out_specs=(VMEM,) * 5,
            compiler_params=PARAMS,
            name="local",
        )(planes, cells, now, prev, cour)
    )
    za, zb, xa, xb, *others = near(za, zb, xa, xb, *others)
    za = pl.pallas_call(
        functools.partial(relay_kernel, slabs == 4),
        out_shape=inner(span_z + value_rows, depth_y),
        in_specs=[VMEM] * 4,
        out_specs=VMEM,
        compiler_params=PARAMS,
        name="relay",
    )(za, vals, zb, local)
    ca, cb = pl.pallas_call(
        functools.partial(corner_kernel, members, width_z),
        out_shape=(inner(CORNERS, depth_y),) * 2,
        in_specs=[VMEM] * 3,
        out_specs=(VMEM, VMEM),
        compiler_params=PARAMS,
        name="corner",
    )(xa, xb, *near(za))
    za = over_slab(za, pairs_even(slabs))
    ca = over_slab(ca, pairs_even(slabs))
    cb = over_slab(cb, pairs_odd(slabs))
    za, ca, cb = near(za, ca, cb)

    one, nxt, late = pl.pallas_call(
        functools.partial(main_kernel, boxes, slabs, len(others)),
        out_shape=(inner(*half), inner(*half), inner(4 * members, depth_y)),
        in_specs=[VMEM] * (14 + len(others)),
        out_specs=(VMEM, VMEM, VMEM),
        scratch_shapes=[
            inner(2, count, members, width_x, LANES),
            inner(span_x, depth_y),
            inner(span_x, depth_y),
            inner(span_z, depth_y),
            inner(span_z, depth_y),
            inner(value_rows, depth_y),
            inner(steps, high_z, depth_y),
            inner(steps, high_x, depth_y),
        ],
        compiler_params=PARAMS,
        name="main",
    )(
        planes, edges, wide, narrow, rows_x, rows_z, now, local, cour,
        vals, za, zb, xa, xb, *others,
    )
    return pl.pallas_call(
        functools.partial(fix_kernel, boxes, slabs),
        out_shape=(pltpu.HBM(whole, F32),) * 2,
        in_specs=[VMEM] * 5,
        out_specs=(HBM, HBM),
        scratch_shapes=[
            inner(count, 2, members, width_z, LANES),
            pltpu.SemaphoreType.DMA((4 * count * members,)),
        ],
        compiler_params=PARAMS,
        name="fix",
    )(ca, cb, *near(one, nxt, late))


def solution(mesh):
    in_specs = (
        P("ens", "box", "slab", None),
        P("ens", "box", "slab", None),
        P("box", "slab", None),
        P(),
        P("ens"),
        P("slab", None, None),
        P("ens"),
        P(),
        P(),
    )
    out_specs = (P("ens", "box", "slab", None), P("ens", "box", "slab", None))
    boxes, slabs = mesh.shape["box"], mesh.shape["slab"]
    return jax.shard_map(
        functools.partial(on_device, boxes, slabs),
        mesh=mesh,
        in_specs=in_specs,
        out_specs=out_specs,
        check_vma=False,
    )
```

```python
import functools

import jax
import jax.numpy as jnp
from jax import lax
from jax.experimental import pallas as pl
from jax.experimental.pallas import tpu as pltpu
from jax.sharding import PartitionSpec as P


F32 = jnp.float32
BF16 = jnp.bfloat16
VMEM = pl.BlockSpec(memory_space=pltpu.VMEM)
SMEM = pl.BlockSpec(memory_space=pltpu.SMEM)
HBM = pl.BlockSpec(memory_space=pl.ANY)
CORNERS = 8
VALUE_FACES = 4
PARAMS = pltpu.CompilerParams(vmem_limit_bytes=16 * 1024 * 1024)


LANES = 128
STRIP = 8


def rows_of(shape, axis):
    return lax.broadcasted_iota(jnp.int32, shape, axis)


def up16(n):
    return (n + 15) // 16 * 16


def beside_y(tiles):
    lane = rows_of(tiles[0].shape, 1)
    right = [pltpu.roll(t, 1, 1) for t in tiles]
    left = [pltpu.roll(t, LANES - 1, 1) for t in tiles]
    before = [0.0] + right[:-1]
    after = left[1:] + [0.0]
    return [
        jnp.where(lane == 0, b, r) + jnp.where(lane == LANES - 1, a, l)
        for b, r, l, a in zip(before, right, left, after)
    ]


def beside_rows(tile, low, high):
    strips = [tile[i : i + STRIP] for i in range(0, tile.shape[0], STRIP)]
    row = rows_of(strips[0].shape, 0)
    down = [pltpu.roll(t, 1, 0) for t in strips]
    up = [pltpu.roll(t, STRIP - 1, 0) for t in strips]
    below = [low] + down[:-1]
    above = up[1:] + [high]
    sums = [
        jnp.where(row == 0, b, d) + jnp.where(row == STRIP - 1, a, u)
        for b, d, u, a in zip(below, down, up, above)
    ]
    return jnp.concatenate(sums, axis=0)


def halves(ref):
    return range(ref.shape[0])


def lanes(h):
    return slice(h * LANES, (h + 1) * LANES)


def depth_rows(ref, z, *lead):
    width_x, width_z = ref.shape[-3:-1]
    count = 1
    for n in ref.shape[:-3]:
        count = count * n
    at = 0
    for i, n in zip(lead, ref.shape[:-3]):
        at = at * n + i
    flat = ref.reshape(count * width_x * width_z, LANES)
    return flat[pl.ds(at * width_x * width_z + z, width_x, stride=width_z), :]


def pack_kernel(
    slots, depth_devices, home, ids_in, weights_in, prof_in, now_in, prev_in, cour_in, cells_in, slabs,
    now, prev, cour, cells, planes, edges, za, zb, vals, xa, xb, ids, weights, prof, block, sems,
):
    _, members, width_x, width_z, _ = now.shape
    steps, samples = weights.shape
    box, slab = lax.axis_index("box"), lax.axis_index("slab")
    total_z = prof.shape[1]
    pairs = [(ids_in, ids), (prof_in, prof), (weights_in, weights)]
    for h in halves(now):
        pairs.append((cour_in.at[:, :, pl.ds(h * LANES, LANES)], cour.at[h]))
    groups = [len(pairs)]
    for h in halves(now):
        pairs.append((now_in.at[:, :, :, pl.ds(h * LANES, LANES)], now.at[h]))
        pairs.append((prev_in.at[:, :, :, pl.ds(h * LANES, LANES)], prev.at[h]))
    groups = groups + [len(pairs)] * members
    fields = len(pairs)
    pairs.append((slabs.at[lax.rem(home[0], slots)], block))
    pairs.append((cells_in, cells))
    loads = [pltpu.make_async_copy(a, b, sems.at[i]) for i, (a, b) in enumerate(pairs)]
    for load in loads:
        load.start()
    start_z = slab * width_z
    for load in loads[:3]:
        load.wait()
    row = rows_of((width_z, LANES), 0)
    for m in range(members):
        plane = jnp.zeros((width_z, LANES), F32)
        for z in range(width_z):
            plane = jnp.where(row == z, 1.0 + prof[ids[m], start_z + z], plane)
        planes[m] = plane
        for s, z in ((0, start_z - 1), (1, start_z + width_z)):
            beyond = 1.0 + prof[ids[m], jnp.clip(z, 0, total_z - 1)]
            edges[2 * m + s : 2 * m + s + 1] = jnp.full((1, LANES), beyond, F32)
    owner = slab == home[0] // slots
    width = vals.shape[1]
    sample = rows_of((samples, width), 0)
    columns = []
    for t in range(steps):
        column = jnp.zeros((samples, width), F32)
        for k in range(samples):
            column = jnp.where(sample == k, weights[t, k], column)
        columns.append(jnp.where(owner, column, 0.0))
    zero = jnp.zeros((1, LANES), F32)
    for load in loads[3 : groups[0]]:
        load.wait()
    face, side = lax.rem(box, 2), lax.rem(slab, 2)

    def local_step(heres, prevs, inners, coefs):
        near = beside_y(heres)
        out = []
        for here, prev_here, inner, coef, n in zip(heres, prevs, inners, coefs, near):
            around = n + beside_rows(here, zero, zero) + inner
            out.append(2.0 * here - prev_here + coef * (around - 6.0 * here))
        return out

    sides = (
        (za, zb, side == 0, width_x, (0, 1), (width_z - 1, width_z - 2), True),
        (xa, xb, face == 0, width_z, (0, 1), (width_x - 1, width_x - 2), False),
    )

    def plane(ref, at, deep, *lead):
        return depth_rows(ref, at, *lead) if deep else ref[lead + (at,)]

    def put(a, b, at_high, at, h, low, high):
        n = low.shape[0]
        a[at * n : (at + 1) * n, lanes(h)] = jnp.where(at_high, high, low)
        b[at * n : (at + 1) * n, lanes(h)] = jnp.where(at_high, low, high)

    for a, b, at_high, _, (low, _), (high, _), deep in sides:
        for h in halves(now):
            courant = [plane(cour, at, deep, h) for at in (low, high)]
            put(a, b, at_high, 2 * members, h, *courant)
    for m in range(members):
        for load in loads[groups[m] : groups[m + 1]]:
            load.wait()
        for a, b, at_high, _, low, high, deep in sides:
            ends = []
            for at, inner in (low, high):
                heres, prevs, inners = (
                    [plane(ref, i, deep, h, m) for h in halves(now)]
                    for ref, i in ((now, at), (prev, at), (now, inner))
                )
                scale = 1.0 + prof[ids[m], start_z + at] if deep else planes[m]
                coefs = [plane(cour, at, deep, h) * scale for h in halves(now)]
                ends.append((heres, local_step(heres, prevs, inners, coefs)))
            for h in halves(now):
                put(a, b, at_high, m, h, ends[0][0][h], ends[1][0][h])
                put(a, b, at_high, members + m, h, ends[0][1][h], ends[1][1][h])
    per_face = cells.shape[1]
    per = per_face // width
    low_half = slab < depth_devices // 2
    tail = (2 * members + 1) * width_x
    loads[fields].wait()
    picks = (
        (0, jnp.where(box == 0, 0, 1), True, True),
        (1, jnp.where(low_half, 2, 3), True, False),
        (1, jnp.where(low_half, 3, 2), False, True),
        (2, 4, True, True),
        (3, 5, True, True),
    )
    for slot, f, for_near, for_far in picks:
        for i in range(per):
            start = pl.multiple_of(f * per_face + i * width, width)
            piece = block[:, pl.ds(start, width)]
            for t in range(steps):
                at = (t * VALUE_FACES + slot) * per + i
                row_value = jnp.sum(columns[t] * piece, axis=0, keepdims=True)
                if for_near:
                    vals[at : at + 1] = row_value
                if for_far:
                    zb[tail + at : tail + at + 1] = row_value
    loads[fields + 1].wait()


def relay_kernel(relay, face, vals, zb, after, za):
    tail = face.shape[0]
    za[:tail] = face[...]
    za[tail:] = vals[...] + zb[tail:] if relay else vals[...]


def corner_kernel(members, width_z, xa, xb, after, ca, cb):
    box, slab = lax.axis_index("box"), lax.axis_index("slab")
    face, side = lax.rem(box, 2), lax.rem(slab, 2)
    for out, last in ((ca, side == 0), (cb, side == 1)):
        for m in range(members):
            lo, hi = m * width_z, (m + 1) * width_z - 1
            a = jnp.where(last, xa[hi : hi + 1], xa[lo : lo + 1])
            b = jnp.where(last, xb[hi : hi + 1], xb[lo : lo + 1])
            out[2 * m : 2 * m + 1] = jnp.where(face == 0, b, a)
            out[2 * m + 1 : 2 * m + 2] = jnp.where(face == 0, a, b)


def split_cell(cell, total_z, depth_y):
    plane = total_z * depth_y
    x = cell // plane
    rest = cell - x * plane
    z = rest // depth_y
    return x, z, rest - z * depth_y


def extended_row(coordinate, start, width):
    d = coordinate - start
    edge = jnp.where(d == -1, width, jnp.where(d == width, width + 1, -1))
    return jnp.where((d >= 0) & (d < width), d, edge)


def one_hot(index, high):
    rows = rows_of((high, index.shape[1]), 0)
    return jnp.where(rows == index, 1.0, 0.0).astype(BF16)


def faces_of(box, slab):
    return jnp.where(box == 0, 0, 1), jnp.where(slab == 0, 2, 3), 4, 5


def local_kernel(
    boxes, slabs, total_z, planes, cells, now, prev, cour, local, wide, narrow, rows_x, rows_z,
):
    count, members, width_x, width_z, _ = now.shape
    depth_y = count * LANES
    box, slab = lax.axis_index("box"), lax.axis_index("slab")
    zero = jnp.zeros((1, LANES), F32)
    for x in range(width_x):
        for m in range(members):
            heres = [now[h, m, x] for h in range(count)]
            near = beside_y(heres)
            for h, here in enumerate(heres):
                around = near[h] + beside_rows(here, zero, zero)
                if x > 0:
                    around = around + now[h, m, x - 1]
                if x < width_x - 1:
                    around = around + now[h, m, x + 1]
                coef = cour[h, x] * planes[m]
                local[h, m, x] = 2.0 * here - prev[h, m, x] + coef * (around - 6.0 * here)
    on_x = (box == 0) | (box == boxes - 1)
    on_z = (slab == 0) | (slab == slabs - 1)
    for i, f in enumerate(faces_of(box, slab)):
        x, z, y = split_cell(cells[pl.ds(f, 1), :], total_z, depth_y)
        x = extended_row(x, box * width_x, width_x)
        z = extended_row(z, slab * width_z, width_z)
        if i == 0:
            rows_z[0] = one_hot(jnp.where(on_x, z, -1), rows_z.shape[1])
            wide[0] = one_hot(y, depth_y)
        elif i == 1:
            rows_x[...] = one_hot(jnp.where(on_z, x, -1), rows_x.shape[0])
            wide[1] = one_hot(y, depth_y)
        else:
            rows_z[i - 1] = one_hot(z, rows_z.shape[1])
            narrow[i - 2] = one_hot(x, narrow.shape[1])


def three_parts(v):
    first = v.astype(BF16)
    rest = v - first.astype(F32)
    second = rest.astype(BF16)
    third = (rest - second.astype(F32)).astype(BF16)
    return first, second, third


def face_source(values, rows, rhs, width):
    heights = [rows.shape[0]] + [up16(width)] * (len(values) - 1)
    parts = []
    for v, high in zip(values, heights):
        for part in three_parts(v):
            parts.append(rows[:high] * jnp.broadcast_to(part, (high, part.shape[1])))
    out = lax.dot_general(
        jnp.concatenate(parts, axis=0), rhs, (((1,), (1,)), ((), ())), preferred_element_type=F32
    )
    sums, at = [], 0
    for high in heights:
        one, two, three = (out[at + i * high : at + (i + 1) * high] for i in range(3))
        sums.append((three + two) + one)
        at = at + 3 * high
    return sums


def main_kernel(
    boxes, slabs, received, planes, edges, wide, narrow, rows_x, rows_z, now, local, cour,
    vals, za, zb, xa, xb, *rest,
):
    others, rest = rest[:received], rest[received:]
    last, one, nxt, late, hz, xlo, xhi, zlo, zhi, value, xsrc, zsrc, sems = rest
    count, members, width_x, width_z, _ = now.shape
    depth_y = count * LANES
    box, slab = lax.axis_index("box"), lax.axis_index("slab")
    face, side = lax.rem(box, 2), lax.rem(slab, 2)
    span_z = (2 * members + 1) * width_x
    low, high = (box > 0, slab > 0), (box < boxes - 1, slab < slabs - 1)
    xlo[...] = jnp.where(low[0], jnp.where(face == 0, xb[...], xa[...]), 0.0)
    xhi[...] = jnp.where(high[0], jnp.where(face == 0, xa[...], xb[...]), 0.0)
    zlo[...] = jnp.where(low[1], jnp.where(side == 0, zb[:span_z], za[:span_z]), 0.0)
    zhi[...] = jnp.where(high[1], jnp.where(side == 0, za[:span_z], zb[:span_z]), 0.0)
    total = vals[...] + za[span_z:]
    if slabs == 4:
        total = total + zb[span_z:]
    for other in others:
        total = total + other[...]
    value[...] = total

    steps = xsrc.shape[0]
    chunks = value.shape[0] // steps
    per = wide.shape[2] // depth_y

    def of_face(f):
        vs = []
        for t in range(steps):
            pieces = [value[t * chunks + f * per + i : t * chunks + f * per + i + 1, :] for i in range(per)]
            vs.append(jnp.concatenate(pieces, axis=1))
        return vs

    for t, s in enumerate(face_source(of_face(0), rows_z[0], wide[0], width_z)):
        xsrc[t, : s.shape[0]] = s
    for t, s in enumerate(face_source(of_face(1), rows_x[...], wide[1], width_x)):
        zsrc[t, : s.shape[0]] = s
    ys = [
        face_source(of_face(2 + i), rows_z[1 + i], narrow[i], width_z) for i in range(2)
    ]

    lane = rows_of((width_z, LANES), 1)
    row = rows_of((width_z, LANES), 0)
    row_of_z = jnp.where(slab == 0, 0, jnp.where(slab == slabs - 1, width_z - 1, -1))
    row_of_x = jnp.where(box == 0, 0, jnp.where(box == boxes - 1, width_x - 1, -1))

    def plane_source(t, x):
        out = []
        for h in range(count):
            part = jnp.where(row == row_of_z, zsrc[t, x : x + 1, lanes(h)], 0.0)
            if h == 0:
                part = part + jnp.where(lane == 0, ys[0][t][:width_z, x : x + 1], 0.0)
            if h == count - 1:
                part = part + jnp.where(lane == LANES - 1, ys[1][t][:width_z, x : x + 1], 0.0)
            if x in (0, width_x - 1):
                part = part + jnp.where(row_of_x == x, xsrc[t, :width_z, lanes(h)], 0.0)
            out.append(part)
        return out

    lane_x = rows_of((width_x, LANES), 1)
    row_x = rows_of((width_x, LANES), 0)
    turned = [jnp.transpose(y[0]) for y in ys]

    def row_source(z):
        out = []
        for h in range(count):
            part = jnp.where(row_x == row_of_x, xsrc[0, z : z + 1, lanes(h)], 0.0)
            if h == 0:
                part = part + jnp.where(lane_x == 0, turned[0][:width_x, z : z + 1], 0.0)
            if h == count - 1:
                part = part + jnp.where(lane_x == LANES - 1, turned[1][:width_x, z : z + 1], 0.0)
            out.append(part)
        return out

    side_x, side_z = 2 * members * width_z, 2 * members * width_x
    halo_x, coef_x, coef_z = {}, {}, {}
    for s, (ref, x) in enumerate(((xlo, 0), (xhi, width_x - 1))):
        source = plane_source(0, width_x + s)
        for m in range(members):
            for h in range(count):
                coef = ref[side_x:, lanes(h)] * planes[m]
                base = ref[(members + m) * width_z : (members + m + 1) * width_z, lanes(h)]
                halo_x[s, m, h] = base + coef * now[h, m, x] + source[h]
                coef_x[s, m, h] = coef
    for s, (ref, z) in enumerate(((zlo, 0), (zhi, width_z - 1))):
        source = row_source(width_z + s)
        for m in range(members):
            for h in range(count):
                coef = ref[side_z:, lanes(h)] * edges[2 * m + s : 2 * m + s + 1]
                base = ref[(members + m) * width_x : (members + m + 1) * width_x, lanes(h)]
                hz[s, h, m] = base + coef * depth_rows(now, z, h, m) + source[h]
                coef_z[s, m, h] = coef
    sources = [plane_source(0, x) for x in range(width_x)]
    copies = []
    for m in range(members):
        for x in range(width_x):
            at = m * width_x + x
            for h in range(count):
                low_row, high_row = zlo[at : at + 1, lanes(h)], zhi[at : at + 1, lanes(h)]
                more = jnp.where(row == 0, low_row, jnp.where(row == width_z - 1, high_row, 0.0))
                if x == 0:
                    more = more + xlo[m * width_z : (m + 1) * width_z, lanes(h)]
                if x == width_x - 1:
                    more = more + xhi[m * width_z : (m + 1) * width_z, lanes(h)]
                one[h, m, x] = local[h, m, x] + (cour[h, x] * planes[m]) * more + sources[x][h]
        for h in range(count):
            copies.append(
                pltpu.make_async_copy(
                    one.at[h, m], last.at[m, :, :, pl.ds(h * LANES, LANES)], sems.at[len(copies)]
                )
            )
            copies[-1].start()
    for x in range(width_x):
        source = plane_source(1, x)
        for m in range(members):
            heres = [one[h, m, x] for h in range(count)]
            near = beside_y(heres)
            for h, here in enumerate(heres):
                rows = beside_rows(here, hz[0, h, m, x : x + 1], hz[1, h, m, x : x + 1])
                around = near[h] + rows
                around = around + (one[h, m, x - 1] if x > 0 else halo_x[0, m, h])
                around = around + (one[h, m, x + 1] if x < width_x - 1 else halo_x[1, m, h])
                coef = cour[h, x] * planes[m]
                nxt[h, m, x] = 2.0 * here - now[h, m, x] + coef * (around - 6.0 * here) + source[h]
                if x in (0, width_x - 1):
                    s = 0 if x == 0 else 1
                    for e, z in ((0, 0), (1, width_z - 1)):
                        beyond = coef_z[e, m, h][x : x + 1] + coef_x[s, m, h][z : z + 1]
                        at = 2 * (members * e + m) + s
                        late[at : at + 1, lanes(h)] = coef[z : z + 1] * beyond
    for copy in copies:
        copy.wait()


def fix_kernel(boxes, slabs, ca, cb, one, nxt, late, first, out, last, done, sems):
    count, members, width_x, width_z, _ = nxt.shape
    box, slab = lax.axis_index("box"), lax.axis_index("slab")
    side = lax.rem(slab, 2)
    open_x = (box > 0, box < boxes - 1)
    open_z = (slab > 0, slab < slabs - 1)
    row = rows_of((width_z, LANES), 0)
    copies = []

    def send(source, target):
        copies.append(pltpu.make_async_copy(source, target, sems.at[len(copies)]))
        copies[-1].start()

    for h in range(count):
        inside = pl.ds(1, width_x - 2)
        for m in range(members):
            send(nxt.at[h, m, inside], out.at[m, inside, :, pl.ds(h * LANES, LANES)])
    for h in range(count):
        for m in range(members):
            for s, x in ((0, 0), (1, width_x - 1)):
                at = 2 * m + s
                add = 0.0
                for e, z in ((0, 0), (1, width_z - 1)):
                    got = jnp.where(
                        side == e, cb[at : at + 1, lanes(h)], ca[at : at + 1, lanes(h)]
                    )
                    got = jnp.where(open_x[s] & open_z[e], got, 0.0)
                    k = 2 * members * e + at
                    add = jnp.where(row == z, late[k : k + 1, lanes(h)] * got, add)
                done[h, s, m] = nxt[h, m, x] + add
                send(done.at[h, s, m], out.at[m, x, :, pl.ds(h * LANES, LANES)])
    for copy in copies:
        copy.wait()


def pairs_even(n):
    return [i ^ 1 for i in range(n)]


def pairs_odd(n):
    return [(i + 1) % n if i % 2 else (i - 1) % n for i in range(n)]


def on_device(
    boxes, slabs, pressure_now, pressure_prev, courant_sq, member_profiles, member_ids,
    stored_slabs, slab_home, interp_weights, surface_cells,
):
    members, width_x, width_z, depth_y = pressure_now.shape
    slots, samples, points = stored_slabs.shape
    steps = interp_weights.shape[0]
    total_z = width_z * slabs
    value_rows = steps * VALUE_FACES * surface_cells.shape[1] // depth_y
    span_x = (2 * members + 1) * width_z
    span_z = (2 * members + 1) * width_x
    count = depth_y // LANES

    def inner(*dims, dtype=F32):
        return pltpu.VMEM(dims, dtype)

    def far(*arrays):
        return [pltpu.with_memory_space_constraint(a, pltpu.HBM) for a in arrays]

    def near(*arrays):
        return [pltpu.with_memory_space_constraint(a, pltpu.VMEM) for a in arrays]

    def over_slab(x, partner):
        return lax.ppermute(x, "slab", list(enumerate(partner)))

    def over_box(x, odd):
        pairs = []
        for b in range(boxes):
            other = b ^ 1
            if odd:
                other = b + 1 if b % 2 else b - 1
            for s in range(slabs):
                inside = 0 <= other < boxes
                to = other * slabs + s if inside else b * slabs + (s ^ 1)
                pairs.append((b * slabs + s, to))
        return lax.ppermute(x, ("box", "slab"), pairs)

    whole = pressure_now.shape
    half = (count,) + whole[:3] + (LANES,)
    now, prev, cour, cells, planes, edges, za, zb, vals, xa, xb = pl.pallas_call(
        functools.partial(pack_kernel, slots, slabs),
        out_shape=(
            inner(*half),
            inner(*half),
            inner(count, width_x, width_z, LANES),
            inner(*surface_cells.shape, dtype=jnp.int32),
            inner(members, width_z, LANES),
            inner(2 * members, LANES),
            inner(span_z, depth_y),
            inner(span_z + value_rows, depth_y),
            inner(value_rows, depth_y),
            inner(span_x, depth_y),
            inner(span_x, depth_y),
        ),
        in_specs=[SMEM] + [HBM] * 8,
        out_specs=(VMEM,) * 11,
        scratch_shapes=[
            pltpu.SMEM(member_ids.shape, jnp.int32),
            pltpu.SMEM(interp_weights.shape, F32),
            pltpu.SMEM(member_profiles.shape, F32),
            pltpu.VMEM((samples, points), F32),
            pltpu.SemaphoreType.DMA((5 + 3 * count,)),
        ],
        compiler_params=PARAMS,
        name="pack",
    )(
        slab_home, *far(member_ids, interp_weights, member_profiles),
        *far(pressure_now, pressure_prev, courant_sq, surface_cells, stored_slabs),
    )

    per_face = surface_cells.shape[1]
    away = zb[span_z:]
    zb = over_slab(zb, pairs_odd(slabs))
    xa = over_box(xa, False)
    xb = over_box(xb, True)
    others = [
        over_slab(vals if k < slabs // 2 else away, [i ^ k for i in range(slabs)])
        for k in range(2, slabs)
        if slabs != 4
    ]
    now, prev, cour, cells, vals, planes, edges = near(
        now, prev, cour, cells, vals, planes, edges
    )
    high_x, high_z = up16(width_x + 2), up16(width_z + 2)
    local, wide, narrow, rows_x, rows_z = near(
        *pl.pallas_call(
            functools.partial(local_kernel, boxes, slabs, total_z),
            out_shape=(
                inner(*half),
                inner(2, depth_y, per_face, dtype=BF16),
                inner(2, high_x, per_face, dtype=BF16),
                inner(high_x, per_face, dtype=BF16),
                inner(3, high_z, per_face, dtype=BF16),
            ),
            in_specs=[VMEM] * 5,
            out_specs=(VMEM,) * 5,
            compiler_params=PARAMS,
            name="local",
        )(planes, cells, now, prev, cour)
    )
    za, zb, xa, xb, *others = near(za, zb, xa, xb, *others)
    za = pl.pallas_call(
        functools.partial(relay_kernel, slabs == 4),
        out_shape=inner(span_z + value_rows, depth_y),
        in_specs=[VMEM] * 4,
        out_specs=VMEM,
        compiler_params=PARAMS,
        name="relay",
    )(za, vals, zb, local)
    ca, cb = pl.pallas_call(
        functools.partial(corner_kernel, members, width_z),
        out_shape=(inner(CORNERS, depth_y),) * 2,
        in_specs=[VMEM] * 3,
        out_specs=(VMEM, VMEM),
        compiler_params=PARAMS,
        name="corner",
    )(xa, xb, *near(za))
    za = over_slab(za, pairs_even(slabs))
    ca = over_slab(ca, pairs_even(slabs))
    cb = over_slab(cb, pairs_odd(slabs))
    za, ca, cb = near(za, ca, cb)

    last, one, nxt, late = pl.pallas_call(
        functools.partial(main_kernel, boxes, slabs, len(others)),
        out_shape=(
            pltpu.HBM(whole, F32), inner(*half), inner(*half), inner(4 * members, depth_y),
        ),
        in_specs=[VMEM] * (14 + len(others)),
        out_specs=(HBM, VMEM, VMEM, VMEM),
        scratch_shapes=[
            inner(2, count, members, width_x, LANES),
            inner(span_x, depth_y),
            inner(span_x, depth_y),
            inner(span_z, depth_y),
            inner(span_z, depth_y),
            inner(value_rows, depth_y),
            inner(steps, high_z, depth_y),
            inner(steps, high_x, depth_y),
            pltpu.SemaphoreType.DMA((count * members,)),
        ],
        compiler_params=PARAMS,
        name="main",
    )(
        planes, edges, wide, narrow, rows_x, rows_z, now, local, cour,
        vals, za, zb, xa, xb, *others,
    )
    return pl.pallas_call(
        functools.partial(fix_kernel, boxes, slabs),
        out_shape=(pltpu.HBM(whole, F32),) * 2,
        in_specs=[VMEM] * 5 + [HBM],
        out_specs=(HBM, HBM),
        input_output_aliases={5: 1},
        scratch_shapes=[
            inner(count, 2, members, width_z, LANES),
            pltpu.SemaphoreType.DMA((4 * count * members,)),
        ],
        compiler_params=PARAMS,
        name="fix",
    )(ca, cb, *near(one, nxt, late), *far(last))


def solution(mesh):
    in_specs = (
        P("ens", "box", "slab", None),
        P("ens", "box", "slab", None),
        P("box", "slab", None),
        P(),
        P("ens"),
        P("slab", None, None),
        P("ens"),
        P(),
        P(),
    )
    out_specs = (P("ens", "box", "slab", None), P("ens", "box", "slab", None))
    boxes, slabs = mesh.shape["box"], mesh.shape["slab"]
    return jax.shard_map(
        functools.partial(on_device, boxes, slabs),
        mesh=mesh,
        in_specs=in_specs,
        out_specs=out_specs,
        check_vma=False,
    )
```

```python
import functools

import jax
import jax.numpy as jnp
from jax import lax
from jax.experimental import pallas as pl
from jax.experimental.pallas import tpu as pltpu
from jax.sharding import PartitionSpec as P


F32 = jnp.float32
BF16 = jnp.bfloat16
VMEM = pl.BlockSpec(memory_space=pltpu.VMEM)
SMEM = pl.BlockSpec(memory_space=pltpu.SMEM)
HBM = pl.BlockSpec(memory_space=pl.ANY)
CORNERS = 8
VALUE_FACES = 4
PARAMS = pltpu.CompilerParams(vmem_limit_bytes=16 * 1024 * 1024)


LANES = 128
STRIP = 8


def rows_of(shape, axis):
    return lax.broadcasted_iota(jnp.int32, shape, axis)


def up16(n):
    return (n + 15) // 16 * 16


def beside_y(tiles):
    lane = rows_of(tiles[0].shape, 1)
    right = [pltpu.roll(t, 1, 1) for t in tiles]
    left = [pltpu.roll(t, LANES - 1, 1) for t in tiles]
    before = [0.0] + right[:-1]
    after = left[1:] + [0.0]
    return [
        jnp.where(lane == 0, b, r) + jnp.where(lane == LANES - 1, a, l)
        for b, r, l, a in zip(before, right, left, after)
    ]


def beside_rows(tile, low, high):
    strips = [tile[i : i + STRIP] for i in range(0, tile.shape[0], STRIP)]
    row = rows_of(strips[0].shape, 0)
    down = [pltpu.roll(t, 1, 0) for t in strips]
    up = [pltpu.roll(t, STRIP - 1, 0) for t in strips]
    below = [low] + down[:-1]
    above = up[1:] + [high]
    sums = [
        jnp.where(row == 0, b, d) + jnp.where(row == STRIP - 1, a, u)
        for b, d, u, a in zip(below, down, up, above)
    ]
    return jnp.concatenate(sums, axis=0)


def halves(ref):
    return range(ref.shape[0])


def lanes(h):
    return slice(h * LANES, (h + 1) * LANES)


def depth_rows(ref, z, *lead):
    width_x, width_z = ref.shape[-3:-1]
    count = 1
    for n in ref.shape[:-3]:
        count = count * n
    at = 0
    for i, n in zip(lead, ref.shape[:-3]):
        at = at * n + i
    flat = ref.reshape(count * width_x * width_z, LANES)
    return flat[pl.ds(at * width_x * width_z + z, width_x, stride=width_z), :]


def pack_kernel(
    slots, depth_devices, home, ids_in, weights_in, prof_in, now_in, prev_in, cour_in, cells_in, slabs,
    now, prev, cour, cells, planes, edges, za, zb, vals, xa, xb, ids, weights, prof, block, sems,
):
    _, members, width_x, width_z, _ = now.shape
    steps, samples = weights.shape
    box, slab = lax.axis_index("box"), lax.axis_index("slab")
    total_z = prof.shape[1]
    pairs = [(ids_in, ids), (prof_in, prof), (weights_in, weights)]
    for h in halves(now):
        pairs.append((cour_in.at[:, :, pl.ds(h * LANES, LANES)], cour.at[h]))
    groups = [len(pairs)]
    for h in halves(now):
        pairs.append((now_in.at[:, :, :, pl.ds(h * LANES, LANES)], now.at[h]))
        pairs.append((prev_in.at[:, :, :, pl.ds(h * LANES, LANES)], prev.at[h]))
    groups = groups + [len(pairs)] * members
    fields = len(pairs)
    pairs.append((slabs.at[lax.rem(home[0], slots)], block))
    pairs.append((cells_in, cells))
    loads = [pltpu.make_async_copy(a, b, sems.at[i]) for i, (a, b) in enumerate(pairs)]
    for load in loads:
        load.start()
    start_z = slab * width_z
    for load in loads[:3]:
        load.wait()
    row = rows_of((width_z, LANES), 0)
    for m in range(members):
        plane = jnp.zeros((width_z, LANES), F32)
        for z in range(width_z):
            plane = jnp.where(row == z, 1.0 + prof[ids[m], start_z + z], plane)
        planes[m] = plane
        for s, z in ((0, start_z - 1), (1, start_z + width_z)):
            beyond = 1.0 + prof[ids[m], jnp.clip(z, 0, total_z - 1)]
            edges[2 * m + s : 2 * m + s + 1] = jnp.full((1, LANES), beyond, F32)
    owner = slab == home[0] // slots
    width = vals.shape[1]
    sample = rows_of((samples, width), 0)
    columns = []
    for t in range(steps):
        column = jnp.zeros((samples, width), F32)
        for k in range(samples):
            column = jnp.where(sample == k, weights[t, k], column)
        columns.append(jnp.where(owner, column, 0.0))
    zero = jnp.zeros((1, LANES), F32)
    for load in loads[3 : groups[0]]:
        load.wait()
    face, side = lax.rem(box, 2), lax.rem(slab, 2)

    def local_step(heres, prevs, inners, coefs):
        near = beside_y(heres)
        out = []
        for here, prev_here, inner, coef, n in zip(heres, prevs, inners, coefs, near):
            around = n + beside_rows(here, zero, zero) + inner
            out.append(2.0 * here - prev_here + coef * (around - 6.0 * here))
        return out

    sides = (
        (za, zb, side == 0, width_x, (0, 1), (width_z - 1, width_z - 2), True),
        (xa, xb, face == 0, width_z, (0, 1), (width_x - 1, width_x - 2), False),
    )

    def plane(ref, at, deep, *lead):
        return depth_rows(ref, at, *lead) if deep else ref[lead + (at,)]

    def put(a, b, at_high, at, h, low, high):
        n = low.shape[0]
        a[at * n : (at + 1) * n, lanes(h)] = jnp.where(at_high, high, low)
        b[at * n : (at + 1) * n, lanes(h)] = jnp.where(at_high, low, high)

    for a, b, at_high, _, (low, _), (high, _), deep in sides:
        for h in halves(now):
            courant = [plane(cour, at, deep, h) for at in (low, high)]
            put(a, b, at_high, 2 * members, h, *courant)
    for m in range(members):
        for load in loads[groups[m] : groups[m + 1]]:
            load.wait()
        for a, b, at_high, _, low, high, deep in sides:
            ends = []
            for at, inner in (low, high):
                heres, prevs, inners = (
                    [plane(ref, i, deep, h, m) for h in halves(now)]
                    for ref, i in ((now, at), (prev, at), (now, inner))
                )
                scale = 1.0 + prof[ids[m], start_z + at] if deep else planes[m]
                coefs = [plane(cour, at, deep, h) * scale for h in halves(now)]
                ends.append((heres, local_step(heres, prevs, inners, coefs)))
            for h in halves(now):
                put(a, b, at_high, m, h, ends[0][0][h], ends[1][0][h])
                put(a, b, at_high, members + m, h, ends[0][1][h], ends[1][1][h])
    per_face = cells.shape[1]
    per = per_face // width
    low_half = slab < depth_devices // 2
    tail = (2 * members + 1) * width_x
    loads[fields].wait()
    picks = (
        (0, jnp.where(box == 0, 0, 1), True, True),
        (1, jnp.where(low_half, 2, 3), True, False),
        (1, jnp.where(low_half, 3, 2), False, True),
        (2, 4, True, True),
        (3, 5, True, True),
    )
    for slot, f, for_near, for_far in picks:
        for i in range(per):
            start = pl.multiple_of(f * per_face + i * width, width)
            piece = block[:, pl.ds(start, width)]
            for t in range(steps):
                at = (t * VALUE_FACES + slot) * per + i
                row_value = jnp.sum(columns[t] * piece, axis=0, keepdims=True)
                if for_near:
                    vals[at : at + 1] = row_value
                if for_far:
                    zb[tail + at : tail + at + 1] = row_value
    loads[fields + 1].wait()


def relay_kernel(relay, face, vals, zb, after, za):
    tail = face.shape[0]
    za[:tail] = face[...]
    za[tail:] = vals[...] + zb[tail:] if relay else vals[...]


def corner_kernel(members, width_z, xa, xb, after, ca, cb):
    box, slab = lax.axis_index("box"), lax.axis_index("slab")
    face, side = lax.rem(box, 2), lax.rem(slab, 2)
    for out, last in ((ca, side == 0), (cb, side == 1)):
        for m in range(members):
            lo, hi = m * width_z, (m + 1) * width_z - 1
            a = jnp.where(last, xa[hi : hi + 1], xa[lo : lo + 1])
            b = jnp.where(last, xb[hi : hi + 1], xb[lo : lo + 1])
            out[2 * m : 2 * m + 1] = jnp.where(face == 0, b, a)
            out[2 * m + 1 : 2 * m + 2] = jnp.where(face == 0, a, b)


def split_cell(cell, total_z, depth_y):
    plane = total_z * depth_y
    x = cell // plane
    rest = cell - x * plane
    z = rest // depth_y
    return x, z, rest - z * depth_y


def extended_row(coordinate, start, width):
    d = coordinate - start
    edge = jnp.where(d == -1, width, jnp.where(d == width, width + 1, -1))
    return jnp.where((d >= 0) & (d < width), d, edge)


def one_hot(index, high):
    rows = rows_of((high, index.shape[1]), 0)
    return jnp.where(rows == index, 1.0, 0.0).astype(BF16)


def faces_of(box, slab):
    return jnp.where(box == 0, 0, 1), jnp.where(slab == 0, 2, 3), 4, 5


def local_kernel(
    boxes, slabs, total_z, planes, cells, now, prev, cour, local, wide, narrow, rows_x, rows_z,
):
    count, members, width_x, width_z, _ = now.shape
    depth_y = count * LANES
    box, slab = lax.axis_index("box"), lax.axis_index("slab")
    zero = jnp.zeros((1, LANES), F32)
    for x in range(width_x):
        for m in range(members):
            heres = [now[h, m, x] for h in range(count)]
            near = beside_y(heres)
            for h, here in enumerate(heres):
                around = near[h] + beside_rows(here, zero, zero)
                if x > 0:
                    around = around + now[h, m, x - 1]
                if x < width_x - 1:
                    around = around + now[h, m, x + 1]
                coef = cour[h, x] * planes[m]
                local[h, m, x] = 2.0 * here - prev[h, m, x] + coef * (around - 6.0 * here)
    on_x = (box == 0) | (box == boxes - 1)
    on_z = (slab == 0) | (slab == slabs - 1)
    for i, f in enumerate(faces_of(box, slab)):
        x, z, y = split_cell(cells[pl.ds(f, 1), :], total_z, depth_y)
        x = extended_row(x, box * width_x, width_x)
        z = extended_row(z, slab * width_z, width_z)
        if i == 0:
            rows_z[0] = one_hot(jnp.where(on_x, z, -1), rows_z.shape[1])
            wide[0] = one_hot(y, depth_y)
        elif i == 1:
            rows_x[...] = one_hot(jnp.where(on_z, x, -1), rows_x.shape[0])
            wide[1] = one_hot(y, depth_y)
        else:
            rows_z[i - 1] = one_hot(z, rows_z.shape[1])
            narrow[i - 2] = one_hot(x, narrow.shape[1])


def three_parts(v):
    first = v.astype(BF16)
    rest = v - first.astype(F32)
    second = rest.astype(BF16)
    third = (rest - second.astype(F32)).astype(BF16)
    return first, second, third


def face_source(values, rows, rhs, width):
    heights = [rows.shape[0]] + [up16(width)] * (len(values) - 1)
    parts = []
    for v, high in zip(values, heights):
        for part in three_parts(v):
            parts.append(rows[:high] * jnp.broadcast_to(part, (high, part.shape[1])))
    out = lax.dot_general(
        jnp.concatenate(parts, axis=0), rhs, (((1,), (1,)), ((), ())), preferred_element_type=F32
    )
    sums, at = [], 0
    for high in heights:
        one, two, three = (out[at + i * high : at + (i + 1) * high] for i in range(3))
        sums.append((three + two) + one)
        at = at + 3 * high
    return sums


def main_kernel(
    boxes, slabs, received, planes, edges, wide, narrow, rows_x, rows_z, now, local, cour,
    vals, za, zb, xa, xb, *rest,
):
    others, rest = rest[:received], rest[received:]
    last, one, nxt, late, hz, xlo, xhi, zlo, zhi, value, xsrc, zsrc, sems = rest
    count, members, width_x, width_z, _ = now.shape
    depth_y = count * LANES
    box, slab = lax.axis_index("box"), lax.axis_index("slab")
    face, side = lax.rem(box, 2), lax.rem(slab, 2)
    span_z = (2 * members + 1) * width_x
    low, high = (box > 0, slab > 0), (box < boxes - 1, slab < slabs - 1)
    xlo[...] = jnp.where(low[0], jnp.where(face == 0, xb[...], xa[...]), 0.0)
    xhi[...] = jnp.where(high[0], jnp.where(face == 0, xa[...], xb[...]), 0.0)
    zlo[...] = jnp.where(low[1], jnp.where(side == 0, zb[:span_z], za[:span_z]), 0.0)
    zhi[...] = jnp.where(high[1], jnp.where(side == 0, za[:span_z], zb[:span_z]), 0.0)
    total = vals[...] + za[span_z:]
    if slabs == 4:
        total = total + zb[span_z:]
    for other in others:
        total = total + other[...]
    value[...] = total

    steps = xsrc.shape[0]
    chunks = value.shape[0] // steps
    per = wide.shape[2] // depth_y

    def of_face(f):
        vs = []
        for t in range(steps):
            pieces = [value[t * chunks + f * per + i : t * chunks + f * per + i + 1, :] for i in range(per)]
            vs.append(jnp.concatenate(pieces, axis=1))
        return vs

    for t, s in enumerate(face_source(of_face(0), rows_z[0], wide[0], width_z)):
        xsrc[t, : s.shape[0]] = s
    for t, s in enumerate(face_source(of_face(1), rows_x[...], wide[1], width_x)):
        zsrc[t, : s.shape[0]] = s
    ys = [
        face_source(of_face(2 + i), rows_z[1 + i], narrow[i], width_z) for i in range(2)
    ]

    lane = rows_of((width_z, LANES), 1)
    row = rows_of((width_z, LANES), 0)
    row_of_z = jnp.where(slab == 0, 0, jnp.where(slab == slabs - 1, width_z - 1, -1))
    row_of_x = jnp.where(box == 0, 0, jnp.where(box == boxes - 1, width_x - 1, -1))

    def plane_source(t, x):
        out = []
        for h in range(count):
            part = jnp.where(row == row_of_z, zsrc[t, x : x + 1, lanes(h)], 0.0)
            if h == 0:
                part = part + jnp.where(lane == 0, ys[0][t][:width_z, x : x + 1], 0.0)
            if h == count - 1:
                part = part + jnp.where(lane == LANES - 1, ys[1][t][:width_z, x : x + 1], 0.0)
            if x in (0, width_x - 1):
                part = part + jnp.where(row_of_x == x, xsrc[t, :width_z, lanes(h)], 0.0)
            out.append(part)
        return out

    lane_x = rows_of((width_x, LANES), 1)
    row_x = rows_of((width_x, LANES), 0)
    turned = [jnp.transpose(y[0]) for y in ys]

    def row_source(z):
        out = []
        for h in range(count):
            part = jnp.where(row_x == row_of_x, xsrc[0, z : z + 1, lanes(h)], 0.0)
            if h == 0:
                part = part + jnp.where(lane_x == 0, turned[0][:width_x, z : z + 1], 0.0)
            if h == count - 1:
                part = part + jnp.where(lane_x == LANES - 1, turned[1][:width_x, z : z + 1], 0.0)
            out.append(part)
        return out

    side_x, side_z = 2 * members * width_z, 2 * members * width_x
    halo_x, coef_x, coef_z = {}, {}, {}
    for s, (ref, x) in enumerate(((xlo, 0), (xhi, width_x - 1))):
        source = plane_source(0, width_x + s)
        for m in range(members):
            for h in range(count):
                coef = ref[side_x:, lanes(h)] * planes[m]
                base = ref[(members + m) * width_z : (members + m + 1) * width_z, lanes(h)]
                halo_x[s, m, h] = base + coef * now[h, m, x] + source[h]
                coef_x[s, m, h] = coef
    for s, (ref, z) in enumerate(((zlo, 0), (zhi, width_z - 1))):
        source = row_source(width_z + s)
        for m in range(members):
            for h in range(count):
                coef = ref[side_z:, lanes(h)] * edges[2 * m + s : 2 * m + s + 1]
                base = ref[(members + m) * width_x : (members + m + 1) * width_x, lanes(h)]
                hz[s, h, m] = base + coef * depth_rows(now, z, h, m) + source[h]
                coef_z[s, m, h] = coef
    sources = [plane_source(0, x) for x in range(width_x)]
    copies = []
    for m in range(members):
        for x in range(width_x):
            at = m * width_x + x
            for h in range(count):
                low_row, high_row = zlo[at : at + 1, lanes(h)], zhi[at : at + 1, lanes(h)]
                more = jnp.where(row == 0, low_row, jnp.where(row == width_z - 1, high_row, 0.0))
                if x == 0:
                    more = more + xlo[m * width_z : (m + 1) * width_z, lanes(h)]
                if x == width_x - 1:
                    more = more + xhi[m * width_z : (m + 1) * width_z, lanes(h)]
                one[h, m, x] = local[h, m, x] + (cour[h, x] * planes[m]) * more + sources[x][h]
        for h in range(count):
            copies.append(
                pltpu.make_async_copy(
                    one.at[h, m], last.at[m, :, :, pl.ds(h * LANES, LANES)], sems.at[len(copies)]
                )
            )
            copies[-1].start()
    for x in range(width_x):
        source = plane_source(1, x)
        for m in range(members):
            heres = [one[h, m, x] for h in range(count)]
            near = beside_y(heres)
            for h, here in enumerate(heres):
                rows = beside_rows(here, hz[0, h, m, x : x + 1], hz[1, h, m, x : x + 1])
                around = near[h] + rows
                around = around + (one[h, m, x - 1] if x > 0 else halo_x[0, m, h])
                around = around + (one[h, m, x + 1] if x < width_x - 1 else halo_x[1, m, h])
                coef = cour[h, x] * planes[m]
                nxt[h, m, x] = 2.0 * here - now[h, m, x] + coef * (around - 6.0 * here) + source[h]
                if x in (0, width_x - 1):
                    s = 0 if x == 0 else 1
                    for e, z in ((0, 0), (1, width_z - 1)):
                        beyond = coef_z[e, m, h][x : x + 1] + coef_x[s, m, h][z : z + 1]
                        at = 2 * (members * e + m) + s
                        late[at : at + 1, lanes(h)] = coef[z : z + 1] * beyond
    for copy in copies:
        copy.wait()


def fix_kernel(boxes, slabs, ca, cb, one, nxt, late, first, out, last, done, sems):
    count, members, width_x, width_z, _ = nxt.shape
    box, slab = lax.axis_index("box"), lax.axis_index("slab")
    side = lax.rem(slab, 2)
    open_x = (box > 0, box < boxes - 1)
    open_z = (slab > 0, slab < slabs - 1)
    row = rows_of((width_z, LANES), 0)
    copies = []

    def send(source, target):
        copies.append(pltpu.make_async_copy(source, target, sems.at[len(copies)]))
        copies[-1].start()

    for h in range(count):
        inside = pl.ds(1, width_x - 2)
        send(nxt.at[h, :, inside], out.at[:, inside, :, pl.ds(h * LANES, LANES)])
    for h in range(count):
        for s, x in ((0, 0), (1, width_x - 1)):
            for m in range(members):
                at = 2 * m + s
                add = 0.0
                for e, z in ((0, 0), (1, width_z - 1)):
                    got = jnp.where(
                        side == e, cb[at : at + 1, lanes(h)], ca[at : at + 1, lanes(h)]
                    )
                    got = jnp.where(open_x[s] & open_z[e], got, 0.0)
                    k = 2 * members * e + at
                    add = jnp.where(row == z, late[k : k + 1, lanes(h)] * got, add)
                done[h, s, m] = nxt[h, m, x] + add
            send(done.at[h, s], out.at[:, x, :, pl.ds(h * LANES, LANES)])
    for copy in copies:
        copy.wait()


def pairs_even(n):
    return [i ^ 1 for i in range(n)]


def pairs_odd(n):
    return [(i + 1) % n if i % 2 else (i - 1) % n for i in range(n)]


def on_device(
    boxes, slabs, pressure_now, pressure_prev, courant_sq, member_profiles, member_ids,
    stored_slabs, slab_home, interp_weights, surface_cells,
):
    members, width_x, width_z, depth_y = pressure_now.shape
    slots, samples, points = stored_slabs.shape
    steps = interp_weights.shape[0]
    total_z = width_z * slabs
    value_rows = steps * VALUE_FACES * surface_cells.shape[1] // depth_y
    span_x = (2 * members + 1) * width_z
    span_z = (2 * members + 1) * width_x
    count = depth_y // LANES

    def inner(*dims, dtype=F32):
        return pltpu.VMEM(dims, dtype)

    def far(*arrays):
        return [pltpu.with_memory_space_constraint(a, pltpu.HBM) for a in arrays]

    def near(*arrays):
        return [pltpu.with_memory_space_constraint(a, pltpu.VMEM) for a in arrays]

    def over_slab(x, partner):
        return lax.ppermute(x, "slab", list(enumerate(partner)))

    def over_box(x, odd):
        pairs = []
        for b in range(boxes):
            other = b ^ 1
            if odd:
                other = b + 1 if b % 2 else b - 1
            for s in range(slabs):
                inside = 0 <= other < boxes
                to = other * slabs + s if inside else b * slabs + (s ^ 1)
                pairs.append((b * slabs + s, to))
        return lax.ppermute(x, ("box", "slab"), pairs)

    whole = pressure_now.shape
    half = (count,) + whole[:3] + (LANES,)
    now, prev, cour, cells, planes, edges, za, zb, vals, xa, xb = pl.pallas_call(
        functools.partial(pack_kernel, slots, slabs),
        out_shape=(
            inner(*half),
            inner(*half),
            inner(count, width_x, width_z, LANES),
            inner(*surface_cells.shape, dtype=jnp.int32),
            inner(members, width_z, LANES),
            inner(2 * members, LANES),
            inner(span_z, depth_y),
            inner(span_z + value_rows, depth_y),
            inner(value_rows, depth_y),
            inner(span_x, depth_y),
            inner(span_x, depth_y),
        ),
        in_specs=[SMEM] + [HBM] * 8,
        out_specs=(VMEM,) * 11,
        scratch_shapes=[
            pltpu.SMEM(member_ids.shape, jnp.int32),
            pltpu.SMEM(interp_weights.shape, F32),
            pltpu.SMEM(member_profiles.shape, F32),
            pltpu.VMEM((samples, points), F32),
            pltpu.SemaphoreType.DMA((5 + 3 * count,)),
        ],
        compiler_params=PARAMS,
        name="pack",
    )(
        slab_home, *far(member_ids, interp_weights, member_profiles),
        *far(pressure_now, pressure_prev, courant_sq, surface_cells, stored_slabs),
    )

    per_face = surface_cells.shape[1]
    away = zb[span_z:]
    zb = over_slab(zb, pairs_odd(slabs))
    xa = over_box(xa, False)
    xb = over_box(xb, True)
    others = [
        over_slab(vals if k < slabs // 2 else away, [i ^ k for i in range(slabs)])
        for k in range(2, slabs)
        if slabs != 4
    ]
    now, prev, cour, cells, vals, planes, edges = near(
        now, prev, cour, cells, vals, planes, edges
    )
    high_x, high_z = up16(width_x + 2), up16(width_z + 2)
    local, wide, narrow, rows_x, rows_z = near(
        *pl.pallas_call(
            functools.partial(local_kernel, boxes, slabs, total_z),
            out_shape=(
                inner(*half),
                inner(2, depth_y, per_face, dtype=BF16),
                inner(2, high_x, per_face, dtype=BF16),
                inner(high_x, per_face, dtype=BF16),
                inner(3, high_z, per_face, dtype=BF16),
            ),
            in_specs=[VMEM] * 5,
            out_specs=(VMEM,) * 5,
            compiler_params=PARAMS,
            name="local",
        )(planes, cells, now, prev, cour)
    )
    za, zb, xa, xb, *others = near(za, zb, xa, xb, *others)
    za = pl.pallas_call(
        functools.partial(relay_kernel, slabs == 4),
        out_shape=inner(span_z + value_rows, depth_y),
        in_specs=[VMEM] * 4,
        out_specs=VMEM,
        compiler_params=PARAMS,
        name="relay",
    )(za, vals, zb, local)
    ca, cb = pl.pallas_call(
        functools.partial(corner_kernel, members, width_z),
        out_shape=(inner(CORNERS, depth_y),) * 2,
        in_specs=[VMEM] * 3,
        out_specs=(VMEM, VMEM),
        compiler_params=PARAMS,
        name="corner",
    )(xa, xb, *near(za))
    za = over_slab(za, pairs_even(slabs))
    ca = over_slab(ca, pairs_even(slabs))
    cb = over_slab(cb, pairs_odd(slabs))
    za, ca, cb = near(za, ca, cb)

    last, one, nxt, late = pl.pallas_call(
        functools.partial(main_kernel, boxes, slabs, len(others)),
        out_shape=(
            pltpu.HBM(whole, F32), inner(*half), inner(*half), inner(4 * members, depth_y),
        ),
        in_specs=[VMEM] * (14 + len(others)),
        out_specs=(HBM, VMEM, VMEM, VMEM),
        scratch_shapes=[
            inner(2, count, members, width_x, LANES),
            inner(span_x, depth_y),
            inner(span_x, depth_y),
            inner(span_z, depth_y),
            inner(span_z, depth_y),
            inner(value_rows, depth_y),
            inner(steps, high_z, depth_y),
            inner(steps, high_x, depth_y),
            pltpu.SemaphoreType.DMA((count * members,)),
        ],
        compiler_params=PARAMS,
        name="main",
    )(
        planes, edges, wide, narrow, rows_x, rows_z, now, local, cour,
        vals, za, zb, xa, xb, *others,
    )
    return pl.pallas_call(
        functools.partial(fix_kernel, boxes, slabs),
        out_shape=(pltpu.HBM(whole, F32),) * 2,
        in_specs=[VMEM] * 5 + [HBM],
        out_specs=(HBM, HBM),
        input_output_aliases={5: 1},
        scratch_shapes=[
            inner(count, 2, members, width_z, LANES),
            pltpu.SemaphoreType.DMA((3 * count,)),
        ],
        compiler_params=PARAMS,
        name="fix",
    )(ca, cb, *near(one, nxt, late), *far(last))


def solution(mesh):
    in_specs = (
        P("ens", "box", "slab", None),
        P("ens", "box", "slab", None),
        P("box", "slab", None),
        P(),
        P("ens"),
        P("slab", None, None),
        P("ens"),
        P(),
        P(),
    )
    out_specs = (P("ens", "box", "slab", None), P("ens", "box", "slab", None))
    boxes, slabs = mesh.shape["box"], mesh.shape["slab"]
    return jax.shard_map(
        functools.partial(on_device, boxes, slabs),
        mesh=mesh,
        in_specs=in_specs,
        out_specs=out_specs,
        check_vma=False,
    )
```

```python
import functools

import jax
import jax.numpy as jnp
from jax import lax
from jax.experimental import pallas as pl
from jax.experimental.pallas import tpu as pltpu
from jax.sharding import PartitionSpec as P


F32 = jnp.float32
BF16 = jnp.bfloat16
VMEM = pl.BlockSpec(memory_space=pltpu.VMEM)
SMEM = pl.BlockSpec(memory_space=pltpu.SMEM)
HBM = pl.BlockSpec(memory_space=pl.ANY)
CORNERS = 8
VALUE_FACES = 4
PARAMS = pltpu.CompilerParams(vmem_limit_bytes=16 * 1024 * 1024)


LANES = 128
STRIP = 8


def rows_of(shape, axis):
    return lax.broadcasted_iota(jnp.int32, shape, axis)


def up16(n):
    return (n + 15) // 16 * 16


def beside_y(tiles):
    lane = rows_of(tiles[0].shape, 1)
    right = [pltpu.roll(t, 1, 1) for t in tiles]
    left = [pltpu.roll(t, LANES - 1, 1) for t in tiles]
    before = [0.0] + right[:-1]
    after = left[1:] + [0.0]
    return [
        jnp.where(lane == 0, b, r) + jnp.where(lane == LANES - 1, a, l)
        for b, r, l, a in zip(before, right, left, after)
    ]


def beside_rows(tile, low, high):
    strips = [tile[i : i + STRIP] for i in range(0, tile.shape[0], STRIP)]
    row = rows_of(strips[0].shape, 0)
    down = [pltpu.roll(t, 1, 0) for t in strips]
    up = [pltpu.roll(t, STRIP - 1, 0) for t in strips]
    below = [low] + down[:-1]
    above = up[1:] + [high]
    sums = [
        jnp.where(row == 0, b, d) + jnp.where(row == STRIP - 1, a, u)
        for b, d, u, a in zip(below, down, up, above)
    ]
    return jnp.concatenate(sums, axis=0)


def halves(ref):
    return range(ref.shape[0])


def lanes(h):
    return slice(h * LANES, (h + 1) * LANES)


def depth_rows(ref, z, *lead):
    width_x, width_z = ref.shape[-3:-1]
    count = 1
    for n in ref.shape[:-3]:
        count = count * n
    at = 0
    for i, n in zip(lead, ref.shape[:-3]):
        at = at * n + i
    flat = ref.reshape(count * width_x * width_z, LANES)
    return flat[pl.ds(at * width_x * width_z + z, width_x, stride=width_z), :]


def pack_kernel(
    slots, depth_devices, home, ids_in, weights_in, prof_in, now_in, prev_in, cour_in, cells_in, slabs,
    now, prev, cour, cells, planes, edges, za, zb, vals, xa, xb, ids, weights, prof, block, sems,
):
    _, members, width_x, width_z, _ = now.shape
    steps, samples = weights.shape
    box, slab = lax.axis_index("box"), lax.axis_index("slab")
    total_z = prof.shape[1]
    pairs = [(ids_in, ids), (prof_in, prof), (weights_in, weights)]
    for h in halves(now):
        pairs.append((cour_in.at[:, :, pl.ds(h * LANES, LANES)], cour.at[h]))
    groups = [len(pairs)]
    for h in halves(now):
        pairs.append((now_in.at[:, :, :, pl.ds(h * LANES, LANES)], now.at[h]))
        pairs.append((prev_in.at[:, :, :, pl.ds(h * LANES, LANES)], prev.at[h]))
    groups = groups + [len(pairs)] * members
    fields = len(pairs)
    pairs.append((slabs.at[lax.rem(home[0], slots)], block))
    pairs.append((cells_in, cells))
    loads = [pltpu.make_async_copy(a, b, sems.at[i]) for i, (a, b) in enumerate(pairs)]
    owner = slab == home[0] // slots
    for load in loads[:fields]:
        load.start()

    @pl.when(owner)
    def _():
        loads[fields].start()

    loads[fields + 1].start()
    start_z = slab * width_z
    for load in loads[:3]:
        load.wait()
    row = rows_of((width_z, LANES), 0)
    for m in range(members):
        plane = jnp.zeros((width_z, LANES), F32)
        for z in range(width_z):
            plane = jnp.where(row == z, 1.0 + prof[ids[m], start_z + z], plane)
        planes[m] = plane
        for s, z in ((0, start_z - 1), (1, start_z + width_z)):
            beyond = 1.0 + prof[ids[m], jnp.clip(z, 0, total_z - 1)]
            edges[2 * m + s : 2 * m + s + 1] = jnp.full((1, LANES), beyond, F32)
    width = vals.shape[1]
    sample = rows_of((samples, width), 0)
    columns = []
    for t in range(steps):
        column = jnp.zeros((samples, width), F32)
        for k in range(samples):
            column = jnp.where(sample == k, weights[t, k], column)
        columns.append(column)
    zero = jnp.zeros((1, LANES), F32)
    for load in loads[3 : groups[0]]:
        load.wait()
    face, side = lax.rem(box, 2), lax.rem(slab, 2)

    def local_step(heres, prevs, inners, coefs):
        near = beside_y(heres)
        out = []
        for here, prev_here, inner, coef, n in zip(heres, prevs, inners, coefs, near):
            around = n + beside_rows(here, zero, zero) + inner
            out.append(2.0 * here - prev_here + coef * (around - 6.0 * here))
        return out

    sides = (
        (za, zb, side == 0, width_x, (0, 1), (width_z - 1, width_z - 2), True),
        (xa, xb, face == 0, width_z, (0, 1), (width_x - 1, width_x - 2), False),
    )

    def plane(ref, at, deep, *lead):
        return depth_rows(ref, at, *lead) if deep else ref[lead + (at,)]

    def put(a, b, at_high, at, h, low, high):
        n = low.shape[0]
        a[at * n : (at + 1) * n, lanes(h)] = jnp.where(at_high, high, low)
        b[at * n : (at + 1) * n, lanes(h)] = jnp.where(at_high, low, high)

    for a, b, at_high, _, (low, _), (high, _), deep in sides:
        for h in halves(now):
            courant = [plane(cour, at, deep, h) for at in (low, high)]
            put(a, b, at_high, 2 * members, h, *courant)
    for m in range(members):
        for load in loads[groups[m] : groups[m + 1]]:
            load.wait()
        for a, b, at_high, _, low, high, deep in sides:
            ends = []
            for at, inner in (low, high):
                heres, prevs, inners = (
                    [plane(ref, i, deep, h, m) for h in halves(now)]
                    for ref, i in ((now, at), (prev, at), (now, inner))
                )
                scale = 1.0 + prof[ids[m], start_z + at] if deep else planes[m]
                coefs = [plane(cour, at, deep, h) * scale for h in halves(now)]
                ends.append((heres, local_step(heres, prevs, inners, coefs)))
            for h in halves(now):
                put(a, b, at_high, m, h, ends[0][0][h], ends[1][0][h])
                put(a, b, at_high, members + m, h, ends[0][1][h], ends[1][1][h])
    per_face = cells.shape[1]
    per = per_face // width
    low_half = slab < depth_devices // 2
    tail = (2 * members + 1) * width_x
    picks = (
        (0, jnp.where(box == 0, 0, 1), True, True),
        (1, jnp.where(low_half, 2, 3), True, False),
        (1, jnp.where(low_half, 3, 2), False, True),
        (2, 4, True, True),
        (3, 5, True, True),
    )

    @pl.when(owner)
    def _():
        loads[fields].wait()
        for slot, f, for_near, for_far in picks:
            for i in range(per):
                start = pl.multiple_of(f * per_face + i * width, width)
                piece = block[:, pl.ds(start, width)]
                for t in range(steps):
                    at = (t * VALUE_FACES + slot) * per + i
                    row_value = jnp.sum(columns[t] * piece, axis=0, keepdims=True)
                    if for_near:
                        vals[at : at + 1] = row_value
                    if for_far:
                        zb[tail + at : tail + at + 1] = row_value

    @pl.when(~owner)
    def _():
        vals[...] = jnp.zeros(vals.shape, F32)
        zb[tail:] = jnp.zeros(vals.shape, F32)

    loads[fields + 1].wait()


def relay_kernel(relay, face, vals, zb, after, za):
    tail = face.shape[0]
    za[:tail] = face[...]
    za[tail:] = vals[...] + zb[tail:] if relay else vals[...]


def corner_kernel(members, width_z, xa, xb, after, ca, cb):
    box, slab = lax.axis_index("box"), lax.axis_index("slab")
    face, side = lax.rem(box, 2), lax.rem(slab, 2)
    for out, last in ((ca, side == 0), (cb, side == 1)):
        for m in range(members):
            lo, hi = m * width_z, (m + 1) * width_z - 1
            a = jnp.where(last, xa[hi : hi + 1], xa[lo : lo + 1])
            b = jnp.where(last, xb[hi : hi + 1], xb[lo : lo + 1])
            out[2 * m : 2 * m + 1] = jnp.where(face == 0, b, a)
            out[2 * m + 1 : 2 * m + 2] = jnp.where(face == 0, a, b)


def split_cell(cell, total_z, depth_y):
    plane = total_z * depth_y
    x = cell // plane
    rest = cell - x * plane
    z = rest // depth_y
    return x, z, rest - z * depth_y


def extended_row(coordinate, start, width):
    d = coordinate - start
    edge = jnp.where(d == -1, width, jnp.where(d == width, width + 1, -1))
    return jnp.where((d >= 0) & (d < width), d, edge)


def one_hot(index, high):
    rows = rows_of((high, index.shape[1]), 0)
    return jnp.where(rows == index, 1.0, 0.0).astype(BF16)


def faces_of(box, slab):
    return jnp.where(box == 0, 0, 1), jnp.where(slab == 0, 2, 3), 4, 5


def local_kernel(
    boxes, slabs, total_z, planes, cells, now, prev, cour, local, wide, narrow, rows_x, rows_z,
):
    count, members, width_x, width_z, _ = now.shape
    depth_y = count * LANES
    box, slab = lax.axis_index("box"), lax.axis_index("slab")
    zero = jnp.zeros((1, LANES), F32)
    for x in range(width_x):
        for m in range(members):
            heres = [now[h, m, x] for h in range(count)]
            near = beside_y(heres)
            for h, here in enumerate(heres):
                around = near[h] + beside_rows(here, zero, zero)
                if x > 0:
                    around = around + now[h, m, x - 1]
                if x < width_x - 1:
                    around = around + now[h, m, x + 1]
                coef = cour[h, x] * planes[m]
                local[h, m, x] = 2.0 * here - prev[h, m, x] + coef * (around - 6.0 * here)
    on_x = (box == 0) | (box == boxes - 1)
    on_z = (slab == 0) | (slab == slabs - 1)
    for i, f in enumerate(faces_of(box, slab)):
        x, z, y = split_cell(cells[pl.ds(f, 1), :], total_z, depth_y)
        x = extended_row(x, box * width_x, width_x)
        z = extended_row(z, slab * width_z, width_z)
        if i == 0:
            rows_z[0] = one_hot(jnp.where(on_x, z, -1), rows_z.shape[1])
            wide[0] = one_hot(y, depth_y)
        elif i == 1:
            rows_x[...] = one_hot(jnp.where(on_z, x, -1), rows_x.shape[0])
            wide[1] = one_hot(y, depth_y)
        else:
            rows_z[i - 1] = one_hot(z, rows_z.shape[1])
            narrow[i - 2] = one_hot(x, narrow.shape[1])


def three_parts(v):
    first = v.astype(BF16)
    rest = v - first.astype(F32)
    second = rest.astype(BF16)
    third = (rest - second.astype(F32)).astype(BF16)
    return first, second, third


def face_source(values, rows, rhs, width):
    heights = [rows.shape[0]] + [up16(width)] * (len(values) - 1)
    parts = []
    for v, high in zip(values, heights):
        for part in three_parts(v):
            parts.append(rows[:high] * jnp.broadcast_to(part, (high, part.shape[1])))
    out = lax.dot_general(
        jnp.concatenate(parts, axis=0), rhs, (((1,), (1,)), ((), ())), preferred_element_type=F32
    )
    sums, at = [], 0
    for high in heights:
        one, two, three = (out[at + i * high : at + (i + 1) * high] for i in range(3))
        sums.append((three + two) + one)
        at = at + 3 * high
    return sums


def main_kernel(
    boxes, slabs, received, planes, edges, wide, narrow, rows_x, rows_z, now, local, cour,
    vals, za, zb, xa, xb, *rest,
):
    others, rest = rest[:received], rest[received:]
    last, one, nxt, late, hz, xlo, xhi, zlo, zhi, value, xsrc, zsrc, sems = rest
    count, members, width_x, width_z, _ = now.shape
    depth_y = count * LANES
    box, slab = lax.axis_index("box"), lax.axis_index("slab")
    face, side = lax.rem(box, 2), lax.rem(slab, 2)
    span_z = (2 * members + 1) * width_x
    low, high = (box > 0, slab > 0), (box < boxes - 1, slab < slabs - 1)
    xlo[...] = jnp.where(low[0], jnp.where(face == 0, xb[...], xa[...]), 0.0)
    xhi[...] = jnp.where(high[0], jnp.where(face == 0, xa[...], xb[...]), 0.0)
    zlo[...] = jnp.where(low[1], jnp.where(side == 0, zb[:span_z], za[:span_z]), 0.0)
    zhi[...] = jnp.where(high[1], jnp.where(side == 0, za[:span_z], zb[:span_z]), 0.0)
    total = vals[...] + za[span_z:]
    if slabs == 4:
        total = total + zb[span_z:]
    for other in others:
        total = total + other[...]
    value[...] = total

    steps = xsrc.shape[0]
    chunks = value.shape[0] // steps
    per = wide.shape[2] // depth_y

    def of_face(f):
        vs = []
        for t in range(steps):
            pieces = [value[t * chunks + f * per + i : t * chunks + f * per + i + 1, :] for i in range(per)]
            vs.append(jnp.concatenate(pieces, axis=1))
        return vs

    for t, s in enumerate(face_source(of_face(0), rows_z[0], wide[0], width_z)):
        xsrc[t, : s.shape[0]] = s
    for t, s in enumerate(face_source(of_face(1), rows_x[...], wide[1], width_x)):
        zsrc[t, : s.shape[0]] = s
    ys = [
        face_source(of_face(2 + i), rows_z[1 + i], narrow[i], width_z) for i in range(2)
    ]

    lane = rows_of((width_z, LANES), 1)
    row = rows_of((width_z, LANES), 0)
    row_of_z = jnp.where(slab == 0, 0, jnp.where(slab == slabs - 1, width_z - 1, -1))
    row_of_x = jnp.where(box == 0, 0, jnp.where(box == boxes - 1, width_x - 1, -1))

    def plane_source(t, x):
        out = []
        for h in range(count):
            part = jnp.where(row == row_of_z, zsrc[t, x : x + 1, lanes(h)], 0.0)
            if h == 0:
                part = part + jnp.where(lane == 0, ys[0][t][:width_z, x : x + 1], 0.0)
            if h == count - 1:
                part = part + jnp.where(lane == LANES - 1, ys[1][t][:width_z, x : x + 1], 0.0)
            if x in (0, width_x - 1):
                part = part + jnp.where(row_of_x == x, xsrc[t, :width_z, lanes(h)], 0.0)
            out.append(part)
        return out

    lane_x = rows_of((width_x, LANES), 1)
    row_x = rows_of((width_x, LANES), 0)
    turned = [jnp.transpose(y[0]) for y in ys]

    def row_source(z):
        out = []
        for h in range(count):
            part = jnp.where(row_x == row_of_x, xsrc[0, z : z + 1, lanes(h)], 0.0)
            if h == 0:
                part = part + jnp.where(lane_x == 0, turned[0][:width_x, z : z + 1], 0.0)
            if h == count - 1:
                part = part + jnp.where(lane_x == LANES - 1, turned[1][:width_x, z : z + 1], 0.0)
            out.append(part)
        return out

    side_x, side_z = 2 * members * width_z, 2 * members * width_x
    halo_x, coef_x, coef_z = {}, {}, {}
    for s, (ref, x) in enumerate(((xlo, 0), (xhi, width_x - 1))):
        source = plane_source(0, width_x + s)
        for m in range(members):
            for h in range(count):
                coef = ref[side_x:, lanes(h)] * planes[m]
                base = ref[(members + m) * width_z : (members + m + 1) * width_z, lanes(h)]
                halo_x[s, m, h] = base + coef * now[h, m, x] + source[h]
                coef_x[s, m, h] = coef
    for s, (ref, z) in enumerate(((zlo, 0), (zhi, width_z - 1))):
        source = row_source(width_z + s)
        for m in range(members):
            for h in range(count):
                coef = ref[side_z:, lanes(h)] * edges[2 * m + s : 2 * m + s + 1]
                base = ref[(members + m) * width_x : (members + m + 1) * width_x, lanes(h)]
                hz[s, h, m] = base + coef * depth_rows(now, z, h, m) + source[h]
                coef_z[s, m, h] = coef
    sources = [plane_source(0, x) for x in range(width_x)]
    copies = []
    for m in range(members):
        for x in range(width_x):
            at = m * width_x + x
            for h in range(count):
                low_row, high_row = zlo[at : at + 1, lanes(h)], zhi[at : at + 1, lanes(h)]
                more = jnp.where(row == 0, low_row, jnp.where(row == width_z - 1, high_row, 0.0))
                if x == 0:
                    more = more + xlo[m * width_z : (m + 1) * width_z, lanes(h)]
                if x == width_x - 1:
                    more = more + xhi[m * width_z : (m + 1) * width_z, lanes(h)]
                one[h, m, x] = local[h, m, x] + (cour[h, x] * planes[m]) * more + sources[x][h]
        for h in range(count):
            copies.append(
                pltpu.make_async_copy(
                    one.at[h, m], last.at[m, :, :, pl.ds(h * LANES, LANES)], sems.at[len(copies)]
                )
            )
            copies[-1].start()
    for x in range(width_x):
        source = plane_source(1, x)
        for m in range(members):
            heres = [one[h, m, x] for h in range(count)]
            near = beside_y(heres)
            for h, here in enumerate(heres):
                rows = beside_rows(here, hz[0, h, m, x : x + 1], hz[1, h, m, x : x + 1])
                around = near[h] + rows
                around = around + (one[h, m, x - 1] if x > 0 else halo_x[0, m, h])
                around = around + (one[h, m, x + 1] if x < width_x - 1 else halo_x[1, m, h])
                coef = cour[h, x] * planes[m]
                nxt[h, m, x] = 2.0 * here - now[h, m, x] + coef * (around - 6.0 * here) + source[h]
                if x in (0, width_x - 1):
                    s = 0 if x == 0 else 1
                    for e, z in ((0, 0), (1, width_z - 1)):
                        beyond = coef_z[e, m, h][x : x + 1] + coef_x[s, m, h][z : z + 1]
                        at = 2 * (members * e + m) + s
                        late[at : at + 1, lanes(h)] = coef[z : z + 1] * beyond
    for copy in copies:
        copy.wait()


def fix_kernel(boxes, slabs, ca, cb, one, nxt, late, first, out, last, done, sems):
    count, members, width_x, width_z, _ = nxt.shape
    box, slab = lax.axis_index("box"), lax.axis_index("slab")
    side = lax.rem(slab, 2)
    open_x = (box > 0, box < boxes - 1)
    open_z = (slab > 0, slab < slabs - 1)
    row = rows_of((width_z, LANES), 0)
    copies = []

    def send(source, target):
        copies.append(pltpu.make_async_copy(source, target, sems.at[len(copies)]))
        copies[-1].start()

    for h in range(count):
        inside = pl.ds(1, width_x - 2)
        send(nxt.at[h, :, inside], out.at[:, inside, :, pl.ds(h * LANES, LANES)])
    for h in range(count):
        for s, x in ((0, 0), (1, width_x - 1)):
            for m in range(members):
                at = 2 * m + s
                add = 0.0
                for e, z in ((0, 0), (1, width_z - 1)):
                    got = jnp.where(
                        side == e, cb[at : at + 1, lanes(h)], ca[at : at + 1, lanes(h)]
                    )
                    got = jnp.where(open_x[s] & open_z[e], got, 0.0)
                    k = 2 * members * e + at
                    add = jnp.where(row == z, late[k : k + 1, lanes(h)] * got, add)
                done[h, s, m] = nxt[h, m, x] + add
            send(done.at[h, s], out.at[:, x, :, pl.ds(h * LANES, LANES)])
    for copy in copies:
        copy.wait()


def pairs_even(n):
    return [i ^ 1 for i in range(n)]


def pairs_odd(n):
    return [(i + 1) % n if i % 2 else (i - 1) % n for i in range(n)]


def on_device(
    boxes, slabs, pressure_now, pressure_prev, courant_sq, member_profiles, member_ids,
    stored_slabs, slab_home, interp_weights, surface_cells,
):
    members, width_x, width_z, depth_y = pressure_now.shape
    slots, samples, points = stored_slabs.shape
    steps = interp_weights.shape[0]
    total_z = width_z * slabs
    value_rows = steps * VALUE_FACES * surface_cells.shape[1] // depth_y
    span_x = (2 * members + 1) * width_z
    span_z = (2 * members + 1) * width_x
    count = depth_y // LANES

    def inner(*dims, dtype=F32):
        return pltpu.VMEM(dims, dtype)

    def far(*arrays):
        return [pltpu.with_memory_space_constraint(a, pltpu.HBM) for a in arrays]

    def near(*arrays):
        return [pltpu.with_memory_space_constraint(a, pltpu.VMEM) for a in arrays]

    def over_slab(x, partner):
        return lax.ppermute(x, "slab", list(enumerate(partner)))

    def over_box(x, odd):
        pairs = []
        for b in range(boxes):
            other = b ^ 1
            if odd:
                other = b + 1 if b % 2 else b - 1
            for s in range(slabs):
                inside = 0 <= other < boxes
                to = other * slabs + s if inside else b * slabs + (s ^ 1)
                pairs.append((b * slabs + s, to))
        return lax.ppermute(x, ("box", "slab"), pairs)

    whole = pressure_now.shape
    half = (count,) + whole[:3] + (LANES,)
    now, prev, cour, cells, planes, edges, za, zb, vals, xa, xb = pl.pallas_call(
        functools.partial(pack_kernel, slots, slabs),
        out_shape=(
            inner(*half),
            inner(*half),
            inner(count, width_x, width_z, LANES),
            inner(*surface_cells.shape, dtype=jnp.int32),
            inner(members, width_z, LANES),
            inner(2 * members, LANES),
            inner(span_z, depth_y),
            inner(span_z + value_rows, depth_y),
            inner(value_rows, depth_y),
            inner(span_x, depth_y),
            inner(span_x, depth_y),
        ),
        in_specs=[SMEM] + [HBM] * 8,
        out_specs=(VMEM,) * 11,
        scratch_shapes=[
            pltpu.SMEM(member_ids.shape, jnp.int32),
            pltpu.SMEM(interp_weights.shape, F32),
            pltpu.SMEM(member_profiles.shape, F32),
            pltpu.VMEM((samples, points), F32),
            pltpu.SemaphoreType.DMA((5 + 3 * count,)),
        ],
        compiler_params=PARAMS,
        name="pack",
    )(
        slab_home, *far(member_ids, interp_weights, member_profiles),
        *far(pressure_now, pressure_prev, courant_sq, surface_cells, stored_slabs),
    )

    per_face = surface_cells.shape[1]
    away = zb[span_z:]
    zb = over_slab(zb, pairs_odd(slabs))
    xa = over_box(xa, False)
    xb = over_box(xb, True)
    others = [
        over_slab(vals if k < slabs // 2 else away, [i ^ k for i in range(slabs)])
        for k in range(2, slabs)
        if slabs != 4
    ]
    now, prev, cour, cells, vals, planes, edges = near(
        now, prev, cour, cells, vals, planes, edges
    )
    high_x, high_z = up16(width_x + 2), up16(width_z + 2)
    local, wide, narrow, rows_x, rows_z = near(
        *pl.pallas_call(
            functools.partial(local_kernel, boxes, slabs, total_z),
            out_shape=(
                inner(*half),
                inner(2, depth_y, per_face, dtype=BF16),
                inner(2, high_x, per_face, dtype=BF16),
                inner(high_x, per_face, dtype=BF16),
                inner(3, high_z, per_face, dtype=BF16),
            ),
            in_specs=[VMEM] * 5,
            out_specs=(VMEM,) * 5,
            compiler_params=PARAMS,
            name="local",
        )(planes, cells, now, prev, cour)
    )
    za, zb, xa, xb, *others = near(za, zb, xa, xb, *others)
    za = pl.pallas_call(
        functools.partial(relay_kernel, slabs == 4),
        out_shape=inner(span_z + value_rows, depth_y),
        in_specs=[VMEM] * 4,
        out_specs=VMEM,
        compiler_params=PARAMS,
        name="relay",
    )(za, vals, zb, local)
    ca, cb = pl.pallas_call(
        functools.partial(corner_kernel, members, width_z),
        out_shape=(inner(CORNERS, depth_y),) * 2,
        in_specs=[VMEM] * 3,
        out_specs=(VMEM, VMEM),
        compiler_params=PARAMS,
        name="corner",
    )(xa, xb, *near(za))
    za = over_slab(za, pairs_even(slabs))
    ca = over_slab(ca, pairs_even(slabs))
    cb = over_slab(cb, pairs_odd(slabs))
    za, ca, cb = near(za, ca, cb)

    last, one, nxt, late = pl.pallas_call(
        functools.partial(main_kernel, boxes, slabs, len(others)),
        out_shape=(
            pltpu.HBM(whole, F32), inner(*half), inner(*half), inner(4 * members, depth_y),
        ),
        in_specs=[VMEM] * (14 + len(others)),
        out_specs=(HBM, VMEM, VMEM, VMEM),
        scratch_shapes=[
            inner(2, count, members, width_x, LANES),
            inner(span_x, depth_y),
            inner(span_x, depth_y),
            inner(span_z, depth_y),
            inner(span_z, depth_y),
            inner(value_rows, depth_y),
            inner(steps, high_z, depth_y),
            inner(steps, high_x, depth_y),
            pltpu.SemaphoreType.DMA((count * members,)),
        ],
        compiler_params=PARAMS,
        name="main",
    )(
        planes, edges, wide, narrow, rows_x, rows_z, now, local, cour,
        vals, za, zb, xa, xb, *others,
    )
    return pl.pallas_call(
        functools.partial(fix_kernel, boxes, slabs),
        out_shape=(pltpu.HBM(whole, F32),) * 2,
        in_specs=[VMEM] * 5 + [HBM],
        out_specs=(HBM, HBM),
        input_output_aliases={5: 1},
        scratch_shapes=[
            inner(count, 2, members, width_z, LANES),
            pltpu.SemaphoreType.DMA((3 * count,)),
        ],
        compiler_params=PARAMS,
        name="fix",
    )(ca, cb, *near(one, nxt, late), *far(last))


def solution(mesh):
    in_specs = (
        P("ens", "box", "slab", None),
        P("ens", "box", "slab", None),
        P("box", "slab", None),
        P(),
        P("ens"),
        P("slab", None, None),
        P("ens"),
        P(),
        P(),
    )
    out_specs = (P("ens", "box", "slab", None), P("ens", "box", "slab", None))
    boxes, slabs = mesh.shape["box"], mesh.shape["slab"]
    return jax.shard_map(
        functools.partial(on_device, boxes, slabs),
        mesh=mesh,
        in_specs=in_specs,
        out_specs=out_specs,
        check_vma=False,
    )
```
